256 devices in a mesh: seq: 32 (over y, z), head: 8 (over x, core).
Axes of the slice: x: 4, y: 4, z: 8, core: 2. Of those that a mesh axis runs over, the one named last changes fastest.
Arguments:
- tokens: bfloat16 [24576, 2560], P(('seq', 'head')), may hold values from -12 to 12
- pre_gain: float32 [2560], replicated, may hold values from 0.25 to 1.75
- inner_proj: bfloat16 [2560, 2, 5120], P(None, None, 'head'), may hold values from -0.125 to 0.125
- outer_proj: bfloat16 [2560, 336], replicated, may hold values from -0.125 to 0.125
- kernel_x: float32 [4, 5120], P(None, 'head'), may hold values from -3 to 3
- kernel_bc: float32 [4, 256], replicated, may hold values from -3 to 3
- offset_x: float32 [5120], P('head'), may hold values from -3 to 3
- offset_bc: float32 [256], replicated, may hold values from -3 to 3
- dt_bias: float32 [80], P('head'), may hold values from -7 to -5
- a_log: float32 [80], P('head'), may hold values from -12 to 4
- skip_gain: float32 [80], P('head'), may hold values from 0.5 to 1.5
- norm_gain: float32 [5120], P('head'), may hold values from 0.25 to 1.75
- out_proj: bfloat16 [5120, 2560], P('head'), may hold values from -0.078125 to 0.078125
Outputs:
- mixed: bfloat16 [24576, 2560], P(('seq', 'head'))
The draws below stay inside these ranges and needn't reach their ends.
All inputs are finite; a program needn't handle non-finite values.
Results may differ from the reference program's by a relative error of at most 0.014.
Values may be sent and summed in bfloat16 or wider, within the bound.
A program may use at most 128 MiB of HBM per device.

```python
import jax
import jax.numpy as jnp
from jax import lax

D = 2560
H = 80
P_SIZE = 64
N = 128
CONV = 4
SPAN = 256
DI = 5120
TOKENS = 24576
N_HEAD = 8


def draw_tokens(key, part):
    noise_key, level_key, course_key = jax.random.split(key, 3)
    blocks = TOKENS // SPAN
    noise = jax.random.normal(noise_key, (TOKENS, D), jnp.float32)
    levels = 2.0 * jax.random.normal(level_key, (blocks, 1, 1), jnp.float32)
    course = jax.random.normal(course_key, (1, 1, D), jnp.float32)
    shifted = noise.reshape(blocks, SPAN, D) + levels * course
    return jnp.clip(shifted.reshape(TOKENS, D), -12.0, 12.0).astype(jnp.bfloat16)


def draw_a_log(key, part):
    order_key, rate_key = jax.random.split(key)
    order = jax.random.permutation(order_key, H)
    share = H // 2
    quick = order < share
    spread = jax.random.uniform(rate_key, (H,), jnp.float32)
    quick_rate = jnp.log(4.0) + spread * jnp.log(10.0)
    patient_rate = jnp.log(10.0 / TOKENS) + spread * jnp.log(10.0)
    return jnp.where(quick, quick_rate, patient_rate).astype(jnp.float32)


def block_levels(own_key, dims, cuts, least, top_value):
    level = 1.0
    for dim, blocks in cuts:
        heights = jax.random.uniform(jax.random.fold_in(jax.random.fold_in(own_key, 6), dim), (blocks,), jnp.float32, least / len(cuts), top_value / len(cuts))
        level = level * jnp.repeat(jnp.exp(heights), dims[dim] // blocks).reshape((-1,) + (1,) * (len(dims) - 1 - dim))
    return level


def normal_values(stream_key, dims, scale, limit, cuts=(), kind=jnp.bfloat16):
    drawn = jax.random.normal(stream_key, dims, jnp.float32) * scale
    if len(cuts) > 0:
        drawn = block_levels(stream_key, dims, cuts, -0.22, 0.18) * drawn
    return jnp.clip(drawn, min=-limit, max=limit).astype(kind)


def setup_inputs(seed: int = 0) -> dict:
    streams_of = jax.random.split(jax.random.key(seed), 14)
    tokens = draw_tokens(jax.random.fold_in(streams_of[13], 71), 0)
    pre_gain = jnp.clip(1.0 + 0.15 * jax.random.normal(streams_of[1], (D,), jnp.float32), 0.25, 1.75)
    inner_proj = normal_values(streams_of[2], (D, 2, DI), D ** -0.5, 0.125, ((2, 8),))
    outer_proj = normal_values(streams_of[3], (D, 2 * N + H), D ** -0.5, 0.125)
    kernel_x = normal_values(streams_of[4], (CONV, DI), CONV ** -0.5, 3.0, ((1, 8),), jnp.float32)
    kernel_bc = normal_values(streams_of[5], (CONV, 2 * N), CONV ** -0.5, 3.0, (), jnp.float32)
    offset_x = normal_values(streams_of[6], (DI,), 0.5, 3.0, ((0, 8),), jnp.float32)
    offset_bc = normal_values(streams_of[7], (2 * N,), 0.5, 3.0, (), jnp.float32)
    dt_bias = jnp.clip(-7.0 + 2.0 * jax.random.uniform(streams_of[8], (H,), jnp.float32) ** block_levels(streams_of[8], (H,), ((0, 8),), -0.2, 0.2), -7.0, -5.0)
    a_log = draw_a_log(jax.random.fold_in(streams_of[13], 71), 0)
    skip_gain = jnp.clip(0.5 + 1.0 * jax.random.uniform(streams_of[10], (H,), jnp.float32) ** block_levels(streams_of[10], (H,), ((0, 8),), -0.2, 0.2), 0.5, 1.5)
    norm_gain = jnp.clip(1.0 + 0.15 * jax.random.normal(streams_of[11], (DI,), jnp.float32), 0.25, 1.75)
    out_proj = normal_values(streams_of[12], (DI, D), DI ** -0.5, 0.078125, ((0, 8),))
    return {"tokens": tokens, "pre_gain": pre_gain, "inner_proj": inner_proj, "outer_proj": outer_proj, "kernel_x": kernel_x, "kernel_bc": kernel_bc, "offset_x": offset_x, "offset_bc": offset_bc, "dt_bias": dt_bias, "a_log": a_log, "skip_gain": skip_gain, "norm_gain": norm_gain, "out_proj": out_proj}


norm_floor = 0.1

def row_norm(row_block, gain_vector):
    widened = row_block.astype(jnp.float32)
    inverse_rms = lax.rsqrt(lax.optimization_barrier(jnp.mean(widened * widened, axis=-1, keepdims=True)) + norm_floor)
    return widened * inverse_rms * gain_vector

def masked_exp(log_gap, causal):
    return jnp.where(causal, jnp.exp(jnp.where(causal, log_gap, 0.0)), 0.0)

def block_scan(values_x, values_b, values_c, step_sizes, decay_rate, ssm_state):
    running = jnp.cumsum(step_sizes * decay_rate, axis=0)
    score_rows = jnp.dot(values_c, values_b.T, preferred_element_type=jnp.float32)
    running_heads = running.T
    row_index = lax.broadcasted_iota(jnp.int32, (SPAN, SPAN), 0)
    col_index = lax.broadcasted_iota(jnp.int32, (SPAN, SPAN), 1)
    decay_factor = masked_exp(running_heads[:, :, None] - running_heads[:, None, :], row_index >= col_index)
    mix_weights = (score_rows[None] * decay_factor * step_sizes.T[:, None, :]).astype(jnp.bfloat16)
    intra_out = jnp.einsum('hts,shp->thp', mix_weights.astype(jnp.float32), values_x.astype(jnp.float32))
    end_weight = jnp.exp(running[-1:] - running) * step_sizes
    scaled_x = (values_x.astype(jnp.float32) * end_weight[:, :, None]).astype(jnp.bfloat16)
    block_state = jnp.einsum('shp,sn->hpn', scaled_x.astype(jnp.float32), values_b.astype(jnp.float32))
    cross_out = jnp.exp(running)[:, :, None] * jnp.einsum('tn,hpn->thp', values_c.astype(jnp.float32), ssm_state, precision=lax.Precision.HIGHEST)
    next_state = jnp.exp(running[-1])[:, None, None] * ssm_state + block_state
    return (intra_out + cross_out, next_state)

def reference(tokens, pre_gain, inner_proj, outer_proj, kernel_x, kernel_bc, offset_x, offset_bc, dt_bias, a_log, skip_gain, norm_gain, out_proj):
    decay_rate = -jnp.exp(a_log)
    joined_proj = inner_proj.reshape(D, 2 * DI)
    conv_weight = jnp.concatenate([kernel_x, kernel_bc], axis=1)
    conv_bias = jnp.concatenate([offset_x, offset_bc])
    group_width = DI // N_HEAD

    def advance(carry, row_block):
        ssm_state, conv_tail = carry
        normed = row_norm(row_block, pre_gain).astype(jnp.bfloat16)
        inner_part = jnp.dot(normed, joined_proj, preferred_element_type=jnp.float32)
        outer_part = jnp.dot(normed, outer_proj, preferred_element_type=jnp.float32)
        gate_in = inner_part[:, :DI].astype(jnp.bfloat16)
        x_in = inner_part[:, DI:].astype(jnp.bfloat16)
        bc_in = outer_part[:, :2 * N].astype(jnp.bfloat16)
        dt_raw = outer_part[:, 2 * N:]
        conv_input = jnp.concatenate([x_in, bc_in], axis=1)
        extended = jnp.concatenate([conv_tail, conv_input], axis=0)
        summed = jnp.broadcast_to(conv_bias, conv_input.shape).astype(jnp.float32)
        for offset in range(CONV):
            summed = summed + conv_weight[offset] * extended[offset:offset + SPAN].astype(jnp.float32)
        conv_out = jax.nn.silu(summed).astype(jnp.bfloat16)
        values_x = conv_out[:, :DI].reshape(SPAN, H, P_SIZE)
        values_b = conv_out[:, DI:DI + N]
        values_c = conv_out[:, DI + N:]
        step_sizes = jax.nn.softplus(dt_raw + dt_bias)
        scan_out, next_state = block_scan(values_x, values_b, values_c, step_sizes, decay_rate, ssm_state)
        mixer_out = (scan_out + skip_gain[:, None] * values_x.astype(jnp.float32)).reshape(SPAN, DI)
        gated = mixer_out * jax.nn.silu(gate_in.astype(jnp.float32))
        normed_out = row_norm(gated, norm_gain).astype(jnp.bfloat16)
        total = jnp.zeros((SPAN, D), jnp.float32)
        for offset in range(N_HEAD):
            lower = offset * group_width
            partial_value = jnp.dot(normed_out[:, lower:lower + group_width], out_proj[lower:lower + group_width], preferred_element_type=jnp.float32).astype(jnp.bfloat16)
            total = total + lax.optimization_barrier(partial_value).astype(jnp.float32)
        next_tail = extended[SPAN:]
        return ((next_state, next_tail), total.astype(jnp.bfloat16))
    start_state = jnp.zeros((H, P_SIZE, N), jnp.float32)
    start_tail = jnp.zeros((CONV - 1, DI + 2 * N), jnp.bfloat16)
    blocks_in = tokens.reshape(TOKENS // SPAN, SPAN, D)
    final_carry, outputs = lax.scan(advance, (start_state, start_tail), blocks_in)
    return outputs.reshape(TOKENS, D)
```

```python
import functools

import jax
import jax.numpy as jnp
from jax import lax
from jax.experimental import pallas as pl
from jax.experimental.pallas import tpu as pltpu
from jax.sharding import PartitionSpec as P

MESH = pl.DeviceIdType.MESH
BF16 = jnp.bfloat16
F32 = jnp.float32

NORM_FLOOR = 0.1
D = 2560
DL = 640
NS = 128
R = 96
HALF = 48
T = 768
Q = 128
NQ = 6
CH = 192
HEADS = 10
NY, NZ, NX = 4, 8, 4


def dot(a, b):
    return jnp.dot(a, b, preferred_element_type=F32)


def dot_t(a, b):
    return lax.dot_general(a, b, (((1,), (1,)), ((), ())), preferred_element_type=F32)


def t_dot(a, b):
    return lax.dot_general(a, b, (((0,), (0,)), ((), ())), preferred_element_type=F32)


def split2(v):
    hi = v.astype(BF16)
    lo = (v - hi.astype(F32)).astype(BF16)
    return hi, lo


def split3(v):
    hi, mid = split2(v)
    lo = (v - hi.astype(F32) - mid.astype(F32)).astype(BF16)
    return hi, mid, lo


def silu(v):
    return v / (1.0 + jnp.exp(-v))


def remote(src, dst, send, recv, device):
    return pltpu.make_async_remote_copy(
        src_ref=src, dst_ref=dst, send_sem=send, recv_sem=recv, device_id=device, device_id_type=MESH
    )


def kernel(
    tokens, pre_gain, w_hbm, wo_hbm, kernel_x, kernel_bc, offset_x, offset_bc, dt_bias, a_log,
    skip_gain, norm_gain, wout_hbm,
    out,
    w, wo, wout, rows, xin, dtr, zs, xb, bmat, cmat, dts, cum, expand, ef, sl, sacc, pdr, pdacc,
    yv, sb, drow, rz, rd, pz, pdz, tb, tdb, ty, tdy, cacc, pb, cr, gb, sqc, part, pr, ps, rl, rf,
    sqs, sqr, small,
    ag_s, ag_r, halo_s, halo_r, zs_s, zs_r, zd_s, zd_r, y_s, y_r, yd_s, yd_r, bk_s, bk_r,
    pp_s, pp_r, rl_s, rl_r, rf_s, rf_r, sq_s, sq_r, w_s,
):
    s = lax.axis_index("seq")
    h = lax.axis_index("head")
    y = s // NZ
    z = s % NZ
    x = h // 2
    c = h % 2
    partner = x * 2 + (1 - c)
    xr = (x + 1) % NX
    xl = (x + NX - 1) % NX
    xo = (x + 2) % NX
    hr, hl, ho = xr * 2 + c, xl * 2 + c, xo * 2 + c

    w_copies = [
        pltpu.make_async_copy(w_hbm, w, w_s.at[0]),
        pltpu.make_async_copy(wo_hbm, wo, w_s.at[1]),
        pltpu.make_async_copy(wout_hbm, wout, w_s.at[2]),
    ]
    for cp in w_copies:
        cp.start()

    barrier = pltpu.get_barrier_semaphore()
    for k in range(1, 8):
        pl.semaphore_signal(barrier, inc=1, device_id=(s, (h + k) % 8), device_id_type=MESH)
    for k in range(1, NZ):
        pl.semaphore_signal(barrier, inc=1, device_id=(y * NZ + (z + k) % NZ, h), device_id_type=MESH)
    for k in range(1, NY):
        pl.semaphore_signal(barrier, inc=1, device_id=(((y + k) % NY) * NZ + z, h), device_id_type=MESH)
    for k in (1, 31):
        pl.semaphore_signal(barrier, inc=1, device_id=((s + k) % 32, h), device_id_type=MESH)

    for half in range(2):
        tk = tokens[half * HALF : (half + 1) * HALF, :].astype(F32)
        inv = lax.rsqrt(jnp.mean(tk * tk, axis=1, keepdims=True) + NORM_FLOOR)
        rows[h, half] = (tk * inv * pre_gain[...]).astype(BF16)

    pl.semaphore_wait(barrier, 19)

    def ag(origin, half, role, device):
        return remote(
            rows.at[origin, half], rows.at[origin, half], ag_s.at[role], ag_r.at[role], (s, device)
        )

    own_pair = remote(rows.at[h], rows.at[h], ag_s.at[6], ag_r.at[6], (s, partner))
    sends = [ag(h, 0, 0, hr), ag(h, 1, 3, hl), ag(h, 1, 1, hr), ag(h, 0, 2, hl)]
    own_pair.start()
    for cp in sends:
        cp.start()

    li = lax.broadcasted_iota(jnp.int32, (2 * Q, DL), 0)
    lc = lax.broadcasted_iota(jnp.int32, (2 * Q, DL), 1)
    head_of = lax.shift_right_logical(lc, 6)
    expand[...] = jnp.where(jnp.bitwise_and(li, Q - 1) == head_of, 1.0, 0.0).astype(BF16)
    small[...] = jnp.zeros_like(small)
    small[0:1, 0:HEADS] = dt_bias[...]
    small[1:2, 0:HEADS] = a_log[...]
    small[2:3, 0:HEADS] = skip_gain[...]
    dtr[...] = jnp.zeros_like(dtr)
    for cp in w_copies:
        cp.wait()

    def project(chip, with_x, with_z):
        n = rows[pl.ds(2 * chip, 2)].reshape(CH, D)
        at = pl.multiple_of(chip * CH, CH)
        if with_x:
            xin[pl.ds(pl.multiple_of(at + 8, 8), CH), 0:DL] = dot(n, w[1]).astype(BF16).astype(F32)
            xin[pl.ds(pl.multiple_of(at + 8, 8), CH), DL : DL + 2 * NS] = (
                dot_t(n, wo[0 : 2 * NS, :]).astype(BF16).astype(F32)
            )
            dtr[pl.ds(at, CH), 0:80] = dot_t(n, wo[2 * NS : 2 * NS + 80, :])
        if with_z:
            zz = dot(n, w[0]).astype(BF16).astype(F32)
            zs[pl.ds(at, CH), :] = silu(zz)

    remote(rows.at[partner], rows.at[partner], ag_s.at[6], ag_r.at[6], (s, partner)).wait_recv()
    project(x, True, True)

    def to_partner(origin, half, role):
        cp = ag(origin, half, 7 + role, partner)
        cp.start()
        sends.append(cp)

    def partner_done(chip, half, role):
        ag(chip * 2 + 1 - c, half, 7 + role, partner).wait_recv()

    ag(hl, 0, 0, hr).wait_recv()
    cp = ag(hl, 0, 4, hr)
    cp.start()
    sends.append(cp)
    ag(hr, 1, 3, hl).wait_recv()
    cp = ag(hr, 1, 5, hl)
    cp.start()
    sends.append(cp)
    to_partner(hl, 0, 0)
    to_partner(hr, 1, 3)
    ag(hl, 1, 1, hr).wait_recv()
    to_partner(hl, 1, 1)
    ag(hr, 0, 2, hl).wait_recv()
    to_partner(hr, 0, 2)
    partner_done(xl, 0, 0)
    partner_done(xl, 1, 1)
    project(xl, True, True)
    partner_done(xr, 1, 3)
    partner_done(xr, 0, 2)
    project(xr, True, True)
    ag(ho, 0, 4, hr).wait_recv()
    to_partner(ho, 0, 4)
    ag(ho, 1, 5, hl).wait_recv()
    to_partner(ho, 1, 5)
    partner_done(xo, 0, 4)
    partner_done(xo, 1, 5)
    project(xo, True, False)

    halo = remote(xin.at[pl.ds(T, 8)], xin.at[pl.ds(0, 8)], halo_s, halo_r, ((s + 1) % 32, h))

    @pl.when(s < 31)
    def _():
        halo.start()

    lane = lax.broadcasted_iota(jnp.int32, (1, Q), 1)
    ri = lax.broadcasted_iota(jnp.int32, (Q, Q), 0)
    ci = lax.broadcasted_iota(jnp.int32, (Q, Q), 1)
    tri = jnp.where(ri >= ci, 1.0, 0.0).astype(BF16)
    bias_row = small[0:1, :]
    rate_row = -jnp.exp(small[1:2, :])
    shift = (Q - h * HEADS) % Q
    total = jnp.zeros((1, Q), F32)
    for q in range(NQ):
        raw = pltpu.roll(dtr[q * Q : (q + 1) * Q, :], shift, 1) + bias_row
        step = jnp.maximum(raw, 0.0) + jnp.log1p(jnp.exp(-jnp.abs(raw)))
        step = jnp.where(lane < HEADS, step, 0.0)
        la = step * rate_row
        dts[q] = step
        p3 = dot(tri, jnp.concatenate(split3(la), axis=1))
        cq = p3[:, 0:Q] + p3[:, Q : 2 * Q] + p3[:, 2 * Q : 3 * Q]
        cum[q] = cq
        total = total + cq[Q - 1 : Q, :]
    drow[...] = jnp.broadcast_to(jnp.exp(total), (8, Q))
    rd[z] = drow[...]

    def z_peer(k):
        return (z + k) % NZ

    for k in range(1, NZ):
        zp = z_peer(k)
        remote(drow, rd.at[z], zd_s.at[k], zd_r.at[z], (y * NZ + zp, h)).start()

    def conv_block(i):
        at = pl.multiple_of(i * 64, 64)
        for lo, hi, kern, off in ((0, DL, kernel_x, offset_x), (DL, DL + 2 * NS, kernel_bc, offset_bc)):
            u = jnp.broadcast_to(off[...], (64, hi - lo))
            v = xin[pl.ds(at, 72), lo:hi]
            for k in range(4):
                u = u + kern[k : k + 1, :] * v[5 + k : 69 + k, :]
            v = silu(u).astype(BF16)
            if lo == 0:
                xb[pl.ds(at, 64), :] = v
            else:
                bmat[pl.ds(at, 64), :] = v[:, 0:NS]
                cmat[pl.ds(at, 64), :] = v[:, NS : 2 * NS]

    def conv_step(i, carry):
        conv_block(i)
        return carry

    lax.fori_loop(1, T // 64, conv_step, 0)

    @pl.when(s == 0)
    def _():
        xin[0:8, :] = jnp.zeros((8, DL + 2 * NS), F32)

    @pl.when(s > 0)
    def _():
        halo.wait_recv()

    conv_block(0)

    sacc[...] = jnp.zeros_like(sacc)
    pdacc[...] = jnp.ones_like(pdacc)

    def state_step(q, carry):
        at = pl.multiple_of(q * Q, Q)
        cq = cum[q]
        fac = jnp.exp(cq[Q - 1 : Q, :] - cq) * dts[q]
        fx = dot(jnp.concatenate(split2(fac), axis=1), expand[...])
        ex = dot(jnp.concatenate(split2(jnp.exp(cq)), axis=1), expand[...])
        ef[q] = ex
        xw = (xb[pl.ds(at, Q), :].astype(F32) * fx).astype(BF16)
        st = t_dot(bmat[pl.ds(at, Q), :], xw)
        dec = ex[Q - 1 : Q, :]
        prev = sacc[...]
        sl[q] = prev
        sacc[...] = prev * dec + st
        pdr[q] = pdacc[...]
        pdacc[...] = pdacc[...] * dec
        return carry

    lax.fori_loop(0, NQ, state_step, 0)
    sb[...] = sacc[...].astype(BF16)
    rz[z] = sb[pl.ds(pl.multiple_of(z * 16, 16), 16), :]

    for k in range(1, NZ):
        zp = z_peer(k)
        remote(
            sb.at[pl.ds(pl.multiple_of(zp * 16, 16), 16)], rz.at[z], zs_s.at[k], zs_r.at[z],
            (y * NZ + zp, h),
        ).start()

    project(xo, False, True)
    s3 = jnp.concatenate(split2(jnp.broadcast_to(small[2:3, :], (8, Q))), axis=1)
    skip_row = dot(s3, expand[...])[0:1, :]
    low = lax.broadcasted_iota(jnp.int32, (Q, Q), 1) < 64

    def intra_step(q, carry):
        at = pl.multiple_of(q * Q, Q)
        cq = cum[q]
        cqt = jnp.transpose(cq)
        dtt = jnp.transpose(dts[q])
        cb = dot_t(cmat[pl.ds(at, Q), :], bmat[pl.ds(at, Q), :])
        cbm = jnp.where(ri >= ci, cb, 0.0)
        for j in range(HEADS // 2):
            mixes = []
            for hh in (2 * j, 2 * j + 1):
                gap = jnp.minimum(cq[:, hh : hh + 1] - cqt[hh : hh + 1, :], 0.0)
                mixes.append((cbm * jnp.exp(gap) * dtt[hh : hh + 1, :]).astype(BF16))
            xp = xb[pl.ds(at, Q), j * Q : (j + 1) * Q].astype(F32)
            xd = jnp.concatenate(
                [jnp.where(low, xp, 0.0).astype(BF16), jnp.where(low, 0.0, xp).astype(BF16)], axis=0
            )
            yq = dot(jnp.concatenate(mixes, axis=1), xd)
            yv[pl.ds(at, Q), j * Q : (j + 1) * Q] = yq + skip_row[:, j * Q : (j + 1) * Q] * xp
        return carry

    lax.fori_loop(0, NQ, intra_step, 0)

    for k in range(1, NZ):
        zp = z_peer(k)
        remote(drow, rd.at[zp], zd_s.at[k], zd_r.at[zp], (y * NZ + zp, h)).wait_recv()
        remote(sb.at[pl.ds(0, 16)], rz.at[zp], zs_s.at[k], zs_r.at[zp], (y * NZ + zp, h)).wait_recv()
    dz = jnp.concatenate([rd[k][0:1, :] for k in range(NZ)], axis=0)
    dx = dot(jnp.concatenate(split2(dz), axis=1), expand[...])
    acc = jnp.zeros((16, DL), F32)
    pd = jnp.ones((1, DL), F32)
    for k in range(NZ):
        pz[k] = acc
        pdz[k] = jnp.broadcast_to(pd, (8, DL))
        acc = acc * dx[k : k + 1, :] + rz[k].astype(F32)
        pd = pd * dx[k : k + 1, :]
    tb[...] = acc.astype(BF16)
    tdb[...] = jnp.broadcast_to(pd, (8, DL))

    for k in range(1, NY):
        @pl.when(y + k < NY)
        def _(k=k):
            dev = ((y + k) % NY * NZ + z, h)
            remote(tb, ty.at[y], y_s.at[k], y_r.at[y], dev).start()
            remote(tdb, tdy.at[y], yd_s.at[k], yd_r.at[y], dev).start()

    cacc[...] = jnp.zeros_like(cacc)
    for k in range(NY - 1):
        @pl.when(k < y)
        def _(k=k):
            dev = (k * NZ + z, h)
            remote(tb, ty.at[k], y_s.at[1], y_r.at[k], dev).wait_recv()
            remote(tdb, tdy.at[k], yd_s.at[1], yd_r.at[k], dev).wait_recv()
            cacc[...] = cacc[...] * tdy[k][0:1, :] + ty[k].astype(F32)

    for k in range(NZ):
        pb[k] = (pz[k] + pdz[k][0:1, :] * cacc[...]).astype(BF16)
    cr[z] = pb[z]
    for k in range(1, NZ):
        zp = z_peer(k)
        remote(pb.at[zp], cr.at[z], bk_s.at[k], bk_r.at[z], (y * NZ + zp, h)).start()
    for k in range(1, NZ):
        zp = z_peer(k)
        remote(pb.at[zp], cr.at[zp], bk_s.at[k], bk_r.at[zp], (y * NZ + zp, h)).wait_recv()

    def out_step(q, carry):
        at = pl.multiple_of(q * Q, Q)
        state = (sl[q] + pdr[q][0:1, :] * cr[...].reshape(NS, DL).astype(F32)).astype(BF16)
        cross = dot(cmat[pl.ds(at, Q), :], state)
        g = (yv[pl.ds(at, Q), :] + ef[q] * cross) * zs[pl.ds(at, Q), :]
        sqc[pl.ds(at, Q), :] = jnp.broadcast_to(jnp.sum(g * g, axis=1, keepdims=True), (Q, Q))
        gb[pl.ds(at, Q), :] = (g * norm_gain[...]).astype(BF16)
        return carry

    pair_sends = []

    def out_chip(d):
        n = gb[pl.ds(pl.multiple_of(d * CH, CH), CH), :]
        for lo in range(0, D, 512):
            part[pl.ds(2 * d, 2), :, :, lo : lo + 512] = (
                dot(n, wout[:, lo : lo + 512]).astype(BF16).reshape(2, 2, HALF, 512)
            )
        cp = remote(part.at[2 * d + 1 - c], pr.at[d], pp_s.at[d], pp_r.at[d], (s, partner))
        cp.start()
        pair_sends.append(cp)

    def pair_sum(d, half):
        return part[2 * d + c, half].astype(F32) + pr[d, half].astype(F32)

    def pair_wait(d):
        remote(part.at[0], pr.at[d], pp_s.at[d], pp_r.at[d], (s, partner)).wait_recv()

    first = xo // 2
    d1 = xo + 1 - 2 * (xo % 2)
    d2 = x + 1 - 2 * (x % 2)
    lax.fori_loop(first * 3, first * 3 + 3, out_step, 0)
    out_chip(xo)
    out_chip(d1)
    pair_wait(xo)
    for half in range(2):
        ps[0, half] = pair_sum(xo, half).astype(BF16)
    relays = [
        remote(ps.at[0, 0], rl.at[0], rl_s.at[0], rl_r.at[0], (s, hr)),
        remote(ps.at[0, 1], rl.at[1], rl_s.at[1], rl_r.at[1], (s, hl)),
    ]
    for cp in relays:
        cp.start()

    def side_of(d):
        return jnp.where(d == xr, 0, 1)

    finals = []

    def final_send(slot, d, half):
        side = side_of(d)
        cp = remote(
            ps.at[slot, half], rf.at[side, half], rf_s.at[side, half], rf_r.at[side, half], (s, 2 * d + c)
        )
        cp.start()
        finals.append(cp)

    def send_direct(slot, d):
        half = 1 - side_of(d)
        pair_wait(d)
        ps[slot, half] = pair_sum(d, half).astype(BF16)
        final_send(slot, d, half)

    def send_relayed(slot, d):
        half = side_of(d)
        remote(ps.at[0, 0], rl.at[half], rl_s.at[half], rl_r.at[half], (s, hr)).wait_recv()
        ps[slot, half] = (pair_sum(d, half) + rl[half].astype(F32)).astype(BF16)
        final_send(slot, d, half)

    send_direct(1, d1)
    second = x // 2
    lax.fori_loop(second * 3, second * 3 + 3, out_step, 0)
    out_chip(d2)
    send_direct(2, d2)
    send_relayed(1, d1)
    send_relayed(2, d2)
    out_chip(x)

    sq_sends = []
    for k in range(8):
        col = sqc[pl.ds(pl.multiple_of(((h + k) % 8) * R, 32), Q), :]
        sqs[(h + k) % 8] = jnp.transpose(col)[0:8, :]
        if k == 0:
            sqr[h] = sqs[h]
        else:
            cp = remote(sqs.at[(h + k) % 8], sqr.at[h], sq_s.at[k], sq_r.at[h], (s, (h + k) % 8))
            cp.start()
            sq_sends.append(cp)
    pair_wait(x)
    for k in range(1, 8):
        hk = (h + k) % 8
        remote(sqs.at[0], sqr.at[hk], sq_s.at[k], sq_r.at[hk], (s, hk)).wait_recv()
    squares = jnp.sum(sqr[...], axis=0)[0:1, :]
    inv_row = lax.rsqrt(squares / (DL * 8) + NORM_FLOOR)
    inv_col = jnp.transpose(jnp.broadcast_to(inv_row, (Q, Q)))
    for half in range(2):
        for side in range(2):
            remote(
                ps.at[1, half], rf.at[side, half], rf_s.at[side, half], rf_r.at[side, half], (s, hl)
            ).wait_recv()
    for half in range(2):
        tot = pair_sum(x, half) + rf[0, half].astype(F32) + rf[1, half].astype(F32)
        out[half * HALF : (half + 1) * HALF, :] = (
            tot * inv_col[half * HALF : (half + 1) * HALF, 0:1]
        ).astype(BF16)

    own_pair.wait_send()
    for cp in sends + pair_sends + relays + finals + sq_sends:
        cp.wait_send()

    @pl.when(s < 31)
    def _():
        halo.wait_send()

    for k in range(1, NZ):
        zp = z_peer(k)
        dev = (y * NZ + zp, h)
        remote(drow, rd.at[z], zd_s.at[k], zd_r.at[z], dev).wait_send()
        remote(sb.at[pl.ds(0, 16)], rz.at[z], zs_s.at[k], zs_r.at[z], dev).wait_send()
        remote(pb.at[zp], cr.at[z], bk_s.at[k], bk_r.at[z], dev).wait_send()
    for k in range(1, NY):
        @pl.when(y + k < NY)
        def _(k=k):
            dev = ((y + k) % NY * NZ + z, h)
            remote(tb, ty.at[y], y_s.at[k], y_r.at[y], dev).wait_send()
            remote(tdb, tdy.at[y], yd_s.at[k], yd_r.at[y], dev).wait_send()


def on_device(
    tokens, pre_gain, inner_proj, outer_proj, kernel_x, kernel_bc, offset_x, offset_bc, dt_bias, a_log,
    skip_gain, norm_gain, out_proj,
):
    w = jnp.transpose(inner_proj, (1, 0, 2))
    vm = pl.BlockSpec(memory_space=pltpu.VMEM)
    hbm = pl.BlockSpec(memory_space=pl.ANY)
    dma = pltpu.SemaphoreType.DMA
    V = pltpu.VMEM
    scratch = [
        V((2, D, DL), BF16), V((336, D), BF16), V((DL, D), BF16), V((8, 2, HALF, D), BF16),
        V((T + 8, DL + 2 * NS), F32), V((T, Q), F32), V((T, DL), F32), V((T, DL), BF16),
        V((T, NS), BF16), V((T, NS), BF16), V((NQ, Q, Q), F32), V((NQ, Q, Q), F32),
        V((2 * Q, DL), BF16), V((NQ, Q, DL), F32), V((NQ, NS, DL), F32), V((NS, DL), F32),
        V((NQ, 8, DL), F32), V((8, DL), F32),
        V((T, DL), F32), V((NS, DL), BF16), V((8, Q), F32), V((NZ, 16, DL), BF16), V((NZ, 8, Q), F32),
        V((NZ, 16, DL), F32), V((NZ, 8, DL), F32), V((16, DL), BF16), V((8, DL), F32),
        V((NY, 16, DL), BF16), V((NY, 8, DL), F32), V((16, DL), F32), V((NZ, 16, DL), BF16),
        V((NZ, 16, DL), BF16), V((T, DL), BF16), V((T + 32, Q), F32), V((8, 2, HALF, D), BF16),
        V((NX, 2, HALF, D), BF16), V((3, 2, HALF, D), BF16), V((2, HALF, D), BF16), V((2, 2, HALF, D), BF16),
        V((8, 8, Q), F32), V((8, 8, Q), F32), V((8, Q), F32),
        dma((13,)), dma((13,)), dma, dma, dma((NZ,)), dma((NZ,)), dma((NZ,)), dma((NZ,)),
        dma((NY,)), dma((NY,)), dma((NY,)), dma((NY,)), dma((NZ,)), dma((NZ,)),
        dma((NX,)), dma((NX,)), dma((2,)), dma((2,)), dma((2, 2)), dma((2, 2)), dma((8,)), dma((8,)),
        dma((3,)),
    ]
    return pl.pallas_call(
        kernel,
        out_shape=jax.ShapeDtypeStruct((R, D), BF16),
        in_specs=[vm, vm, hbm, hbm, vm, vm, vm, vm, vm, vm, vm, vm, hbm],
        out_specs=vm,
        scratch_shapes=scratch,
        compiler_params=pltpu.CompilerParams(
            collective_id=0, has_side_effects=True, vmem_limit_bytes=66_000_000
        ),
    )(
        tokens, pre_gain[None], w, outer_proj.T, kernel_x, kernel_bc, offset_x[None], offset_bc[None],
        dt_bias[None], a_log[None], skip_gain[None], norm_gain[None], out_proj,
    )


def solution(mesh):
    in_specs = (
        P(("seq", "head"), None), P(), P(None, None, "head"), P(), P(None, "head"), P(), P("head"), P(),
        P("head"), P("head"), P("head"), P("head"), P("head", None),
    )
    return jax.shard_map(
        on_device, mesh=mesh, in_specs=in_specs, out_specs=P(("seq", "head"), None), check_vma=False
    )
```

```python
import functools

import jax
import jax.numpy as jnp
from jax import lax
from jax.experimental import pallas as pl
from jax.experimental.pallas import tpu as pltpu
from jax.sharding import PartitionSpec as P

MESH = pl.DeviceIdType.MESH
BF16 = jnp.bfloat16
F32 = jnp.float32

NORM_FLOOR = 0.1
D = 2560
DL = 640
NS = 128
R = 96
HALF = 48
T = 768
Q = 128
NQ = 6
CH = 192
HEADS = 10
NY, NZ, NX = 4, 8, 4


def dot(a, b):
    return jnp.dot(a, b, preferred_element_type=F32)


def dot_t(a, b):
    return lax.dot_general(a, b, (((1,), (1,)), ((), ())), preferred_element_type=F32)


def t_dot(a, b):
    return lax.dot_general(a, b, (((0,), (0,)), ((), ())), preferred_element_type=F32)


def split2(v):
    hi = v.astype(BF16)
    lo = (v - hi.astype(F32)).astype(BF16)
    return hi, lo


def split3(v):
    hi, mid = split2(v)
    lo = (v - hi.astype(F32) - mid.astype(F32)).astype(BF16)
    return hi, mid, lo


def silu(v):
    half = 0.5 * v
    return half + half * jnp.tanh(half)


def remote(src, dst, send, recv, device):
    return pltpu.make_async_remote_copy(
        src_ref=src, dst_ref=dst, send_sem=send, recv_sem=recv, device_id=device, device_id_type=MESH
    )


def kernel(
    tokens_in, pre_gain_in, w_hbm, wo_hbm, kernel_x_in, kernel_bc_in, offset_x_in, offset_bc_in, dt_bias_in,
    a_log_in, skip_gain_in, norm_gain_in, wout_hbm,
    out,
    tokens, pre_gain_v, kernel_x, kernel_bc, offset_x_v, offset_bc, dt_bias, a_log, skip_gain, norm_gain_v,
    wraw, w, wo, wout, rows, xin, dtr, zs, xb, bmat, cmat, dts, cum, expand, ef, sl, pdr,
    yv, sb, drow, rz, rd, pz, pdz, tb, tdb, ty, tdy, cacc, pb, cr, gb, sqc, part, pr, ps, rl, rf,
    sqs, sqr, small, pre_gain, offset_x, norm_gain,
    ag_s, ag_r, halo_s, halo_r, zs_s, zs_r, zd_s, zd_r, y_s, y_r, yd_s, yd_r, bk_s, bk_r,
    pp_s, pp_r, rl_s, rl_r, rf_s, rf_r, sq_s, sq_r, w_s, in_s,
):
    s = lax.axis_index("seq")
    h = lax.axis_index("head")
    y = s // NZ
    z = s % NZ
    x = h // 2
    c = h % 2
    partner = x * 2 + (1 - c)
    xr = (x + 1) % NX
    xl = (x + NX - 1) % NX
    xo = (x + 2) % NX
    hr, hl, ho = xr * 2 + c, xl * 2 + c, xo * 2 + c

    barrier = pltpu.get_barrier_semaphore()
    for k in range(1, 8):
        pl.semaphore_signal(barrier, inc=1, device_id=(s, (h + k) % 8), device_id_type=MESH)
    for k in range(1, NZ):
        pl.semaphore_signal(barrier, inc=1, device_id=(y * NZ + (z + k) % NZ, h), device_id_type=MESH)
    for k in range(1, NY):
        pl.semaphore_signal(barrier, inc=1, device_id=(((y + k) % NY) * NZ + z, h), device_id_type=MESH)
    for k in (1, 31):
        pl.semaphore_signal(barrier, inc=1, device_id=((s + k) % 32, h), device_id_type=MESH)

    pairs = (
        (tokens_in, tokens), (pre_gain_in, pre_gain_v), (kernel_x_in, kernel_x), (kernel_bc_in, kernel_bc),
        (offset_x_in, offset_x_v), (offset_bc_in, offset_bc), (dt_bias_in, dt_bias), (a_log_in, a_log),
        (skip_gain_in, skip_gain), (norm_gain_in, norm_gain_v),
    )
    in_copies = [pltpu.make_async_copy(src, dst, in_s.at[i]) for i, (src, dst) in enumerate(pairs)]
    w_copies = [
        pltpu.make_async_copy(w_hbm, wraw, w_s.at[0]),
        pltpu.make_async_copy(wo_hbm, wo, w_s.at[1]),
        pltpu.make_async_copy(wout_hbm, wout, w_s.at[2]),
    ]
    for cp in in_copies + w_copies:
        cp.start()
    for cp in in_copies:
        cp.wait()

    for src, dst in ((pre_gain_v, pre_gain), (offset_x_v, offset_x), (norm_gain_v, norm_gain)):
        for i in range(src.shape[0]):
            dst[0:1, i * Q : (i + 1) * Q] = src[i : i + 1, :]

    for half in range(2):
        tk = tokens[half * HALF : (half + 1) * HALF, :].astype(F32)
        inv = lax.rsqrt(jnp.mean(tk * tk, axis=1, keepdims=True) + NORM_FLOOR)
        rows[h, half] = (tk * inv * pre_gain[...]).astype(BF16)

    pl.semaphore_wait(barrier, 19)

    def ag(origin, half, role, device):
        return remote(
            rows.at[origin, half], rows.at[origin, half], ag_s.at[role], ag_r.at[role], (s, device)
        )

    own_pair = remote(rows.at[h], rows.at[h], ag_s.at[6], ag_r.at[6], (s, partner))
    sends = [ag(h, 0, 0, hr), ag(h, 1, 3, hl), ag(h, 1, 1, hr), ag(h, 0, 2, hl)]
    own_pair.start()
    for cp in sends:
        cp.start()

    li = lax.broadcasted_iota(jnp.int32, (2 * Q, DL), 0)
    lc = lax.broadcasted_iota(jnp.int32, (2 * Q, DL), 1)
    head_of = lax.shift_right_logical(lc, 6)
    expand[...] = jnp.where(jnp.bitwise_and(li, Q - 1) == head_of, 1.0, 0.0).astype(BF16)
    small[...] = jnp.zeros_like(small)
    small[0:1, 0:HEADS] = dt_bias[...]
    small[1:2, 0:HEADS] = a_log[...]
    small[2:3, 0:HEADS] = skip_gain[...]
    dtr[...] = jnp.zeros_like(dtr)
    for cp in w_copies:
        cp.wait()

    pick_r = lax.broadcasted_iota(jnp.int32, (2 * Q, 2 * Q), 0)
    pick_c = lax.broadcasted_iota(jnp.int32, (2 * Q, 2 * Q), 1)
    pick_t = jnp.where(pick_r < Q, 2 * pick_r, 2 * (pick_r - Q) + 1)
    pick = jnp.where(pick_c == pick_t, 1.0, 0.0).astype(BF16)
    wflat = wraw.reshape(2 * D, DL)

    def split_step(i, carry):
        v = wflat[pl.ds(pl.multiple_of(i * 2 * Q, 2 * Q), 2 * Q), :]
        r = dot(pick, v).astype(BF16)
        w[0, pl.ds(pl.multiple_of(i * Q, Q), Q), :] = r[0:Q, :]
        w[1, pl.ds(pl.multiple_of(i * Q, Q), Q), :] = r[Q : 2 * Q, :]
        return carry

    lax.fori_loop(0, D // Q, split_step, 0)

    def put_rows(n, places):
        xv = dot(n, w[1]).astype(BF16).astype(F32)
        bv = dot_t(n, wo[0 : 2 * NS, :]).astype(BF16).astype(F32)
        dv = dot_t(n, wo[2 * NS : 2 * NS + 80, :])
        for at, lo, hi in places:
            xin[pl.ds(pl.multiple_of(at + 8, 8), hi - lo), 0:DL] = xv[lo:hi, :]
            xin[pl.ds(pl.multiple_of(at + 8, 8), hi - lo), DL : DL + 2 * NS] = bv[lo:hi, :]
            dtr[pl.ds(pl.multiple_of(at, 8), hi - lo), 0:80] = dv[lo:hi, :]

    def project_x(chip):
        n = rows[pl.ds(2 * chip, 2)].reshape(CH, D)
        put_rows(n, [(chip * CH, 0, CH)])

    def project_halves(chip_a, half_a, chip_b, half_b):
        n = jnp.concatenate(
            [rows[pl.ds(2 * chip_a, 2), half_a].reshape(R, D), rows[pl.ds(2 * chip_b, 2), half_b].reshape(R, D)],
            axis=0,
        )
        places = []
        for i, (chip, half) in enumerate(((chip_a, half_a), (chip_b, half_b))):
            for core in range(2):
                lo = i * R + core * HALF
                places.append((chip * CH + core * R + half * HALF, lo, lo + HALF))
        put_rows(n, places)

    def project_z(chip):
        n = rows[pl.ds(2 * chip, 2)].reshape(CH, D)
        zs[pl.ds(pl.multiple_of(chip * CH, CH), CH), :] = silu(dot(n, w[0]).astype(BF16).astype(F32))

    def to_partner(origin, half, role):
        cp = ag(origin, half, 7 + role, partner)
        cp.start()
        sends.append(cp)

    def partner_done(chip, half, role):
        ag(chip * 2 + 1 - c, half, 7 + role, partner).wait_recv()

    def onward(origin, half, role, device):
        cp = ag(origin, half, role, device)
        cp.start()
        sends.append(cp)

    lane = lax.broadcasted_iota(jnp.int32, (1, Q), 1)
    ri = lax.broadcasted_iota(jnp.int32, (Q, Q), 0)
    ci = lax.broadcasted_iota(jnp.int32, (Q, Q), 1)
    tri = jnp.where(ri >= ci, 1.0, 0.0).astype(BF16)
    shift = (Q - h * HEADS) % Q

    def step_sizes(q):
        raw = pltpu.roll(dtr[pl.ds(pl.multiple_of(q * Q, Q), Q), :], shift, 1) + small[0:1, :]
        step = jnp.maximum(raw, 0.0) + jnp.log1p(jnp.exp(-jnp.abs(raw)))
        step = jnp.where(lane < HEADS, step, 0.0)
        la = step * -jnp.exp(small[1:2, :])
        dts[q] = step
        p3 = dot(tri, jnp.concatenate(split3(la), axis=1))
        cum[q] = p3[:, 0:Q] + p3[:, Q : 2 * Q] + p3[:, 2 * Q : 3 * Q]

    def conv_block(i):
        at = pl.multiple_of(i * 64, 64)
        for lo, hi, kern, off in ((0, DL, kernel_x, offset_x), (DL, DL + 2 * NS, kernel_bc, offset_bc)):
            u = jnp.broadcast_to(off[...], (64, hi - lo))
            v = xin[pl.ds(at, 72), lo:hi]
            for k in range(4):
                u = u + kern[k : k + 1, :] * v[5 + k : 69 + k, :]
            v = silu(u).astype(BF16)
            if lo == 0:
                xb[pl.ds(at, 64), :] = v
            else:
                bmat[pl.ds(at, 64), :] = v[:, 0:NS]
                cmat[pl.ds(at, 64), :] = v[:, NS : 2 * NS]

    far = xo // 2
    near = 1 - far
    odd = xo % 2
    late = 3 * far + odd
    other = 3 * far + 2 - 2 * odd

    def conv_early(i, carry):
        chip = (x + 3 + i // 3) % NX
        block = 3 * chip + i % 3
        block = jnp.where(jnp.logical_or(block == 0, i == 0), block + 1, block)
        conv_block(block)
        return carry

    ag(hl, 0, 0, hr).wait_recv()
    onward(hl, 0, 4, hr)
    ag(hr, 1, 3, hl).wait_recv()
    onward(hr, 1, 5, hl)
    to_partner(hl, 0, 0)
    to_partner(hr, 1, 3)
    remote(rows.at[partner], rows.at[partner], ag_s.at[6], ag_r.at[6], (s, partner)).wait_recv()
    project_x(x)
    partner_done(xl, 0, 0)
    partner_done(xr, 1, 3)
    project_halves(xl, 0, xr, 1)
    ag(hl, 1, 1, hr).wait_recv()
    to_partner(hl, 1, 1)
    ag(hr, 0, 2, hl).wait_recv()
    to_partner(hr, 0, 2)
    lax.fori_loop(4, 6, conv_early, 0)
    partner_done(xl, 1, 1)
    partner_done(xr, 0, 2)
    project_halves(xl, 1, xr, 0)
    for q in (3 * near, 3 * near + 1, 3 * near + 2, other):
        step_sizes(q)

    lax.fori_loop(1, 4, conv_early, 0)
    ag(ho, 0, 4, hr).wait_recv()
    to_partner(ho, 0, 4)
    ag(ho, 1, 5, hl).wait_recv()
    to_partner(ho, 1, 5)
    put_rows(rows[ho].reshape(R, D), [(ho * R, 0, R)])
    lax.fori_loop(6, 9, conv_early, 0)
    partner_done(xo, 0, 4)
    partner_done(xo, 1, 5)
    hop = 2 * xo + 1 - c
    put_rows(rows[hop].reshape(R, D), [(hop * R, 0, R)])

    halo = remote(xin.at[pl.ds(T, 8)], xin.at[pl.ds(0, 8)], halo_s, halo_r, ((s + 1) % 32, h))

    @pl.when(s < 31)
    def _():
        halo.start()

    step_sizes(late)
    step_sizes(late + 1)
    total = cum[0][Q - 1 : Q, :]
    for q in range(1, NQ):
        total = total + cum[q][Q - 1 : Q, :]
    drow[...] = jnp.broadcast_to(jnp.exp(total), (8, Q))
    rd[z] = drow[...]

    def z_peer(k):
        return (z + k) % NZ

    for k in range(1, NZ):
        zp = z_peer(k)
        remote(drow, rd.at[z], zd_s.at[k], zd_r.at[z], (y * NZ + zp, h)).start()

    conv_block(3 * xo + 1)
    conv_block(3 * xo + 2)
    conv_block(jnp.where(xo == 0, 3 * xl, 3 * xo))
    conv_block(jnp.where(xl == 0, 3 * xo, 3 * xl))

    def chunk_state(q):
        cq = cum[q]
        fac = jnp.exp(cq[Q - 1 : Q, :] - cq) * dts[q]
        fx = dot(jnp.concatenate(split2(fac), axis=1), expand[...])
        ef[q] = dot(jnp.concatenate(split2(jnp.exp(cq)), axis=1), expand[...])
        xw = (xb[q * Q : (q + 1) * Q, :].astype(F32) * fx).astype(BF16)
        sl[q] = t_dot(bmat[q * Q : (q + 1) * Q, :], xw)

    for q in range(1, NQ):
        chunk_state(q)

    @pl.when(s == 0)
    def _():
        xin[0:8, :] = jnp.zeros((8, DL + 2 * NS), F32)

    @pl.when(s > 0)
    def _():
        halo.wait_recv()

    conv_block(0)
    chunk_state(0)

    for lo in range(0, DL, Q):
        acc = jnp.zeros((NS, Q), F32)
        pd = jnp.ones((1, Q), F32)
        for q in range(NQ):
            st = sl[q, :, lo : lo + Q]
            dec = ef[q, Q - 1 : Q, lo : lo + Q]
            sl[q, :, lo : lo + Q] = acc
            pdr[q, 0:1, lo : lo + Q] = pd
            acc = acc * dec + st
            pd = pd * dec
        sb[:, lo : lo + Q] = acc.astype(BF16)
    rz[z] = sb[pl.ds(pl.multiple_of(z * 16, 16), 16), :]

    far_first = (4, 3, 5, 2, 6, 1, 7)
    for k in far_first:
        zp = z_peer(k)
        remote(
            sb.at[pl.ds(pl.multiple_of(zp * 16, 16), 16)], rz.at[z], zs_s.at[k], zs_r.at[z],
            (y * NZ + zp, h),
        ).start()

    project_z(xo)
    s3 = jnp.concatenate(split2(jnp.broadcast_to(small[2:3, :], (8, Q))), axis=1)
    skip_row = dot(s3, expand[...])[0:1, :]
    low = lax.broadcasted_iota(jnp.int32, (Q, Q), 1) < 64

    def intra_step(q, carry):
        at = pl.multiple_of(q * Q, Q)
        cq = cum[q]
        cqt = jnp.transpose(cq)
        dtt = jnp.transpose(dts[q])
        cb = dot_t(cmat[pl.ds(at, Q), :], bmat[pl.ds(at, Q), :])
        cbm = jnp.where(ri >= ci, cb, 0.0)
        for j in range(HEADS // 2):
            mixes = []
            for hh in (2 * j, 2 * j + 1):
                gap = jnp.minimum(cq[:, hh : hh + 1] - cqt[hh : hh + 1, :], 0.0)
                mixes.append((cbm * jnp.exp(gap) * dtt[hh : hh + 1, :]).astype(BF16))
            xp = xb[pl.ds(at, Q), j * Q : (j + 1) * Q].astype(F32)
            xd = jnp.concatenate(
                [jnp.where(low, xp, 0.0).astype(BF16), jnp.where(low, 0.0, xp).astype(BF16)], axis=0
            )
            yq = dot(jnp.concatenate(mixes, axis=1), xd)
            yv[pl.ds(at, Q), j * Q : (j + 1) * Q] = yq + skip_row[:, j * Q : (j + 1) * Q] * xp
        return carry

    lax.fori_loop(0, NQ, intra_step, 0)

    for k in range(1, NZ):
        zp = z_peer(k)
        remote(drow, rd.at[zp], zd_s.at[k], zd_r.at[zp], (y * NZ + zp, h)).wait_recv()
        remote(sb.at[pl.ds(0, 16)], rz.at[zp], zs_s.at[k], zs_r.at[zp], (y * NZ + zp, h)).wait_recv()
    dz = jnp.concatenate([rd[k][0:1, :] for k in range(NZ)], axis=0)
    dx = dot(jnp.concatenate(split2(dz), axis=1), expand[...])
    acc = jnp.zeros((16, DL), F32)
    pd = jnp.ones((1, DL), F32)
    for k in range(NZ):
        pz[k] = acc
        pdz[k] = jnp.broadcast_to(pd, (8, DL))
        acc = acc * dx[k : k + 1, :] + rz[k].astype(F32)
        pd = pd * dx[k : k + 1, :]
    tb[...] = acc.astype(BF16)
    tdb[...] = jnp.broadcast_to(pd, (8, DL))

    for k in range(1, NY):
        @pl.when(y + k < NY)
        def _(k=k):
            dev = ((y + k) % NY * NZ + z, h)
            remote(tb, ty.at[y], y_s.at[k], y_r.at[y], dev).start()
            remote(tdb, tdy.at[y], yd_s.at[k], yd_r.at[y], dev).start()

    project_z(xl)
    project_z(x)
    cacc[...] = jnp.zeros_like(cacc)
    for k in range(NY - 1):
        @pl.when(k < y)
        def _(k=k):
            dev = (k * NZ + z, h)
            remote(tb, ty.at[k], y_s.at[1], y_r.at[k], dev).wait_recv()
            remote(tdb, tdy.at[k], yd_s.at[1], yd_r.at[k], dev).wait_recv()
            cacc[...] = cacc[...] * tdy[k][0:1, :] + ty[k].astype(F32)

    for k in range(NZ):
        pb[k] = (pz[k] + pdz[k][0:1, :] * cacc[...]).astype(BF16)
    cr[z] = pb[z]
    for k in far_first:
        zp = z_peer(k)
        remote(pb.at[zp], cr.at[z], bk_s.at[k], bk_r.at[z], (y * NZ + zp, h)).start()
    project_z(xr)
    for k in range(1, NZ):
        zp = z_peer(k)
        remote(pb.at[zp], cr.at[zp], bk_s.at[k], bk_r.at[zp], (y * NZ + zp, h)).wait_recv()

    def out_step(q, carry):
        at = pl.multiple_of(q * Q, Q)
        state = (sl[q] + pdr[q][0:1, :] * cr[...].reshape(NS, DL).astype(F32)).astype(BF16)
        cross = dot(cmat[pl.ds(at, Q), :], state)
        g = (yv[pl.ds(at, Q), :] + ef[q] * cross) * zs[pl.ds(at, Q), :]
        sqc[pl.ds(at, Q), :] = jnp.broadcast_to(jnp.sum(g * g, axis=1, keepdims=True), (Q, Q))
        gb[pl.ds(at, Q), :] = (g * norm_gain[...]).astype(BF16)
        return carry

    def pair_copy(d, lo, width, sem):
        return remote(
            part.at[2 * d + 1 - c, :, :, pl.ds(lo, width)], pr.at[d, :, :, pl.ds(lo, width)],
            pp_s.at[sem], pp_r.at[sem], (s, partner),
        )

    def out_part(d, lo, width, sem):
        n = gb[pl.ds(pl.multiple_of(d * CH, CH), CH), :]
        for at in range(lo, lo + width, 256):
            part[pl.ds(2 * d, 2), :, :, at : at + 256] = (
                dot(n, wout[:, at : at + 256]).astype(BF16).reshape(2, 2, HALF, 256)
            )
        pair_copy(d, lo, width, sem).start()

    def out_chip(d):
        out_part(d, 0, D, d)

    def pair_sum(d, half):
        return part[2 * d + c, half].astype(F32) + pr[d, half].astype(F32)

    def pair_wait(d):
        remote(part.at[0], pr.at[d], pp_s.at[d], pp_r.at[d], (s, partner)).wait_recv()

    d1 = xo + 1 - 2 * (xo % 2)
    d2 = x + 1 - 2 * (x % 2)
    out_step(late, 0)
    out_step(late + 1, 0)
    cols = D // 2

    def relay_copy(half, i):
        here = pl.ds(i * cols, cols)
        return remote(
            ps.at[0, half, :, here], rl.at[half, :, here], rl_s.at[half, i], rl_r.at[half, i],
            (s, hl if half else hr),
        )

    def relay(i):
        here = pl.ds(i * cols, cols)
        pair_copy(xo, i * cols, cols, 4 + i).wait_recv()
        for half in range(2):
            ps[0, half, :, here] = (
                part[2 * xo + c, half, :, here].astype(F32) + pr[xo, half, :, here].astype(F32)
            ).astype(BF16)
            relay_copy(half, i).start()

    @pl.when(c == 0)
    def _():
        for i in range(2):
            out_part(xo, i * cols, cols, 4 + i)
            relay(i)
        out_step(other, 0)
        out_chip(d1)

    @pl.when(c == 1)
    def _():
        for i in range(2):
            out_part(xo, i * cols, cols, 4 + i)
        out_step(other, 0)
        out_chip(d1)
        for i in range(2):
            relay(i)

    def side_of(d):
        return jnp.where(d == xr, 0, 1)

    finals = []

    def final_send(slot, d, half):
        side = side_of(d)
        cp = remote(
            ps.at[slot, half], rf.at[side, half], rf_s.at[side, half], rf_r.at[side, half], (s, 2 * d + c)
        )
        cp.start()
        finals.append(cp)

    def send_direct(slot, d):
        half = 1 - side_of(d)
        pair_wait(d)
        ps[slot, half] = pair_sum(d, half).astype(BF16)
        final_send(slot, d, half)

    def send_relayed(slot, d):
        half = side_of(d)
        for i in range(2):
            here = pl.ds(i * cols, cols)
            remote(
                ps.at[0, 0, :, here], rl.at[half, :, here], rl_s.at[half, i], rl_r.at[half, i], (s, hr)
            ).wait_recv()
        ps[slot, half] = (pair_sum(d, half) + rl[half].astype(F32)).astype(BF16)
        final_send(slot, d, half)

    send_direct(1, d1)
    lax.fori_loop(near * 3, near * 3 + 3, out_step, 0)
    out_chip(d2)
    send_direct(2, d2)
    send_relayed(1, d1)
    send_relayed(2, d2)
    out_chip(x)

    sq_sends = []
    for k in range(8):
        col = sqc[pl.ds(pl.multiple_of(((h + k) % 8) * R, 32), Q), :]
        sqs[(h + k) % 8] = jnp.transpose(col)[0:8, :]
        if k == 0:
            sqr[h] = sqs[h]
        else:
            cp = remote(sqs.at[(h + k) % 8], sqr.at[h], sq_s.at[k], sq_r.at[h], (s, (h + k) % 8))
            cp.start()
            sq_sends.append(cp)
    pair_wait(x)
    for k in range(1, 8):
        hk = (h + k) % 8
        remote(sqs.at[0], sqr.at[hk], sq_s.at[k], sq_r.at[hk], (s, hk)).wait_recv()
    squares = jnp.sum(sqr[...], axis=0)[0:1, :]
    inv_row = lax.rsqrt(squares / (DL * 8) + NORM_FLOOR)
    inv_col = jnp.transpose(jnp.broadcast_to(inv_row, (Q, Q)))
    for half in range(2):
        for side in range(2):
            remote(
                ps.at[1, half], rf.at[side, half], rf_s.at[side, half], rf_r.at[side, half], (s, hl)
            ).wait_recv()
    for half in range(2):
        tot = pair_sum(x, half) + rf[0, half].astype(F32) + rf[1, half].astype(F32)
        out[half * HALF : (half + 1) * HALF, :] = (
            tot * inv_col[half * HALF : (half + 1) * HALF, 0:1]
        ).astype(BF16)

    own_pair.wait_send()
    for cp in sends + finals + sq_sends:
        cp.wait_send()
    for i in range(2):
        pair_copy(xo, i * cols, cols, 4 + i).wait_send()
        for half in range(2):
            relay_copy(half, i).wait_send()
    for d in (d1, d2, x):
        pair_copy(d, 0, D, d).wait_send()

    @pl.when(s < 31)
    def _():
        halo.wait_send()

    for k in range(1, NZ):
        zp = z_peer(k)
        dev = (y * NZ + zp, h)
        remote(drow, rd.at[z], zd_s.at[k], zd_r.at[z], dev).wait_send()
        remote(sb.at[pl.ds(0, 16)], rz.at[z], zs_s.at[k], zs_r.at[z], dev).wait_send()
        remote(pb.at[zp], cr.at[z], bk_s.at[k], bk_r.at[z], dev).wait_send()
    for k in range(1, NY):
        @pl.when(y + k < NY)
        def _(k=k):
            dev = ((y + k) % NY * NZ + z, h)
            remote(tb, ty.at[y], y_s.at[k], y_r.at[y], dev).wait_send()
            remote(tdb, tdy.at[y], yd_s.at[k], yd_r.at[y], dev).wait_send()


def on_device(
    tokens, pre_gain, inner_proj, outer_proj, kernel_x, kernel_bc, offset_x, offset_bc, dt_bias, a_log,
    skip_gain, norm_gain, out_proj,
):
    vm = pl.BlockSpec(memory_space=pltpu.VMEM)
    hbm = pl.BlockSpec(memory_space=pltpu.HBM)
    dma = pltpu.SemaphoreType.DMA
    V = pltpu.VMEM
    scratch = [
        V((R, D), BF16), V((D // Q, Q), F32), V((4, DL), F32), V((4, 2 * NS), F32), V((DL // Q, Q), F32),
        V((1, 2 * NS), F32), V((1, HEADS), F32), V((1, HEADS), F32), V((1, HEADS), F32), V((DL // Q, Q), F32),
        V((D, 2, DL), BF16), V((2, D, DL), BF16), V((336, D), BF16), V((DL, D), BF16), V((8, 2, HALF, D), BF16),
        V((T + 8, DL + 2 * NS), F32), V((T, Q), F32), V((T, DL), F32), V((T, DL), BF16),
        V((T, NS), BF16), V((T, NS), BF16), V((NQ, Q, Q), F32), V((NQ, Q, Q), F32),
        V((2 * Q, DL), BF16), V((NQ, Q, DL), F32), V((NQ, NS, DL), F32),
        V((NQ, 8, DL), F32),
        V((T, DL), F32), V((NS, DL), BF16), V((8, Q), F32), V((NZ, 16, DL), BF16), V((NZ, 8, Q), F32),
        V((NZ, 16, DL), F32), V((NZ, 8, DL), F32), V((16, DL), BF16), V((8, DL), F32),
        V((NY, 16, DL), BF16), V((NY, 8, DL), F32), V((16, DL), F32), V((NZ, 16, DL), BF16),
        V((NZ, 16, DL), BF16), V((T, DL), BF16), V((T + 32, Q), F32), V((8, 2, HALF, D), BF16),
        V((NX, 2, HALF, D), BF16), V((3, 2, HALF, D), BF16), V((2, HALF, D), BF16), V((2, 2, HALF, D), BF16),
        V((8, 8, Q), F32), V((8, 8, Q), F32), V((8, Q), F32), V((1, D), F32), V((1, DL), F32),
        V((1, DL), F32),
        dma((13,)), dma((13,)), dma, dma, dma((NZ,)), dma((NZ,)), dma((NZ,)), dma((NZ,)),
        dma((NY,)), dma((NY,)), dma((NY,)), dma((NY,)), dma((NZ,)), dma((NZ,)),
        dma((6,)), dma((6,)), dma((2, 2)), dma((2, 2)), dma((2, 2)), dma((2, 2)), dma((8,)), dma((8,)),
        dma((3,)), dma((10,)),
    ]
    args = (
        tokens, pre_gain.reshape(D // Q, Q), inner_proj, outer_proj.T, kernel_x, kernel_bc,
        offset_x.reshape(DL // Q, Q), offset_bc[None], dt_bias[None], a_log[None], skip_gain[None],
        norm_gain.reshape(DL // Q, Q), out_proj,
    )
    args = [pltpu.with_memory_space_constraint(v, pltpu.HBM) for v in args]
    return pl.pallas_call(
        kernel,
        out_shape=jax.ShapeDtypeStruct((R, D), BF16),
        in_specs=[hbm] * 13,
        out_specs=vm,
        scratch_shapes=scratch,
        compiler_params=pltpu.CompilerParams(
            collective_id=0, has_side_effects=True, vmem_limit_bytes=56_000_000
        ),
    )(*args)


def solution(mesh):
    in_specs = (
        P(("seq", "head"), None), P(), P(None, None, "head"), P(), P(None, "head"), P(), P("head"), P(),
        P("head"), P("head"), P("head"), P("head"), P("head", None),
    )
    return jax.shard_map(
        on_device, mesh=mesh, in_specs=in_specs, out_specs=P(("seq", "head"), None), check_vma=False
    )
```

```python
import jax
import jax.numpy as jnp
from jax import lax
from jax.experimental import pallas as pl
from jax.experimental.pallas import tpu as pltpu
from jax.sharding import PartitionSpec as P

MESH = pl.DeviceIdType.MESH
BF16 = jnp.bfloat16
F32 = jnp.float32

NORM_FLOOR = 0.1
D = 2560
DL = 640
NS = 128
R = 96
HALF = 48
T = 768
Q = 128
NQ = 6
CH = 192
HEADS = 10
NY, NZ, NX = 4, 8, 4


def dot(a, b):
    return jnp.dot(a, b, preferred_element_type=F32)


def dot_t(a, b):
    return lax.dot_general(a, b, (((1,), (1,)), ((), ())), preferred_element_type=F32)


def t_dot(a, b):
    return lax.dot_general(a, b, (((0,), (0,)), ((), ())), preferred_element_type=F32)


def split2(v):
    hi = v.astype(BF16)
    lo = (v - hi.astype(F32)).astype(BF16)
    return hi, lo


def split3(v):
    hi, mid = split2(v)
    lo = (v - hi.astype(F32) - mid.astype(F32)).astype(BF16)
    return hi, mid, lo


def silu(v):
    half = 0.5 * v
    return half + half * jnp.tanh(half)


def remote(src, dst, send, recv, device):
    return pltpu.make_async_remote_copy(
        src_ref=src, dst_ref=dst, send_sem=send, recv_sem=recv, device_id=device, device_id_type=MESH
    )


def kernel(
    tokens_in, pre_gain_in, w_hbm, wo_hbm, kernel_x_in, kernel_bc_in, offset_x_in, offset_bc_in, dt_bias_in,
    a_log_in, skip_gain_in, norm_gain_in, wout_hbm,
    out,
    tokens, pre_gain_v, kernel_x, kernel_bc, offset_x_v, offset_bc, dt_bias, a_log, skip_gain, norm_gain_v,
    wraw, wz, wx, wo, wout, rows, xin, dtr, zs, xb, bmat, cmat, dts, cum, expand, ef, sl, pdr,
    yv, sb, drow, rz, rd, pz, pdz, tb, tdb, ty, tdy, cacc, pb, cr, gb, sqc, part, pr, ps, rl, rf,
    sqs, sqr, small, pre_gain, offset_x, norm_gain, tot,
    ag_s, ag_r, halo_s, halo_r, zs_s, zs_r, zd_s, zd_r, y_s, y_r, yd_s, yd_r, bk_s, bk_r,
    pp_s, pp_r, rl_s, rl_r, rf_s, rf_r, sq_s, sq_r, w_s, in_s,
):
    s = lax.axis_index("seq")
    h = lax.axis_index("head")
    y = s // NZ
    z = s % NZ
    x = h // 2
    c = h % 2
    partner = x * 2 + (1 - c)
    xr = (x + 1) % NX
    xl = (x + NX - 1) % NX
    xo = (x + 2) % NX
    hr, hl, ho = xr * 2 + c, xl * 2 + c, xo * 2 + c

    barrier = pltpu.get_barrier_semaphore()
    for k in range(1, 8):
        pl.semaphore_signal(barrier, inc=1, device_id=(s, (h + k) % 8), device_id_type=MESH)
    for k in range(1, NZ):
        pl.semaphore_signal(barrier, inc=1, device_id=(y * NZ + (z + k) % NZ, h), device_id_type=MESH)
    for k in range(1, NY):
        pl.semaphore_signal(barrier, inc=1, device_id=(((y + k) % NY) * NZ + z, h), device_id_type=MESH)
    for k in (1, 31):
        pl.semaphore_signal(barrier, inc=1, device_id=((s + k) % 32, h), device_id_type=MESH)

    pairs = (
        (tokens_in, tokens), (pre_gain_in, pre_gain_v), (kernel_x_in, kernel_x), (kernel_bc_in, kernel_bc),
        (offset_x_in, offset_x_v), (offset_bc_in, offset_bc), (dt_bias_in, dt_bias), (a_log_in, a_log),
        (skip_gain_in, skip_gain), (norm_gain_in, norm_gain_v),
    )
    in_copies = [pltpu.make_async_copy(src, dst, in_s.at[i]) for i, (src, dst) in enumerate(pairs)]
    quarter = D // 4
    w_copies = [
        pltpu.make_async_copy(
            w_hbm.at[pl.ds(i * quarter, quarter)], wraw.at[pl.ds(i * quarter, quarter)], w_s.at[i]
        )
        for i in range(4)
    ]
    late_copies = [
        pltpu.make_async_copy(wo_hbm, wo.at[pl.ds(0, 336)], w_s.at[4]),
        pltpu.make_async_copy(wout_hbm, wout, w_s.at[5]),
    ]
    for cp in in_copies[0:2]:
        cp.start()
    for cp in in_copies[2:]:
        cp.start()
    for cp in in_copies[0:2]:
        cp.wait()
    for cp in w_copies:
        cp.start()

    def as_row(src, dst):
        for i in range(src.shape[0]):
            dst[0:1, i * Q : (i + 1) * Q] = src[i : i + 1, :]

    as_row(pre_gain_v, pre_gain)

    for half in range(2):
        tk = tokens[half * HALF : (half + 1) * HALF, :].astype(F32)
        inv = lax.rsqrt(jnp.mean(tk * tk, axis=1, keepdims=True) + NORM_FLOOR)
        rows[h, half] = (tk * inv * pre_gain[...]).astype(BF16)

    pl.semaphore_wait(barrier, 19)

    def ag(origin, half, role, device):
        return remote(
            rows.at[origin, half], rows.at[origin, half], ag_s.at[role], ag_r.at[role], (s, device)
        )

    own_pair = remote(rows.at[h], rows.at[h], ag_s.at[6], ag_r.at[6], (s, partner))
    sends = [ag(h, 0, 0, hr), ag(h, 1, 3, hl), ag(h, 1, 1, hr), ag(h, 0, 2, hl)]
    own_pair.start()
    for cp in sends:
        cp.start()

    for cp in late_copies:
        cp.start()
    for cp in in_copies[2:]:
        cp.wait()
    as_row(offset_x_v, offset_x)
    as_row(norm_gain_v, norm_gain)

    li = lax.broadcasted_iota(jnp.int32, (2 * Q, DL), 0)
    lc = lax.broadcasted_iota(jnp.int32, (2 * Q, DL), 1)
    head_of = lax.shift_right_logical(lc, 6)
    expand[...] = jnp.where(jnp.bitwise_and(li, Q - 1) == head_of, 1.0, 0.0).astype(BF16)
    small[...] = jnp.zeros_like(small)
    small[0:1, 0:HEADS] = dt_bias[...]
    small[1:2, 0:HEADS] = a_log[...]
    small[2:3, 0:HEADS] = skip_gain[...]
    pick_r = lax.broadcasted_iota(jnp.int32, (2 * Q, 2 * Q), 0)
    pick_c = lax.broadcasted_iota(jnp.int32, (2 * Q, 2 * Q), 1)
    pick_t = jnp.where(pick_r < Q, 2 * pick_r, 2 * (pick_r - Q) + 1)
    pick = jnp.where(pick_c == pick_t, 1.0, 0.0).astype(BF16)
    wflat = wraw.reshape(2 * D, DL)

    def split_step(i, carry):
        v = wflat[pl.ds(pl.multiple_of(i * 2 * Q, 2 * Q), 2 * Q), :]
        r = dot(pick, v).astype(BF16)
        wz[pl.ds(pl.multiple_of(i * Q, Q), Q), :] = r[0:Q, :]
        wx[pl.ds(pl.multiple_of(i * Q, Q), Q), 0:DL] = r[Q : 2 * Q, :]
        return carry

    for i in range(4):
        w_copies[i].wait()
        lax.fori_loop(i * quarter // Q, (i + 1) * quarter // Q, split_step, 0)
    for cp in late_copies:
        cp.wait()

    wo[336:384, :] = jnp.zeros((48, D), BF16)
    same = jnp.where(pick_r == pick_c, 1.0, 0.0).astype(BF16)
    for i in range(D // (2 * Q)):
        at = slice(i * 2 * Q, (i + 1) * 2 * Q)
        wx[at, DL:] = dot_t(same, wo[:, at]).astype(BF16)

    def put_rows(n, places):
        r = dot(n, wx[...])
        for at, lo, hi in places:
            xin[pl.ds(pl.multiple_of(at + 8, 8), hi - lo), :] = r[lo:hi, 0 : DL + 2 * NS].astype(BF16).astype(F32)
            dtr[pl.ds(pl.multiple_of(at, 8), hi - lo), :] = r[lo:hi, DL + 2 * NS :]

    def project_x(chip):
        n = rows[pl.ds(2 * chip, 2)].reshape(CH, D)
        put_rows(n, [(chip * CH, 0, CH)])

    def project_halves(chip_a, half_a, chip_b, half_b):
        n = jnp.concatenate(
            [rows[pl.ds(2 * chip_a, 2), half_a].reshape(R, D), rows[pl.ds(2 * chip_b, 2), half_b].reshape(R, D)],
            axis=0,
        )
        places = []
        for i, (chip, half) in enumerate(((chip_a, half_a), (chip_b, half_b))):
            for core in range(2):
                lo = i * R + core * HALF
                places.append((chip * CH + core * R + half * HALF, lo, lo + HALF))
        put_rows(n, places)

    def project_z(chip):
        n = rows[pl.ds(2 * chip, 2)].reshape(CH, D)
        zs[pl.ds(pl.multiple_of(chip * CH, CH), CH), :] = silu(dot(n, wz[...]).astype(BF16).astype(F32))

    def to_partner(origin, half, role):
        cp = ag(origin, half, 7 + role, partner)
        cp.start()
        sends.append(cp)

    def partner_done(chip, half, role):
        ag(chip * 2 + 1 - c, half, 7 + role, partner).wait_recv()

    def onward(origin, half, role, device):
        cp = ag(origin, half, role, device)
        cp.start()
        sends.append(cp)

    lane = lax.broadcasted_iota(jnp.int32, (1, Q), 1)
    ri = lax.broadcasted_iota(jnp.int32, (Q, Q), 0)
    ci = lax.broadcasted_iota(jnp.int32, (Q, Q), 1)
    tri = jnp.where(ri >= ci, 1.0, 0.0).astype(BF16)
    shift = (Q - h * HEADS) % Q

    def step_sizes(q):
        raw = pltpu.roll(dtr[pl.ds(pl.multiple_of(q * Q, Q), Q), :], shift, 1) + small[0:1, :]
        step = jnp.maximum(raw, 0.0) + jnp.log1p(jnp.exp(-jnp.abs(raw)))
        step = jnp.where(lane < HEADS, step, 0.0)
        la = step * -jnp.exp(small[1:2, :])
        dts[q] = step
        p3 = dot(tri, jnp.concatenate(split3(la), axis=1))
        cum[q] = p3[:, 0:Q] + p3[:, Q : 2 * Q] + p3[:, 2 * Q : 3 * Q]

    def conv_block(i):
        at = pl.multiple_of(i * 64, 64)
        for j in range((DL + 2 * NS) // Q):
            kern, off, lo = (kernel_x, offset_x, j * Q) if j < 5 else (kernel_bc, offset_bc, (j - 5) * Q)
            v = xin[pl.ds(at, 72), j * Q : (j + 1) * Q]
            u = kern[0:1, lo : lo + Q] * v
            for k in range(1, 4):
                u = pltpu.roll(u, 1, 0) + kern[k : k + 1, lo : lo + Q] * v
            v = silu(u[8:72, :] + off[:, lo : lo + Q]).astype(BF16)
            if j < 5:
                xb[pl.ds(at, 64), lo : lo + Q] = v
            else:
                (bmat, cmat)[j - 5][pl.ds(at, 64), :] = v

    def chunk_state(q):
        at = pl.multiple_of(q * Q, Q)
        cq = cum[q]
        fac = jnp.exp(cq[Q - 1 : Q, :] - cq) * dts[q]
        fx = dot(jnp.concatenate(split2(fac), axis=1), expand[...])
        xw = (xb[pl.ds(at, Q), :].astype(F32) * fx).astype(BF16)
        sl[q] = t_dot(bmat[pl.ds(at, Q), :], xw)

    far = xo // 2
    near = 1 - far
    odd = xo % 2
    late = 3 * far + odd
    other = 3 * far + 2 - 2 * odd

    def conv_early(i, carry):
        chip = (x + 3 + i // 3) % NX
        block = 3 * chip + i % 3
        block = jnp.where(jnp.logical_or(block == 0, i == 0), block + 1, block)
        conv_block(block)
        return carry

    remote(rows.at[partner], rows.at[partner], ag_s.at[6], ag_r.at[6], (s, partner)).wait_recv()
    ag(hl, 0, 0, hr).wait_recv()
    onward(hl, 0, 4, hr)
    ag(hr, 1, 3, hl).wait_recv()
    onward(hr, 1, 5, hl)
    to_partner(hl, 0, 0)
    to_partner(hr, 1, 3)
    project_x(x)
    partner_done(xl, 0, 0)
    partner_done(xr, 1, 3)
    project_halves(xl, 0, xr, 1)
    ag(hl, 1, 1, hr).wait_recv()
    to_partner(hl, 1, 1)
    ag(hr, 0, 2, hl).wait_recv()
    to_partner(hr, 0, 2)

    @pl.when(c == 0)
    def _():
        partner_done(xl, 1, 1)
        partner_done(xr, 0, 2)

    def put_seconds(core):
        n = jnp.concatenate([rows[2 * xl + core, 1], rows[2 * xr + core, 0]], axis=0)
        put_rows(
            n,
            [(xl * CH + core * R + HALF, 0, HALF), (xr * CH + core * R, HALF, R)],
        )

    put_seconds(1)
    lax.fori_loop(4, 6, conv_early, 0)

    @pl.when(c == 1)
    def _():
        partner_done(xl, 1, 1)
        partner_done(xr, 0, 2)

    put_seconds(0)

    def opposite_in():
        ag(ho, 0, 4, hr).wait_recv()
        ag(ho, 0, 11, partner).start()
        ag(ho, 1, 5, hl).wait_recv()
        ag(ho, 1, 12, partner).start()

    @pl.when(c == 1)
    def _():
        opposite_in()

    for q in (3 * near, 3 * near + 1, 3 * near + 2, other):
        step_sizes(q)
    lax.fori_loop(1, 4, conv_early, 0)

    @pl.when(c == 0)
    def _():
        opposite_in()

    lax.fori_loop(6, 9, conv_early, 0)
    chunk_state(3 * near + 1)
    chunk_state(3 * near + 2)
    partner_done(xo, 0, 4)
    partner_done(xo, 1, 5)
    project_x(xo)

    halo = remote(xin.at[pl.ds(T, 8)], xin.at[pl.ds(0, 8)], halo_s, halo_r, ((s + 1) % 32, h))

    @pl.when(s < 31)
    def _():
        halo.start()

    step_sizes(late)
    step_sizes(late + 1)
    total = cum[0][Q - 1 : Q, :]
    for q in range(1, NQ):
        total = total + cum[q][Q - 1 : Q, :]
    drow[...] = jnp.broadcast_to(jnp.exp(total), (8, Q))
    rd[z] = drow[...]

    def z_peer(k):
        return (z + k) % NZ

    for k in range(1, NZ):
        zp = z_peer(k)
        remote(drow, rd.at[z], zd_s.at[k], zd_r.at[z], (y * NZ + zp, h)).start()

    conv_block(3 * xo + 1)
    conv_block(3 * xo + 2)
    conv_block(jnp.where(xo == 0, 3 * xl, 3 * xo))
    conv_block(jnp.where(xl == 0, 3 * xo, 3 * xl))

    rest = jnp.where(near == 0, 3, 1)
    for k in range(3):
        chunk_state(rest + k)

    @pl.when(s == 0)
    def _():
        xin[0:8, :] = jnp.zeros((8, DL + 2 * NS), F32)

    @pl.when(s > 0)
    def _():
        halo.wait_recv()

    conv_block(0)
    chunk_state(0)

    ends = jnp.concatenate([cum[q][Q - 1 : Q, :] for q in range(NQ)] + [jnp.zeros((2, Q), F32)], axis=0)
    decs = dot(jnp.concatenate(split2(jnp.exp(ends)), axis=1), expand[...])
    for lo in range(0, DL, Q):
        acc = jnp.zeros((NS, Q), F32)
        pd = jnp.ones((1, Q), F32)
        for q in range(NQ):
            st = sl[q, :, lo : lo + Q]
            dec = decs[q : q + 1, lo : lo + Q]
            sl[q, :, lo : lo + Q] = acc
            pdr[q, 0:1, lo : lo + Q] = pd
            acc = acc * dec + st
            pd = pd * dec
        sb[:, lo : lo + Q] = acc.astype(BF16)
    rz[z] = sb[pl.ds(pl.multiple_of(z * 16, 16), 16), :]

    far_first = (4, 3, 5, 2, 6, 1, 7)
    for k in far_first:
        zp = z_peer(k)
        remote(
            sb.at[pl.ds(pl.multiple_of(zp * 16, 16), 16)], rz.at[z], zs_s.at[k], zs_r.at[z],
            (y * NZ + zp, h),
        ).start()

    project_z(xo)
    s3 = jnp.concatenate(split2(jnp.broadcast_to(small[2:3, :], (8, Q))), axis=1)
    skip_row = dot(s3, expand[...])[0:1, :]
    low = lax.broadcasted_iota(jnp.int32, (Q, Q), 1) < 64

    def intra_step(q, carry):
        at = pl.multiple_of(q * Q, Q)
        cq = cum[q]
        ef[q] = dot(jnp.concatenate(split2(jnp.exp(cq)), axis=1), expand[...])
        cqt = jnp.transpose(cq)
        dtt = jnp.transpose(dts[q])
        cb = dot_t(cmat[pl.ds(at, Q), :], bmat[pl.ds(at, Q), :])
        cbm = jnp.where(ri >= ci, cb, 0.0)
        for j in range(HEADS // 2):
            mixes = []
            for hh in (2 * j, 2 * j + 1):
                gap = jnp.minimum(cq[:, hh : hh + 1] - cqt[hh : hh + 1, :], 0.0)
                mixes.append((cbm * jnp.exp(gap) * dtt[hh : hh + 1, :]).astype(BF16))
            xp = xb[pl.ds(at, Q), j * Q : (j + 1) * Q].astype(F32)
            xd = jnp.concatenate(
                [jnp.where(low, xp, 0.0).astype(BF16), jnp.where(low, 0.0, xp).astype(BF16)], axis=0
            )
            yq = dot(jnp.concatenate(mixes, axis=1), xd)
            yv[pl.ds(at, Q), j * Q : (j + 1) * Q] = yq + skip_row[:, j * Q : (j + 1) * Q] * xp
        return carry

    lax.fori_loop(0, NQ, intra_step, 0)

    for k in range(1, NZ):
        zp = z_peer(k)
        remote(drow, rd.at[zp], zd_s.at[k], zd_r.at[zp], (y * NZ + zp, h)).wait_recv()
        remote(sb.at[pl.ds(0, 16)], rz.at[zp], zs_s.at[k], zs_r.at[zp], (y * NZ + zp, h)).wait_recv()
    dz = jnp.concatenate([rd[k][0:1, :] for k in range(NZ)], axis=0)
    dx = dot(jnp.concatenate(split2(dz), axis=1), expand[...])
    acc = jnp.zeros((16, DL), F32)
    pd = jnp.ones((1, DL), F32)
    for k in range(NZ):
        pz[k] = acc
        pdz[k] = jnp.broadcast_to(pd, (8, DL))
        acc = acc * dx[k : k + 1, :] + rz[k].astype(F32)
        pd = pd * dx[k : k + 1, :]
    tb[...] = acc.astype(BF16)
    tdb[...] = jnp.broadcast_to(pd, (8, DL))

    for k in range(1, NY):
        @pl.when(y + k < NY)
        def _(k=k):
            dev = ((y + k) % NY * NZ + z, h)
            remote(tb, ty.at[y], y_s.at[k], y_r.at[y], dev).start()
            remote(tdb, tdy.at[y], yd_s.at[k], yd_r.at[y], dev).start()

    project_z(xl)
    project_z(x)
    cacc[...] = jnp.zeros_like(cacc)
    for k in range(NY - 1):
        @pl.when(k < y)
        def _(k=k):
            dev = (k * NZ + z, h)
            remote(tb, ty.at[k], y_s.at[1], y_r.at[k], dev).wait_recv()
            remote(tdb, tdy.at[k], yd_s.at[1], yd_r.at[k], dev).wait_recv()
            cacc[...] = cacc[...] * tdy[k][0:1, :] + ty[k].astype(F32)

    for k in range(NZ):
        pb[k] = (pz[k] + pdz[k][0:1, :] * cacc[...]).astype(BF16)
    cr[z] = pb[z]
    for k in far_first:
        zp = z_peer(k)
        remote(pb.at[zp], cr.at[z], bk_s.at[k], bk_r.at[z], (y * NZ + zp, h)).start()
    project_z(xr)
    for k in range(1, NZ):
        zp = z_peer(k)
        remote(pb.at[zp], cr.at[zp], bk_s.at[k], bk_r.at[zp], (y * NZ + zp, h)).wait_recv()

    def out_step(q, carry):
        at = pl.multiple_of(q * Q, Q)
        state = (sl[q] + pdr[q][0:1, :] * cr[...].reshape(NS, DL).astype(F32)).astype(BF16)
        cross = dot(cmat[pl.ds(at, Q), :], state)
        g = (yv[pl.ds(at, Q), :] + ef[q] * cross) * zs[pl.ds(at, Q), :]
        sqc[pl.ds(at, Q), :] = jnp.broadcast_to(jnp.sum(g * g, axis=1, keepdims=True), (Q, Q))
        gb[pl.ds(at, Q), :] = (g * norm_gain[...]).astype(BF16)
        return carry

    def pair_copy(d, lo, width, sem):
        return remote(
            part.at[2 * d + 1 - c, :, :, pl.ds(lo, width)], pr.at[d, :, :, pl.ds(lo, width)],
            pp_s.at[sem], pp_r.at[sem], (s, partner),
        )

    def out_part(d, lo, width, sem):
        n = gb[pl.ds(pl.multiple_of(d * CH, CH), CH), :]
        for at in range(lo, lo + width, 256):
            end = min(at + 256, lo + width)
            part[pl.ds(2 * d, 2), :, :, at:end] = (
                dot(n, wout[:, at:end]).astype(BF16).reshape(2, 2, HALF, end - at)
            )
        pair_copy(d, lo, width, sem).start()

    def out_chip(d):
        out_part(d, 0, D, d)

    def pair_sum(d, half):
        return part[2 * d + c, half].astype(F32) + pr[d, half].astype(F32)

    def pair_wait(d):
        remote(part.at[0], pr.at[d], pp_s.at[d], pp_r.at[d], (s, partner)).wait_recv()

    d1 = xo + 1 - 2 * (xo % 2)
    d2 = x + 1 - 2 * (x % 2)
    out_step(late, 0)
    out_step(late + 1, 0)
    cuts = ((0, 512), (512, 896), (1408, 1152))
    pieces = len(cuts)

    def relay_copy(half, i):
        here = pl.ds(*cuts[i])
        return remote(
            ps.at[0, half, :, here], rl.at[half, :, here], rl_s.at[half, i], rl_r.at[half, i],
            (s, hl if half else hr),
        )

    def relay(i):
        here = pl.ds(*cuts[i])
        pair_copy(xo, *cuts[i], 4 + i).wait_recv()
        for half in range(2):
            ps[0, half, :, here] = (
                part[2 * xo + c, half, :, here].astype(F32) + pr[xo, half, :, here].astype(F32)
            ).astype(BF16)
            relay_copy(half, i).start()

    @pl.when(c == 0)
    def _():
        for i in range(pieces):
            out_part(xo, *cuts[i], 4 + i)
            if i > 0:
                relay(i - 1)
        relay(pieces - 1)
        out_step(other, 0)
        out_chip(d1)

    @pl.when(c == 1)
    def _():
        for i in range(pieces):
            out_part(xo, *cuts[i], 4 + i)
        relay(0)
        out_step(other, 0)
        relay(1)
        out_chip(d1)
        relay(2)

    lax.fori_loop(near * 3, near * 3 + 3, out_step, 0)
    out_chip(d2)

    def side_of(d):
        return jnp.where(d == xr, 0, 1)

    finals = []

    def final_send(slot, d, half):
        side = side_of(d)
        cp = remote(
            ps.at[slot, half], rf.at[side, half], rf_s.at[side, half], rf_r.at[side, half], (s, 2 * d + c)
        )
        cp.start()
        finals.append(cp)

    def send_direct(slot, d):
        half = 1 - side_of(d)
        pair_wait(d)
        ps[slot, half] = pair_sum(d, half).astype(BF16)
        final_send(slot, d, half)

    def send_relayed(slot, d):
        half = side_of(d)
        for i in range(pieces):
            here = pl.ds(*cuts[i])
            remote(
                ps.at[0, 0, :, here], rl.at[half, :, here], rl_s.at[half, i], rl_r.at[half, i], (s, hr)
            ).wait_recv()
        ps[slot, half] = (pair_sum(d, half) + rl[half].astype(F32)).astype(BF16)
        final_send(slot, d, half)

    send_direct(1, d1)
    sq_sends = []
    for k in range(8):
        col = sqc[pl.ds(pl.multiple_of(((h + k) % 8) * R, 32), Q), :]
        sqs[(h + k) % 8] = jnp.transpose(col)[0:8, :]
        if k == 0:
            sqr[h] = sqs[h]
        else:
            cp = remote(sqs.at[(h + k) % 8], sqr.at[h], sq_s.at[k], sq_r.at[h], (s, (h + k) % 8))
            cp.start()
            sq_sends.append(cp)
    send_direct(2, d2)
    send_relayed(1, d1)
    send_relayed(2, d2)
    out_chip(x)

    pair_wait(x)

    def final_wait(side, half):
        remote(
            ps.at[1, half], rf.at[side, half], rf_s.at[side, half], rf_r.at[side, half], (s, hl)
        ).wait_recv()

    for half in range(2):
        final_wait(1 - half, half)
        tot[half] = pair_sum(x, half) + rf[1 - half, half].astype(F32)
    for k in range(1, 8):
        hk = (h + k) % 8
        remote(sqs.at[0], sqr.at[hk], sq_s.at[k], sq_r.at[hk], (s, hk)).wait_recv()
    squares = jnp.sum(sqr[...], axis=0)[0:1, :]
    inv_row = lax.rsqrt(squares / (DL * 8) + NORM_FLOOR)
    inv_col = jnp.transpose(jnp.broadcast_to(inv_row, (Q, Q)))
    for half in range(2):
        final_wait(half, half)
        out[half * HALF : (half + 1) * HALF, :] = (
            (tot[half] + rf[half, half].astype(F32)) * inv_col[half * HALF : (half + 1) * HALF, 0:1]
        ).astype(BF16)

    own_pair.wait_send()
    ag(ho, 0, 11, partner).wait_send()
    ag(ho, 1, 12, partner).wait_send()
    for cp in sends + finals + sq_sends:
        cp.wait_send()
    for i in range(pieces):
        pair_copy(xo, *cuts[i], 4 + i).wait_send()
        for half in range(2):
            relay_copy(half, i).wait_send()
    for d in (d1, d2, x):
        pair_copy(d, 0, D, d).wait_send()

    @pl.when(s < 31)
    def _():
        halo.wait_send()

    for k in range(1, NZ):
        zp = z_peer(k)
        dev = (y * NZ + zp, h)
        remote(drow, rd.at[z], zd_s.at[k], zd_r.at[z], dev).wait_send()
        remote(sb.at[pl.ds(0, 16)], rz.at[z], zs_s.at[k], zs_r.at[z], dev).wait_send()
        remote(pb.at[zp], cr.at[z], bk_s.at[k], bk_r.at[z], dev).wait_send()
    for k in range(1, NY):
        @pl.when(y + k < NY)
        def _(k=k):
            dev = ((y + k) % NY * NZ + z, h)
            remote(tb, ty.at[y], y_s.at[k], y_r.at[y], dev).wait_send()
            remote(tdb, tdy.at[y], yd_s.at[k], yd_r.at[y], dev).wait_send()


def on_device(
    tokens, pre_gain, inner_proj, outer_proj, kernel_x, kernel_bc, offset_x, offset_bc, dt_bias, a_log,
    skip_gain, norm_gain, out_proj,
):
    vm = pl.BlockSpec(memory_space=pltpu.VMEM)
    hbm = pl.BlockSpec(memory_space=pltpu.HBM)
    dma = pltpu.SemaphoreType.DMA
    V = pltpu.VMEM
    scratch = [
        V((R, D), BF16), V((D // Q, Q), F32), V((4, DL), F32), V((4, 2 * NS), F32), V((DL // Q, Q), F32),
        V((1, 2 * NS), F32), V((1, HEADS), F32), V((1, HEADS), F32), V((1, HEADS), F32), V((DL // Q, Q), F32),
        V((D, 2, DL), BF16), V((D, DL), BF16), V((D, 1024), BF16), V((384, D), BF16), V((DL, D), BF16), V((8, 2, HALF, D), BF16),
        V((T + 8, DL + 2 * NS), F32), V((T, Q), F32), V((T, DL), F32), V((T, DL), BF16),
        V((T, NS), BF16), V((T, NS), BF16), V((NQ, Q, Q), F32), V((NQ, Q, Q), F32),
        V((2 * Q, DL), BF16), V((NQ, Q, DL), F32), V((NQ, NS, DL), F32),
        V((NQ, 8, DL), F32),
        V((T, DL), F32), V((NS, DL), BF16), V((8, Q), F32), V((NZ, 16, DL), BF16), V((NZ, 8, Q), F32),
        V((NZ, 16, DL), F32), V((NZ, 8, DL), F32), V((16, DL), BF16), V((8, DL), F32),
        V((NY, 16, DL), BF16), V((NY, 8, DL), F32), V((16, DL), F32), V((NZ, 16, DL), BF16),
        V((NZ, 16, DL), BF16), V((T, DL), BF16), V((T + 32, Q), F32), V((8, 2, HALF, D), BF16),
        V((NX, 2, HALF, D), BF16), V((3, 2, HALF, D), BF16), V((2, HALF, D), BF16), V((2, 2, HALF, D), BF16),
        V((8, 8, Q), F32), V((8, 8, Q), F32), V((8, Q), F32), V((1, D), F32), V((1, DL), F32),
        V((1, DL), F32), V((2, HALF, D), F32),
        dma((13,)), dma((13,)), dma, dma, dma((NZ,)), dma((NZ,)), dma((NZ,)), dma((NZ,)),
        dma((NY,)), dma((NY,)), dma((NY,)), dma((NY,)), dma((NZ,)), dma((NZ,)),
        dma((7,)), dma((7,)), dma((2, 3)), dma((2, 3)), dma((2, 2)), dma((2, 2)), dma((8,)), dma((8,)),
        dma((6,)), dma((10,)),
    ]
    args = (
        tokens, pre_gain.reshape(D // Q, Q), inner_proj, outer_proj.T, kernel_x, kernel_bc,
        offset_x.reshape(DL // Q, Q), offset_bc[None], dt_bias[None], a_log[None], skip_gain[None],
        norm_gain.reshape(DL // Q, Q), out_proj,
    )
    args = [pltpu.with_memory_space_constraint(v, pltpu.HBM) for v in args]
    return pl.pallas_call(
        kernel,
        out_shape=jax.ShapeDtypeStruct((R, D), BF16),
        in_specs=[hbm] * 13,
        out_specs=vm,
        scratch_shapes=scratch,
        compiler_params=pltpu.CompilerParams(
            collective_id=0, has_side_effects=True, vmem_limit_bytes=55_000_000
        ),
    )(*args)


def solution(mesh):
    in_specs = (
        P(("seq", "head"), None), P(), P(None, None, "head"), P(), P(None, "head"), P(), P("head"), P(),
        P("head"), P("head"), P("head"), P("head"), P("head", None),
    )
    return jax.shard_map(
        on_device, mesh=mesh, in_specs=in_specs, out_specs=P(("seq", "head"), None), check_vma=False
    )
```

```python
import jax
import jax.numpy as jnp
from jax import lax
from jax.experimental import pallas as pl
from jax.experimental.pallas import tpu as pltpu
from jax.sharding import PartitionSpec as P

MESH = pl.DeviceIdType.MESH
BF16 = jnp.bfloat16
F32 = jnp.float32

NORM_FLOOR = 0.1
D = 2560
DL = 640
NS = 128
R = 96
HALF = 48
T = 768
Q = 128
NQ = 6
CH = 192
HEADS = 10
NY, NZ, NX = 4, 8, 4


def dot(a, b):
    return jnp.dot(a, b, preferred_element_type=F32)


def dot_t(a, b):
    return lax.dot_general(a, b, (((1,), (1,)), ((), ())), preferred_element_type=F32)


def t_dot(a, b):
    return lax.dot_general(a, b, (((0,), (0,)), ((), ())), preferred_element_type=F32)


def split2(v):
    hi = v.astype(BF16)
    lo = (v - hi.astype(F32)).astype(BF16)
    return hi, lo


def split3(v):
    hi, mid = split2(v)
    lo = (v - hi.astype(F32) - mid.astype(F32)).astype(BF16)
    return hi, mid, lo


def silu(v):
    half = 0.5 * v
    return half + half * jnp.tanh(half)


def remote(src, dst, send, recv, device):
    return pltpu.make_async_remote_copy(
        src_ref=src, dst_ref=dst, send_sem=send, recv_sem=recv, device_id=device, device_id_type=MESH
    )


def kernel(
    tokens_in, pre_gain_in, w_hbm, wo_hbm, kernel_x_in, kernel_bc_in, offset_x_in, offset_bc_in, dt_bias_in,
    a_log_in, skip_gain_in, norm_gain_in, wout_hbm,
    out,
    tokens, pre_gain_v, kernel_x, kernel_bc, offset_x_v, offset_bc, dt_bias, a_log, skip_gain, norm_gain_v,
    wraw, wz, wx, wo, wout, rows, xin, dtr, zs, xb, bmat, cmat, dts, cum, expand, ef, sl, sacc, pdr,
    yv, sb, drow, rz, rd, pz, pdz, tb, tdb, ty, tdy, cacc, pb, cr, gb, sqc, part, pr, ps, rl, rf,
    sqs, sqr, small, pre_gain, offset_x, norm_gain, tot,
    ag_s, ag_r, halo_s, halo_r, zs_s, zs_r, zd_s, zd_r, y_s, y_r, yd_s, yd_r, bk_s, bk_r,
    pp_s, pp_r, rl_s, rl_r, rf_s, rf_r, sq_s, sq_r, w_s, in_s,
):
    s = lax.axis_index("seq")
    h = lax.axis_index("head")
    y = s // NZ
    z = s % NZ
    x = h // 2
    c = h % 2
    partner = x * 2 + (1 - c)
    xr = (x + 1) % NX
    xl = (x + NX - 1) % NX
    xo = (x + 2) % NX
    hr, hl, ho = xr * 2 + c, xl * 2 + c, xo * 2 + c

    def await_bytes(like, sem):
        pltpu.make_async_copy(like, like, sem).wait()

    barrier = pltpu.get_barrier_semaphore()
    for k in range(1, 8):
        pl.semaphore_signal(barrier, inc=1, device_id=(s, (h + k) % 8), device_id_type=MESH)
    for k in range(1, NZ):
        pl.semaphore_signal(barrier, inc=1, device_id=(y * NZ + (z + k) % NZ, h), device_id_type=MESH)
    for k in range(1, NZ):
        pl.semaphore_signal(barrier, inc=1, device_id=(y * NZ + (z + k) % NZ, partner), device_id_type=MESH)
    for k in range(1, NY):
        pl.semaphore_signal(barrier, inc=1, device_id=(((y + k) % NY) * NZ + z, h), device_id_type=MESH)
    for k in (1, 31):
        pl.semaphore_signal(barrier, inc=1, device_id=((s + k) % 32, h), device_id_type=MESH)

    pairs = (
        (tokens_in, tokens), (pre_gain_in, pre_gain_v), (kernel_x_in, kernel_x), (kernel_bc_in, kernel_bc),
        (offset_x_in, offset_x_v), (offset_bc_in, offset_bc), (dt_bias_in, dt_bias), (a_log_in, a_log),
        (skip_gain_in, skip_gain), (norm_gain_in, norm_gain_v),
    )
    in_copies = [pltpu.make_async_copy(src, dst, in_s.at[i]) for i, (src, dst) in enumerate(pairs)]
    quarter = D // 4
    w_copies = [
        pltpu.make_async_copy(
            w_hbm.at[pl.ds(i * quarter, quarter)], wraw.at[pl.ds(i * quarter, quarter)], w_s.at[i]
        )
        for i in range(4)
    ]
    late_copies = [
        pltpu.make_async_copy(wo_hbm, wo.at[pl.ds(0, 336)], w_s.at[4]),
        pltpu.make_async_copy(wout_hbm, wout, w_s.at[5]),
    ]
    for cp in in_copies[0:2]:
        cp.start()
    for cp in in_copies[2:]:
        cp.start()
    for cp in in_copies[0:2]:
        cp.wait()
    for cp in w_copies:
        cp.start()

    def as_row(src, dst):
        for i in range(src.shape[0]):
            dst[0:1, i * Q : (i + 1) * Q] = src[i : i + 1, :]

    as_row(pre_gain_v, pre_gain)

    for half in range(2):
        tk = tokens[half * HALF : (half + 1) * HALF, :].astype(F32)
        inv = lax.rsqrt(jnp.mean(tk * tk, axis=1, keepdims=True) + NORM_FLOOR)
        rows[h, half] = (tk * inv * pre_gain[...]).astype(BF16)

    pl.semaphore_wait(barrier, 26)

    def ag(origin, half, role, device):
        return remote(
            rows.at[origin, half], rows.at[origin, half], ag_s, ag_r.at[role], (s, device)
        )

    own_pair = remote(rows.at[h], rows.at[h], ag_s, ag_r.at[6], (s, partner))
    sends = [ag(h, 0, 0, hr), ag(h, 1, 3, hl), ag(h, 1, 1, hr), ag(h, 0, 2, hl)]
    own_pair.start()
    for cp in sends:
        cp.start()

    for cp in late_copies:
        cp.start()
    for cp in in_copies[2:]:
        cp.wait()
    as_row(offset_x_v, offset_x)
    as_row(norm_gain_v, norm_gain)

    li = lax.broadcasted_iota(jnp.int32, (2 * Q, DL), 0)
    lc = lax.broadcasted_iota(jnp.int32, (2 * Q, DL), 1)
    head_of = lax.shift_right_logical(lc, 6)
    expand[...] = jnp.where(jnp.bitwise_and(li, Q - 1) == head_of, 1.0, 0.0).astype(BF16)
    small[...] = jnp.zeros_like(small)
    small[0:1, 0:HEADS] = dt_bias[...]
    small[1:2, 0:HEADS] = a_log[...]
    small[2:3, 0:HEADS] = skip_gain[...]
    pick_r = lax.broadcasted_iota(jnp.int32, (2 * Q, 2 * Q), 0)
    pick_c = lax.broadcasted_iota(jnp.int32, (2 * Q, 2 * Q), 1)
    pick_t = jnp.where(pick_r < Q, 2 * pick_r, 2 * (pick_r - Q) + 1)
    pick = jnp.where(pick_c == pick_t, 1.0, 0.0).astype(BF16)
    wflat = wraw.reshape(2 * D, DL)

    def split_step(i, carry):
        v = wflat[pl.ds(pl.multiple_of(i * 2 * Q, 2 * Q), 2 * Q), :]
        r = dot(pick, v).astype(BF16)
        wz[pl.ds(pl.multiple_of(i * Q, Q), Q), :] = r[0:Q, :]
        wx[pl.ds(pl.multiple_of(i * Q, Q), Q), 0:DL] = r[Q : 2 * Q, :]
        return carry

    for i in range(4):
        w_copies[i].wait()
        lax.fori_loop(i * quarter // Q, (i + 1) * quarter // Q, split_step, 0)
    for cp in late_copies:
        cp.wait()

    wo[336:384, :] = jnp.zeros((48, D), BF16)
    same = jnp.where(pick_r == pick_c, 1.0, 0.0).astype(BF16)
    for i in range(D // (2 * Q)):
        at = slice(i * 2 * Q, (i + 1) * 2 * Q)
        wx[at, DL:] = dot_t(same, wo[:, at]).astype(BF16)

    def put_rows(n, places):
        r = dot(n, wx[...])
        for at, lo, hi in places:
            xin[pl.ds(pl.multiple_of(at + 8, 8), hi - lo), :] = r[lo:hi, 0 : DL + 2 * NS].astype(BF16).astype(F32)
            dtr[pl.ds(pl.multiple_of(at, 8), hi - lo), :] = r[lo:hi, DL + 2 * NS :]

    def project_x(chip):
        n = rows[pl.ds(2 * chip, 2)].reshape(CH, D)
        put_rows(n, [(chip * CH, 0, CH)])

    def project_halves(chip_a, half_a, chip_b, half_b):
        n = jnp.concatenate(
            [rows[pl.ds(2 * chip_a, 2), half_a].reshape(R, D), rows[pl.ds(2 * chip_b, 2), half_b].reshape(R, D)],
            axis=0,
        )
        places = []
        for i, (chip, half) in enumerate(((chip_a, half_a), (chip_b, half_b))):
            for core in range(2):
                lo = i * R + core * HALF
                places.append((chip * CH + core * R + half * HALF, lo, lo + HALF))
        put_rows(n, places)

    def project_z(chip):
        n = rows[pl.ds(2 * chip, 2)].reshape(CH, D)
        zs[pl.ds(pl.multiple_of(chip * CH, CH), CH), :] = silu(dot(n, wz[...]).astype(BF16).astype(F32))

    def to_partner(origin, half, role):
        cp = ag(origin, half, 7 + role, partner)
        cp.start()
        sends.append(cp)

    def partner_done(chip, half, role):
        ag(chip * 2 + 1 - c, half, 7 + role, partner).wait_recv()

    def onward(origin, half, role, device):
        cp = ag(origin, half, role, device)
        cp.start()
        sends.append(cp)

    lane = lax.broadcasted_iota(jnp.int32, (1, Q), 1)
    ri = lax.broadcasted_iota(jnp.int32, (Q, Q), 0)
    ci = lax.broadcasted_iota(jnp.int32, (Q, Q), 1)
    tri = jnp.where(ri >= ci, 1.0, 0.0).astype(BF16)
    shift = (Q - h * HEADS) % Q

    def step_sizes(q):
        raw = pltpu.roll(dtr[pl.ds(pl.multiple_of(q * Q, Q), Q), :], shift, 1) + small[0:1, :]
        step = jnp.maximum(raw, 0.0) + jnp.log1p(jnp.exp(-jnp.abs(raw)))
        step = jnp.where(lane < HEADS, step, 0.0)
        la = step * -jnp.exp(small[1:2, :])
        dts[q] = step
        p3 = dot(tri, jnp.concatenate(split3(la), axis=1))
        cum[q] = p3[:, 0:Q] + p3[:, Q : 2 * Q] + p3[:, 2 * Q : 3 * Q]

    def conv_block(i):
        at = pl.multiple_of(i * 64, 64)
        for j in range((DL + 2 * NS) // Q):
            kern, off, lo = (kernel_x, offset_x, j * Q) if j < 5 else (kernel_bc, offset_bc, (j - 5) * Q)
            v = xin[pl.ds(at, 72), j * Q : (j + 1) * Q]
            u = kern[0:1, lo : lo + Q] * v
            for k in range(1, 4):
                u = pltpu.roll(u, 1, 0) + kern[k : k + 1, lo : lo + Q] * v
            v = silu(u[8:72, :] + off[:, lo : lo + Q]).astype(BF16)
            if j < 5:
                xb[pl.ds(at, 64), lo : lo + Q] = v
            else:
                (bmat, cmat)[j - 5][pl.ds(at, 64), :] = v

    def chunk_state(q):
        at = pl.multiple_of(q * Q, Q)
        cq = cum[q]
        fac = jnp.exp(cq[Q - 1 : Q, :] - cq) * dts[q]
        fx = dot(jnp.concatenate(split2(fac), axis=1), expand[...])
        xw = (xb[pl.ds(at, Q), :].astype(F32) * fx).astype(BF16)
        sl[q] = t_dot(bmat[pl.ds(at, Q), :], xw)

    far = xo // 2
    near = 1 - far
    odd = xo % 2
    late = 3 * far + odd
    other = 3 * far + 2 - 2 * odd

    def conv_early(i, carry):
        chip = (x + 3 + i // 3) % NX
        block = 3 * chip + i % 3
        block = jnp.where(jnp.logical_or(block == 0, i == 0), block + 1, block)
        conv_block(block)
        return carry

    remote(rows.at[partner], rows.at[partner], ag_s, ag_r.at[6], (s, partner)).wait_recv()
    ag(hl, 0, 0, hr).wait_recv()
    onward(hl, 0, 4, hr)
    ag(hr, 1, 3, hl).wait_recv()
    onward(hr, 1, 5, hl)
    to_partner(hl, 0, 0)
    to_partner(hr, 1, 3)
    project_x(x)
    partner_done(xl, 0, 0)
    partner_done(xr, 1, 3)
    project_halves(xl, 0, xr, 1)
    ag(hl, 1, 1, hr).wait_recv()
    to_partner(hl, 1, 1)
    ag(hr, 0, 2, hl).wait_recv()
    to_partner(hr, 0, 2)

    @pl.when(c == 0)
    def _():
        partner_done(xl, 1, 1)
        partner_done(xr, 0, 2)

    def put_seconds(core):
        n = jnp.concatenate([rows[2 * xl + core, 1], rows[2 * xr + core, 0]], axis=0)
        put_rows(
            n,
            [(xl * CH + core * R + HALF, 0, HALF), (xr * CH + core * R, HALF, R)],
        )

    put_seconds(1)
    lax.fori_loop(4, 6, conv_early, 0)

    @pl.when(c == 1)
    def _():
        partner_done(xl, 1, 1)
        partner_done(xr, 0, 2)

    put_seconds(0)

    def opposite_in():
        ag(ho, 0, 4, hr).wait_recv()
        ag(ho, 0, 11, partner).start()
        ag(ho, 1, 5, hl).wait_recv()
        ag(ho, 1, 12, partner).start()

    @pl.when(c == 1)
    def _():
        opposite_in()

    for q in (3 * near, 3 * near + 1, 3 * near + 2, other):
        step_sizes(q)
    lax.fori_loop(1, 4, conv_early, 0)

    @pl.when(c == 0)
    def _():
        opposite_in()

    lax.fori_loop(6, 9, conv_early, 0)
    chunk_state(3 * near + 1)
    chunk_state(3 * near + 2)
    partner_done(xo, 0, 4)
    partner_done(xo, 1, 5)
    project_x(xo)

    halo = remote(xin.at[pl.ds(T, 8)], xin.at[pl.ds(0, 8)], halo_s, halo_r, ((s + 1) % 32, h))

    @pl.when(s < 31)
    def _():
        halo.start()

    step_sizes(late)
    step_sizes(late + 1)
    total = cum[0][Q - 1 : Q, :]
    for q in range(1, NQ):
        total = total + cum[q][Q - 1 : Q, :]
    drow[...] = jnp.broadcast_to(jnp.exp(total), (8, Q))

    owner = 2 * x + 1
    far_first = (4, 3, 5, 2, 6, 1, 7)

    def z_peer(k):
        return (z + k) % NZ

    def rate_copy(k):
        return remote(
            drow, rd.at[c, z], zd_s, zd_r.at[c], (y * NZ + z_peer(k), owner)
        )

    def state_copy(k):
        at = pl.multiple_of(z_peer(k) * 16, 16)
        return remote(
            sb.at[pl.ds(at, 16)], rz.at[c, z], zs_s, zs_r.at[c], (y * NZ + z_peer(k), owner)
        )

    def sum_copy(k):
        return remote(tb, ty.at[y], y_s.at[k], y_r.at[y], ((y + k) % NY * NZ + z, h))

    def sum_rate_copy(k):
        return remote(tdb, tdy.at[y], yd_s.at[k], yd_r.at[y], ((y + k) % NY * NZ + z, h))

    def back_copy(g, k):
        zp = z_peer(k)
        return remote(pb.at[g, zp], cr.at[z], bk_s, bk_r, (y * NZ + zp, 2 * x + g))

    for k in range(1, NZ):
        rate_copy(k).start()

    @pl.when(c == 0)
    def _():
        rate_copy(0).start()

    @pl.when(c == 1)
    def _():
        rd[1, z] = drow[...]

    conv_block(3 * xo + 1)
    conv_block(3 * xo + 2)
    conv_block(jnp.where(xo == 0, 3 * xl, 3 * xo))
    conv_block(jnp.where(xl == 0, 3 * xo, 3 * xl))

    rest = jnp.where(near == 0, 3, 1)
    for k in range(3):
        chunk_state(rest + k)

    ends = jnp.concatenate([cum[q][Q - 1 : Q, :] for q in range(NQ)] + [jnp.zeros((2, Q), F32)], axis=0)
    decs = dot(jnp.concatenate(split2(jnp.exp(ends)), axis=1), expand[...])
    for lo in range(0, DL, Q):
        acc = sl[1, :, lo : lo + Q]
        for q in range(2, NQ):
            acc = acc * decs[q : q + 1, lo : lo + Q] + sl[q, :, lo : lo + Q]
        sacc[:, lo : lo + Q] = acc

    @pl.when(s == 0)
    def _():
        xin[0:8, :] = jnp.zeros((8, DL + 2 * NS), F32)

    @pl.when(s > 0)
    def _():
        halo.wait_recv()

    conv_block(0)
    chunk_state(0)
    later = decs[1:2, :]
    for q in range(2, NQ):
        later = later * decs[q : q + 1, :]
    sb[...] = (sacc[...] + later * sl[0]).astype(BF16)

    for k in far_first:
        state_copy(k).start()

    @pl.when(c == 0)
    def _():
        state_copy(0).start()

    @pl.when(c == 1)
    def _():
        rz[1, z] = sb[pl.ds(pl.multiple_of(z * 16, 16), 16), :]

    for lo in range(0, DL, Q):
        acc = jnp.zeros((NS, Q), F32)
        pd = jnp.ones((1, Q), F32)
        for q in range(NQ):
            st = sl[q, :, lo : lo + Q]
            dec = decs[q : q + 1, lo : lo + Q]
            sl[q, :, lo : lo + Q] = acc
            pdr[q, 0:1, lo : lo + Q] = pd
            acc = acc * dec + st
            pd = pd * dec

    project_z(xo)
    s3 = jnp.concatenate(split2(jnp.broadcast_to(small[2:3, :], (8, Q))), axis=1)
    skip_row = dot(s3, expand[...])[0:1, :]
    low = lax.broadcasted_iota(jnp.int32, (Q, Q), 1) < 64

    def intra_step(q, carry):
        at = pl.multiple_of(q * Q, Q)
        cq = cum[q]
        ef[q] = dot(jnp.concatenate(split2(jnp.exp(cq)), axis=1), expand[...])
        cqt = jnp.transpose(cq)
        dtt = jnp.transpose(dts[q])
        cb = dot_t(cmat[pl.ds(at, Q), :], bmat[pl.ds(at, Q), :])
        cbm = jnp.where(ri >= ci, cb, 0.0)
        for j in range(HEADS // 2):
            mixes = []
            for hh in (2 * j, 2 * j + 1):
                gap = jnp.minimum(cq[:, hh : hh + 1] - cqt[hh : hh + 1, :], 0.0)
                mixes.append((cbm * jnp.exp(gap) * dtt[hh : hh + 1, :]).astype(BF16))
            xp = xb[pl.ds(at, Q), j * Q : (j + 1) * Q].astype(F32)
            xd = jnp.concatenate(
                [jnp.where(low, xp, 0.0).astype(BF16), jnp.where(low, 0.0, xp).astype(BF16)], axis=0
            )
            yq = dot(jnp.concatenate(mixes, axis=1), xd)
            yv[pl.ds(at, Q), j * Q : (j + 1) * Q] = yq + skip_row[:, j * Q : (j + 1) * Q] * xp
        return carry

    lax.fori_loop(0, NQ, intra_step, 0)

    @pl.when(c == 1)
    def _():
        for g in (1, 0):
            if g == 1:
                await_bytes(dtr.at[pl.ds(0, 56)], zd_r.at[1])
                await_bytes(xb.at[pl.ds(0, 112)], zs_r.at[1])
            else:
                await_bytes(rd.at[0], zd_r.at[0])
                await_bytes(rz.at[0], zs_r.at[0])
            dz = jnp.concatenate([rd[g, k][0:1, :] for k in range(NZ)], axis=0)
            dx = dot(jnp.concatenate(split2(dz), axis=1), expand[...])
            acc = jnp.zeros((16, DL), F32)
            pd = jnp.ones((1, DL), F32)
            for k in range(NZ):
                pz[g, k] = acc
                pdz[g, k] = jnp.broadcast_to(pd, (8, DL))
                acc = acc * dx[k : k + 1, :] + rz[g, k].astype(F32)
                pd = pd * dx[k : k + 1, :]
            tb[g] = acc.astype(BF16)
            tdb[g] = jnp.broadcast_to(pd, (8, DL))
        for k in range(1, NY):
            @pl.when(y + k < NY)
            def _(k=k):
                sum_copy(k).start()
                sum_rate_copy(k).start()

    project_z(xl)
    project_z(x)

    @pl.when(c == 1)
    def _():
        cacc[...] = jnp.zeros_like(cacc)
        for k in range(NY - 1):
            @pl.when(k < y)
            def _(k=k):
                dev = (k * NZ + z, h)
                remote(tb, ty.at[k], y_s.at[1], y_r.at[k], dev).wait_recv()
                remote(tdb, tdy.at[k], yd_s.at[1], yd_r.at[k], dev).wait_recv()
                for g in range(2):
                    cacc[g] = cacc[g] * tdy[k, g][0:1, :] + ty[k, g].astype(F32)
        for g in range(2):
            for k in range(NZ):
                pb[g, k] = (pz[g, k] + pdz[g, k][0:1, :] * cacc[g]).astype(BF16)
        for k in far_first:
            for g in range(2):
                back_copy(g, k).start()
        back_copy(0, 0).start()
        cr[z] = pb[1, z]

    project_z(xr)

    @pl.when(c == 1)
    def _():
        await_bytes(xb.at[pl.ds(0, 112)], bk_r)

    @pl.when(c == 0)
    def _():
        await_bytes(cr, bk_r)

    def out_step(q, carry):
        at = pl.multiple_of(q * Q, Q)
        state = (sl[q] + pdr[q][0:1, :] * cr[...].reshape(NS, DL).astype(F32)).astype(BF16)
        cross = dot(cmat[pl.ds(at, Q), :], state)
        g = (yv[pl.ds(at, Q), :] + ef[q] * cross) * zs[pl.ds(at, Q), :]
        sqc[pl.ds(at, Q), :] = jnp.broadcast_to(jnp.sum(g * g, axis=1, keepdims=True), (Q, Q))
        gb[pl.ds(at, Q), :] = (g * norm_gain[...]).astype(BF16)
        return carry

    def pair_copy(d, lo, width, sem):
        return remote(
            part.at[2 * d + 1 - c, :, :, pl.ds(lo, width)], pr.at[d, :, :, pl.ds(lo, width)],
            pp_s, pp_r.at[sem], (s, partner),
        )

    def out_part(d, lo, width, sem):
        n = gb[pl.ds(pl.multiple_of(d * CH, CH), CH), :]
        for at in range(lo, lo + width, 256):
            end = min(at + 256, lo + width)
            part[pl.ds(2 * d, 2), :, :, at:end] = (
                dot(n, wout[:, at:end]).astype(BF16).reshape(2, 2, HALF, end - at)
            )
        pair_copy(d, lo, width, sem).start()

    def out_chip(d):
        out_part(d, 0, D, d)

    def pair_sum(d, half):
        return part[2 * d + c, half].astype(F32) + pr[d, half].astype(F32)

    def pair_wait(d):
        remote(part.at[0], pr.at[d], pp_s, pp_r.at[d], (s, partner)).wait_recv()

    d1 = xo + 1 - 2 * (xo % 2)
    d2 = x + 1 - 2 * (x % 2)
    out_step(late, 0)
    out_step(late + 1, 0)
    cuts = ((0, 512), (512, 896), (1408, 1152))
    pieces = len(cuts)

    def relay_copy(half, i):
        here = pl.ds(*cuts[i])
        return remote(
            ps.at[0, half, :, here], rl.at[half, :, here], rl_s, rl_r.at[half, i],
            (s, hl if half else hr),
        )

    def relay(i):
        here = pl.ds(*cuts[i])
        pair_copy(xo, *cuts[i], 4 + i).wait_recv()
        for half in range(2):
            ps[0, half, :, here] = (
                part[2 * xo + c, half, :, here].astype(F32) + pr[xo, half, :, here].astype(F32)
            ).astype(BF16)
            relay_copy(half, i).start()

    @pl.when(c == 0)
    def _():
        for i in range(pieces):
            out_part(xo, *cuts[i], 4 + i)
            if i > 0:
                relay(i - 1)
        relay(pieces - 1)
        out_step(other, 0)
        out_chip(d1)

    @pl.when(c == 1)
    def _():
        for i in range(pieces):
            out_part(xo, *cuts[i], 4 + i)
        relay(0)
        out_step(other, 0)
        relay(1)
        out_chip(d1)
        relay(2)

    lax.fori_loop(near * 3, near * 3 + 3, out_step, 0)
    out_chip(d2)

    def side_of(d):
        return jnp.where(d == xr, 0, 1)

    finals = []

    def final_send(slot, d, half):
        side = side_of(d)
        cp = remote(
            ps.at[slot, half], rf.at[side, half], rf_s, rf_r.at[side, half], (s, 2 * d + c)
        )
        cp.start()
        finals.append(cp)

    def send_direct(slot, d):
        half = 1 - side_of(d)
        pair_wait(d)
        ps[slot, half] = pair_sum(d, half).astype(BF16)
        final_send(slot, d, half)

    def send_relayed(slot, d):
        half = side_of(d)
        for i in range(pieces):
            here = pl.ds(*cuts[i])
            remote(
                ps.at[0, 0, :, here], rl.at[half, :, here], rl_s, rl_r.at[half, i], (s, hr)
            ).wait_recv()
        ps[slot, half] = (pair_sum(d, half) + rl[half].astype(F32)).astype(BF16)
        final_send(slot, d, half)

    send_direct(1, d1)
    sq_sends = []
    for k in range(8):
        col = sqc[pl.ds(pl.multiple_of(((h + k) % 8) * R, 32), Q), :]
        sqs[(h + k) % 8] = jnp.transpose(col)[0:8, :]
        if k == 0:
            sqr[h] = sqs[h]
        else:
            cp = remote(sqs.at[(h + k) % 8], sqr.at[h], sq_s, sq_r, (s, (h + k) % 8))
            cp.start()
            sq_sends.append(cp)
    send_direct(2, d2)
    send_relayed(1, d1)
    send_relayed(2, d2)
    out_chip(x)

    pair_wait(x)

    def final_wait(side, half):
        remote(
            ps.at[1, half], rf.at[side, half], rf_s, rf_r.at[side, half], (s, hl)
        ).wait_recv()

    for half in range(2):
        final_wait(1 - half, half)
        tot[half] = pair_sum(x, half) + rf[1 - half, half].astype(F32)
    await_bytes(dtr.at[pl.ds(0, 56)], sq_r)
    squares = jnp.sum(sqr[...], axis=0)[0:1, :]
    inv_row = lax.rsqrt(squares / (DL * 8) + NORM_FLOOR)
    inv_col = jnp.transpose(jnp.broadcast_to(inv_row, (Q, Q)))
    for half in range(2):
        final_wait(half, half)
        out[half * HALF : (half + 1) * HALF, :] = (
            (tot[half] + rf[half, half].astype(F32)) * inv_col[half * HALF : (half + 1) * HALF, 0:1]
        ).astype(BF16)

    await_bytes(rows.at[pl.ds(0, 7)], ag_s)
    await_bytes(part.at[pl.ds(0, 4)], pp_s)
    await_bytes(part.at[0], rl_s)
    await_bytes(part.at[pl.ds(0, 2)], rf_s)
    await_bytes(dtr.at[pl.ds(0, 56)], sq_s)

    @pl.when(s < 31)
    def _():
        halo.wait_send()

    @pl.when(c == 0)
    def _():
        await_bytes(rd.at[0], zd_s)
        await_bytes(rz.at[0], zs_s)

    @pl.when(c == 1)
    def _():
        await_bytes(dtr.at[pl.ds(0, 56)], zd_s)
        await_bytes(xb.at[pl.ds(0, 112)], zs_s)
        await_bytes(xb.at[pl.ds(0, 240)], bk_s)
        for k in range(1, NY):
            @pl.when(y + k < NY)
            def _(k=k):
                sum_copy(k).wait_send()
                sum_rate_copy(k).wait_send()


def on_device(
    tokens, pre_gain, inner_proj, outer_proj, kernel_x, kernel_bc, offset_x, offset_bc, dt_bias, a_log,
    skip_gain, norm_gain, out_proj,
):
    vm = pl.BlockSpec(memory_space=pltpu.VMEM)
    hbm = pl.BlockSpec(memory_space=pltpu.HBM)
    dma = pltpu.SemaphoreType.DMA
    V = pltpu.VMEM
    scratch = [
        V((R, D), BF16), V((D // Q, Q), F32), V((4, DL), F32), V((4, 2 * NS), F32), V((DL // Q, Q), F32),
        V((1, 2 * NS), F32), V((1, HEADS), F32), V((1, HEADS), F32), V((1, HEADS), F32), V((DL // Q, Q), F32),
        V((D, 2, DL), BF16), V((D, DL), BF16), V((D, 1024), BF16), V((384, D), BF16), V((DL, D), BF16), V((8, 2, HALF, D), BF16),
        V((T + 8, DL + 2 * NS), F32), V((T, Q), F32), V((T, DL), F32), V((T, DL), BF16),
        V((T, NS), BF16), V((T, NS), BF16), V((NQ, Q, Q), F32), V((NQ, Q, Q), F32),
        V((2 * Q, DL), BF16), V((NQ, Q, DL), F32), V((NQ, NS, DL), F32), V((NS, DL), F32),
        V((NQ, 8, DL), F32),
        V((T, DL), F32), V((NS, DL), BF16), V((8, Q), F32), V((2, NZ, 16, DL), BF16), V((2, NZ, 8, Q), F32),
        V((2, NZ, 16, DL), F32), V((2, NZ, 8, DL), F32), V((2, 16, DL), BF16), V((2, 8, DL), F32),
        V((NY, 2, 16, DL), BF16), V((NY, 2, 8, DL), F32), V((2, 16, DL), F32), V((2, NZ, 16, DL), BF16),
        V((NZ, 16, DL), BF16), V((T, DL), BF16), V((T + 32, Q), F32), V((8, 2, HALF, D), BF16),
        V((NX, 2, HALF, D), BF16), V((3, 2, HALF, D), BF16), V((2, HALF, D), BF16), V((2, 2, HALF, D), BF16),
        V((8, 8, Q), F32), V((8, 8, Q), F32), V((8, Q), F32), V((1, D), F32), V((1, DL), F32),
        V((1, DL), F32), V((2, HALF, D), F32),
        dma, dma((13,)), dma, dma, dma, dma((2,)), dma, dma((2,)),
        dma((NY,)), dma((NY,)), dma((NY,)), dma((NY,)), dma, dma,
        dma, dma((7,)), dma, dma((2, 3)), dma, dma((2, 2)), dma, dma,
        dma((6,)), dma((10,)),
    ]
    args = (
        tokens, pre_gain.reshape(D // Q, Q), inner_proj, outer_proj.T, kernel_x, kernel_bc,
        offset_x.reshape(DL // Q, Q), offset_bc[None], dt_bias[None], a_log[None], skip_gain[None],
        norm_gain.reshape(DL // Q, Q), out_proj,
    )
    args = [pltpu.with_memory_space_constraint(v, pltpu.HBM) for v in args]
    return pl.pallas_call(
        kernel,
        out_shape=jax.ShapeDtypeStruct((R, D), BF16),
        in_specs=[hbm] * 13,
        out_specs=vm,
        scratch_shapes=scratch,
        compiler_params=pltpu.CompilerParams(
            collective_id=0, has_side_effects=True, vmem_limit_bytes=55_000_000
        ),
    )(*args)


def solution(mesh):
    in_specs = (
        P(("seq", "head"), None), P(), P(None, None, "head"), P(), P(None, "head"), P(), P("head"), P(),
        P("head"), P("head"), P("head"), P("head"), P("head", None),
    )
    return jax.shard_map(
        on_device, mesh=mesh, in_specs=in_specs, out_specs=P(("seq", "head"), None), check_vma=False
    )
```

```python
import jax
import jax.numpy as jnp
from jax import lax
from jax.experimental import pallas as pl
from jax.experimental.pallas import tpu as pltpu
from jax.sharding import PartitionSpec as P

MESH = pl.DeviceIdType.MESH
BF16 = jnp.bfloat16
F32 = jnp.float32

NORM_FLOOR = 0.1
D = 2560
DL = 640
NS = 128
R = 96
HALF = 48
T = 768
Q = 128
NQ = 6
CH = 192
HEADS = 10
NY, NZ, NX = 4, 8, 4


def dot(a, b):
    return jnp.dot(a, b, preferred_element_type=F32)


def dot_t(a, b):
    return lax.dot_general(a, b, (((1,), (1,)), ((), ())), preferred_element_type=F32)


def t_dot(a, b):
    return lax.dot_general(a, b, (((0,), (0,)), ((), ())), preferred_element_type=F32)


def split2(v):
    hi = v.astype(BF16)
    lo = (v - hi.astype(F32)).astype(BF16)
    return hi, lo


def split3(v):
    hi, mid = split2(v)
    lo = (v - hi.astype(F32) - mid.astype(F32)).astype(BF16)
    return hi, mid, lo


def silu(v):
    half = 0.5 * v
    return half + half * jnp.tanh(half)


def remote(src, dst, send, recv, device):
    return pltpu.make_async_remote_copy(
        src_ref=src, dst_ref=dst, send_sem=send, recv_sem=recv, device_id=device, device_id_type=MESH
    )


def kernel(
    tokens_in, pre_gain_in, w_hbm, wo_hbm, kernel_x_in, kernel_bc_in, offset_x_in, offset_bc_in, dt_bias_in,
    a_log_in, skip_gain_in, norm_gain_in, wout_hbm,
    out,
    tokens, pre_gain_v, kernel_x, kernel_bc, offset_x_v, offset_bc, dt_bias, a_log, skip_gain, norm_gain_v,
    wraw, wz, wx, wo, wout, rows, xin, dtr, zs, xb, bmat, cmat, dts, cum, expand, ef, sl, sacc, pdr,
    yv, sb, drow, rz, rd, dxs, pz, pdz, tb, tdb, ty, tdy, cacc, pb, cr, gb, sqc, part, pr, ps, rl, rf,
    sqs, sqr, small, pre_gain, offset_x, norm_gain, tot,
    ag_s, ag_r, halo_s, halo_r, zs_s, zs_r, zd_s, zd_r, y_s, y_r, yd_s, yd_r, bk_s, bk_r,
    pp_s, pp_r, rl_s, rl_r, rf_s, rf_r, sq_s, sq_r, w_s, in_s,
):
    s = lax.axis_index("seq")
    h = lax.axis_index("head")
    y = s // NZ
    z = s % NZ
    x = h // 2
    c = h % 2
    partner = x * 2 + (1 - c)
    xr = (x + 1) % NX
    xl = (x + NX - 1) % NX
    xo = (x + 2) % NX
    hr, hl, ho = xr * 2 + c, xl * 2 + c, xo * 2 + c

    def await_bytes(like, sem):
        pltpu.make_async_copy(like, like, sem).wait()

    barrier = pltpu.get_barrier_semaphore()
    for k in range(1, 8):
        pl.semaphore_signal(barrier, inc=1, device_id=(s, (h + k) % 8), device_id_type=MESH)
    for k in range(1, NZ):
        pl.semaphore_signal(barrier, inc=1, device_id=(y * NZ + (z + k) % NZ, h), device_id_type=MESH)
    for k in range(1, NZ):
        pl.semaphore_signal(barrier, inc=1, device_id=(y * NZ + (z + k) % NZ, partner), device_id_type=MESH)
    for k in range(1, NY):
        pl.semaphore_signal(barrier, inc=1, device_id=(((y + k) % NY) * NZ + z, h), device_id_type=MESH)
    for k in (1, 31):
        pl.semaphore_signal(barrier, inc=1, device_id=((s + k) % 32, h), device_id_type=MESH)

    pairs = (
        (tokens_in, tokens), (pre_gain_in, pre_gain_v), (kernel_x_in, kernel_x), (kernel_bc_in, kernel_bc),
        (offset_x_in, offset_x_v), (offset_bc_in, offset_bc), (dt_bias_in, dt_bias), (a_log_in, a_log),
        (skip_gain_in, skip_gain), (norm_gain_in, norm_gain_v),
    )
    in_copies = [pltpu.make_async_copy(src, dst, in_s.at[i]) for i, (src, dst) in enumerate(pairs)]
    quarter = D // 4
    w_copies = [
        pltpu.make_async_copy(
            w_hbm.at[pl.ds(i * quarter, quarter)], wraw.at[pl.ds(i * quarter, quarter)], w_s.at[i]
        )
        for i in range(4)
    ]
    late_copies = [
        pltpu.make_async_copy(wo_hbm, wo.at[pl.ds(0, 336)], w_s.at[4]),
        pltpu.make_async_copy(wout_hbm, wout, w_s.at[5]),
    ]
    for cp in in_copies[0:2]:
        cp.start()
    for cp in in_copies[2:]:
        cp.start()
    for cp in in_copies[0:2]:
        cp.wait()
    for cp in w_copies:
        cp.start()

    def as_row(src, dst):
        for i in range(src.shape[0]):
            dst[0:1, i * Q : (i + 1) * Q] = src[i : i + 1, :]

    as_row(pre_gain_v, pre_gain)

    for half in range(2):
        tk = tokens[half * HALF : (half + 1) * HALF, :].astype(F32)
        inv = lax.rsqrt(jnp.mean(tk * tk, axis=1, keepdims=True) + NORM_FLOOR)
        rows[h, half] = (tk * inv * pre_gain[...]).astype(BF16)

    pl.semaphore_wait(barrier, 26)

    def ag(origin, half, role, device):
        return remote(
            rows.at[origin, half], rows.at[origin, half], ag_s, ag_r.at[role], (s, device)
        )

    own_pair = remote(rows.at[h], rows.at[h], ag_s, ag_r.at[6], (s, partner))
    sends = [ag(h, 0, 0, hr), ag(h, 1, 3, hl), ag(h, 1, 1, hr), ag(h, 0, 2, hl)]
    own_pair.start()
    for cp in sends:
        cp.start()

    for cp in late_copies:
        cp.start()
    for cp in in_copies[2:]:
        cp.wait()
    as_row(offset_x_v, offset_x)
    as_row(norm_gain_v, norm_gain)

    li = lax.broadcasted_iota(jnp.int32, (2 * Q, DL), 0)
    lc = lax.broadcasted_iota(jnp.int32, (2 * Q, DL), 1)
    head_of = lax.shift_right_logical(lc, 6)
    expand[...] = jnp.where(jnp.bitwise_and(li, Q - 1) == head_of, 1.0, 0.0).astype(BF16)
    small[...] = jnp.zeros_like(small)
    small[0:1, 0:HEADS] = dt_bias[...]
    small[1:2, 0:HEADS] = a_log[...]
    small[2:3, 0:HEADS] = skip_gain[...]
    pick_r = lax.broadcasted_iota(jnp.int32, (2 * Q, 2 * Q), 0)
    pick_c = lax.broadcasted_iota(jnp.int32, (2 * Q, 2 * Q), 1)
    pick_t = jnp.where(pick_r < Q, 2 * pick_r, 2 * (pick_r - Q) + 1)
    pick = jnp.where(pick_c == pick_t, 1.0, 0.0).astype(BF16)
    wflat = wraw.reshape(2 * D, DL)

    def split_step(i, carry):
        v = wflat[pl.ds(pl.multiple_of(i * 2 * Q, 2 * Q), 2 * Q), :]
        r = dot(pick, v).astype(BF16)
        wz[pl.ds(pl.multiple_of(i * Q, Q), Q), :] = r[0:Q, :]
        wx[pl.ds(pl.multiple_of(i * Q, Q), Q), 0:DL] = r[Q : 2 * Q, :]
        return carry

    for i in range(4):
        w_copies[i].wait()
        lax.fori_loop(i * quarter // Q, (i + 1) * quarter // Q, split_step, 0)
    for cp in late_copies:
        cp.wait()

    wo[336:384, :] = jnp.zeros((48, D), BF16)
    same = jnp.where(pick_r == pick_c, 1.0, 0.0).astype(BF16)
    for i in range(D // (2 * Q)):
        at = slice(i * 2 * Q, (i + 1) * 2 * Q)
        wx[at, DL:] = dot_t(same, wo[:, at]).astype(BF16)

    def put_rows(n, places):
        r = dot(n, wx[...])
        for at, lo, hi in places:
            xin[pl.ds(pl.multiple_of(at + 8, 8), hi - lo), :] = r[lo:hi, 0 : DL + 2 * NS].astype(BF16).astype(F32)
            dtr[pl.ds(pl.multiple_of(at, 8), hi - lo), :] = r[lo:hi, DL + 2 * NS :]

    def project_x(chip):
        n = rows[pl.ds(2 * chip, 2)].reshape(CH, D)
        put_rows(n, [(chip * CH, 0, CH)])

    def project_halves(chip_a, half_a, chip_b, half_b):
        n = jnp.concatenate(
            [rows[pl.ds(2 * chip_a, 2), half_a].reshape(R, D), rows[pl.ds(2 * chip_b, 2), half_b].reshape(R, D)],
            axis=0,
        )
        places = []
        for i, (chip, half) in enumerate(((chip_a, half_a), (chip_b, half_b))):
            for core in range(2):
                lo = i * R + core * HALF
                places.append((chip * CH + core * R + half * HALF, lo, lo + HALF))
        put_rows(n, places)

    def project_z(chip):
        n = rows[pl.ds(2 * chip, 2)].reshape(CH, D)
        zs[pl.ds(pl.multiple_of(chip * CH, CH), CH), :] = silu(dot(n, wz[...]).astype(BF16).astype(F32))

    def to_partner(origin, half, role):
        cp = ag(origin, half, 7 + role, partner)
        cp.start()
        sends.append(cp)

    def partner_done(chip, half, role):
        ag(chip * 2 + 1 - c, half, 7 + role, partner).wait_recv()

    def onward(origin, half, role, device):
        cp = ag(origin, half, role, device)
        cp.start()
        sends.append(cp)

    lane = lax.broadcasted_iota(jnp.int32, (1, Q), 1)
    ri = lax.broadcasted_iota(jnp.int32, (Q, Q), 0)
    ci = lax.broadcasted_iota(jnp.int32, (Q, Q), 1)
    tri = jnp.where(ri >= ci, 1.0, 0.0).astype(BF16)
    shift = (Q - h * HEADS) % Q

    def step_sizes(q):
        raw = pltpu.roll(dtr[pl.ds(pl.multiple_of(q * Q, Q), Q), :], shift, 1) + small[0:1, :]
        step = jnp.maximum(raw, 0.0) + jnp.log1p(jnp.exp(-jnp.abs(raw)))
        step = jnp.where(lane < HEADS, step, 0.0)
        la = step * -jnp.exp(small[1:2, :])
        dts[q] = step
        p3 = dot(tri, jnp.concatenate(split3(la), axis=1))
        cum[q] = p3[:, 0:Q] + p3[:, Q : 2 * Q] + p3[:, 2 * Q : 3 * Q]

    def conv_block(i):
        at = pl.multiple_of(i * 64, 64)
        for j in range((DL + 2 * NS) // Q):
            kern, off, lo = (kernel_x, offset_x, j * Q) if j < 5 else (kernel_bc, offset_bc, (j - 5) * Q)
            v = xin[pl.ds(at, 72), j * Q : (j + 1) * Q]
            u = kern[0:1, lo : lo + Q] * v
            for k in range(1, 4):
                u = pltpu.roll(u, 1, 0) + kern[k : k + 1, lo : lo + Q] * v
            v = silu(u[8:72, :] + off[:, lo : lo + Q]).astype(BF16)
            if j < 5:
                xb[pl.ds(at, 64), lo : lo + Q] = v
            else:
                (bmat, cmat)[j - 5][pl.ds(at, 64), :] = v

    def chunk_state(q):
        at = pl.multiple_of(q * Q, Q)
        cq = cum[q]
        fac = jnp.exp(cq[Q - 1 : Q, :] - cq) * dts[q]
        fx = dot(jnp.concatenate(split2(fac), axis=1), expand[...])
        xw = (xb[pl.ds(at, Q), :].astype(F32) * fx).astype(BF16)
        sl[q] = t_dot(bmat[pl.ds(at, Q), :], xw)

    far = xo // 2
    near = 1 - far
    odd = xo % 2
    late = 3 * far + odd
    other = 3 * far + 2 - 2 * odd

    def conv_early(i, carry):
        chip = (x + 3 + i // 3) % NX
        block = 3 * chip + i % 3
        block = jnp.where(jnp.logical_or(block == 0, i == 0), block + 1, block)
        conv_block(block)
        return carry

    remote(rows.at[partner], rows.at[partner], ag_s, ag_r.at[6], (s, partner)).wait_recv()
    ag(hl, 0, 0, hr).wait_recv()
    onward(hl, 0, 4, hr)
    ag(hr, 1, 3, hl).wait_recv()
    onward(hr, 1, 5, hl)
    to_partner(hl, 0, 0)
    to_partner(hr, 1, 3)
    project_x(x)
    partner_done(xl, 0, 0)
    partner_done(xr, 1, 3)
    project_halves(xl, 0, xr, 1)
    ag(hl, 1, 1, hr).wait_recv()
    to_partner(hl, 1, 1)
    ag(hr, 0, 2, hl).wait_recv()
    to_partner(hr, 0, 2)

    @pl.when(c == 0)
    def _():
        partner_done(xl, 1, 1)
        partner_done(xr, 0, 2)

    def put_seconds(core):
        n = jnp.concatenate([rows[2 * xl + core, 1], rows[2 * xr + core, 0]], axis=0)
        put_rows(
            n,
            [(xl * CH + core * R + HALF, 0, HALF), (xr * CH + core * R, HALF, R)],
        )

    put_seconds(1)
    lax.fori_loop(4, 6, conv_early, 0)

    @pl.when(c == 1)
    def _():
        partner_done(xl, 1, 1)
        partner_done(xr, 0, 2)

    put_seconds(0)

    def opposite_in():
        ag(ho, 0, 4, hr).wait_recv()
        ag(ho, 0, 11, partner).start()
        ag(ho, 1, 5, hl).wait_recv()
        ag(ho, 1, 12, partner).start()

    @pl.when(c == 1)
    def _():
        opposite_in()

    for q in (3 * near, 3 * near + 1, 3 * near + 2, other):
        step_sizes(q)
    lax.fori_loop(1, 4, conv_early, 0)
    lax.fori_loop(6, 8, conv_early, 0)

    @pl.when(c == 0)
    def _():
        opposite_in()

    lax.fori_loop(8, 9, conv_early, 0)
    chunk_state(3 * near + 1)
    chunk_state(3 * near + 2)
    partner_done(xo, 0, 4)
    partner_done(xo, 1, 5)
    project_x(xo)

    halo = remote(xin.at[pl.ds(T, 8)], xin.at[pl.ds(0, 8)], halo_s, halo_r, ((s + 1) % 32, h))

    @pl.when(s < 31)
    def _():
        halo.start()

    step_sizes(late)
    step_sizes(late + 1)
    total = cum[0][Q - 1 : Q, :]
    for q in range(1, NQ):
        total = total + cum[q][Q - 1 : Q, :]
    drow[...] = jnp.broadcast_to(jnp.exp(total), (8, Q))

    owner = 2 * x + 1
    far_first = (4, 3, 5, 2, 6, 1, 7)

    def z_peer(k):
        return (z + k) % NZ

    def rate_copy(k):
        return remote(
            drow, rd.at[c, z], zd_s, zd_r.at[c], (y * NZ + z_peer(k), owner)
        )

    def state_copy(k):
        at = pl.multiple_of(z_peer(k) * 16, 16)
        return remote(
            sb.at[pl.ds(at, 16)], rz.at[c, z], zs_s, zs_r.at[c], (y * NZ + z_peer(k), owner)
        )

    def sum_copy(k):
        return remote(tb, ty.at[y], y_s.at[k - 1], y_r.at[y], ((y + k) % NY * NZ + z, h))

    def sum_rate_copy(k):
        return remote(tdb, tdy.at[y], yd_s.at[k - 1], yd_r.at[y], ((y + k) % NY * NZ + z, h))

    def back_copy(g, k):
        zp = z_peer(k)
        return remote(pb.at[g, zp], cr.at[z], bk_s, bk_r, (y * NZ + zp, 2 * x + g))

    for k in range(1, NZ):
        rate_copy(k).start()

    @pl.when(c == 0)
    def _():
        rate_copy(0).start()

    @pl.when(c == 1)
    def _():
        rd[1, z] = drow[...]

    conv_block(3 * xo + 1)
    conv_block(3 * xo + 2)
    conv_block(jnp.where(xo == 0, 3 * xl, 3 * xo))
    conv_block(jnp.where(xl == 0, 3 * xo, 3 * xl))

    rest = jnp.where(near == 0, 3, 1)
    for k in range(3):
        chunk_state(rest + k)

    ends = jnp.concatenate([cum[q][Q - 1 : Q, :] for q in range(NQ)] + [jnp.zeros((2, Q), F32)], axis=0)
    decs = dot(jnp.concatenate(split2(jnp.exp(ends)), axis=1), expand[...])
    for lo in range(0, DL, Q):
        acc = sl[1, :, lo : lo + Q]
        for q in range(2, NQ):
            acc = acc * decs[q : q + 1, lo : lo + Q] + sl[q, :, lo : lo + Q]
        sacc[:, lo : lo + Q] = acc

    @pl.when(s == 0)
    def _():
        xin[0:8, :] = jnp.zeros((8, DL + 2 * NS), F32)

    @pl.when(s > 0)
    def _():
        halo.wait_recv()

    conv_block(0)
    chunk_state(0)
    later = decs[1:2, :]
    for q in range(2, NQ):
        later = later * decs[q : q + 1, :]
    sb[...] = (sacc[...] + later * sl[0]).astype(BF16)

    for k in far_first:
        state_copy(k).start()

    @pl.when(c == 0)
    def _():
        state_copy(0).start()

    @pl.when(c == 1)
    def _():
        rz[1, z] = sb[pl.ds(pl.multiple_of(z * 16, 16), 16), :]

    for lo in range(0, DL, Q):
        acc = jnp.zeros((NS, Q), F32)
        pd = jnp.ones((1, Q), F32)
        for q in range(NQ):
            st = sl[q, :, lo : lo + Q]
            dec = decs[q : q + 1, lo : lo + Q]
            sl[q, :, lo : lo + Q] = acc
            pdr[q, 0:1, lo : lo + Q] = pd
            acc = acc * dec + st
            pd = pd * dec

    project_z(xo)
    s3 = jnp.concatenate(split2(jnp.broadcast_to(small[2:3, :], (8, Q))), axis=1)
    skip_row = dot(s3, expand[...])[0:1, :]
    low = lax.broadcasted_iota(jnp.int32, (Q, Q), 1) < 64

    def intra_step(q, carry):
        at = pl.multiple_of(q * Q, Q)
        cq = cum[q]
        ef[q] = dot(jnp.concatenate(split2(jnp.exp(cq)), axis=1), expand[...])
        cqt = jnp.transpose(cq)
        dtt = jnp.transpose(dts[q])
        cb = dot_t(cmat[pl.ds(at, Q), :], bmat[pl.ds(at, Q), :])
        cbm = jnp.where(ri >= ci, cb, 0.0)
        for j in range(HEADS // 2):
            mixes = []
            for hh in (2 * j, 2 * j + 1):
                gap = jnp.minimum(cq[:, hh : hh + 1] - cqt[hh : hh + 1, :], 0.0)
                mixes.append((cbm * jnp.exp(gap) * dtt[hh : hh + 1, :]).astype(BF16))
            xp = xb[pl.ds(at, Q), j * Q : (j + 1) * Q].astype(F32)
            xd = jnp.concatenate(
                [jnp.where(low, xp, 0.0).astype(BF16), jnp.where(low, 0.0, xp).astype(BF16)], axis=0
            )
            yq = dot(jnp.concatenate(mixes, axis=1), xd)
            yv[pl.ds(at, Q), j * Q : (j + 1) * Q] = yq + skip_row[:, j * Q : (j + 1) * Q] * xp
        return carry

    lax.fori_loop(0, NQ, intra_step, 0)

    @pl.when(c == 1)
    def _():
        for g in (1, 0):
            if g == 1:
                await_bytes(dtr.at[pl.ds(0, 56)], zd_r.at[1])
            else:
                await_bytes(rd.at[0], zd_r.at[0])
            dz = jnp.concatenate([rd[g, k][0:1, :] for k in range(NZ)], axis=0)
            dx = dot(jnp.concatenate(split2(dz), axis=1), expand[...])
            dxs[g] = dx
            pd = jnp.ones((1, DL), F32)
            for k in range(NZ):
                pdz[g, k] = jnp.broadcast_to(pd, (8, DL))
                pd = pd * dx[k : k + 1, :]
            tdb[g] = jnp.broadcast_to(pd, (8, DL))
        for k in range(1, NY):
            @pl.when(y + k < NY)
            def _(k=k):
                sum_rate_copy(k).start()

        for g in (1, 0):
            if g == 1:
                await_bytes(xb.at[pl.ds(0, 112)], zs_r.at[1])
            else:
                await_bytes(rz.at[0], zs_r.at[0])
            dx = dxs[g]
            acc = jnp.zeros((16, DL), F32)
            for k in range(NZ):
                pz[g, k] = acc
                acc = acc * dx[k : k + 1, :] + rz[g, k].astype(F32)
            tb[g] = acc.astype(BF16)
        for k in (2, 1, 3):
            @pl.when(y + k < NY)
            def _(k=k):
                sum_copy(k).start()

    project_z(xl)
    project_z(x)

    @pl.when(c == 1)
    def _():
        cacc[...] = jnp.zeros_like(cacc)
        for k in range(NY - 1):
            @pl.when(k < y)
            def _(k=k):
                dev = (k * NZ + z, h)
                remote(tb, ty.at[k], y_s.at[0], y_r.at[k], dev).wait_recv()
                remote(tdb, tdy.at[k], yd_s.at[0], yd_r.at[k], dev).wait_recv()
                for g in range(2):
                    cacc[g] = cacc[g] * tdy[k, g][0:1, :] + ty[k, g].astype(F32)
        for g in range(2):
            for k in range(NZ):
                pb[g, k] = (pz[g, k] + pdz[g, k][0:1, :] * cacc[g]).astype(BF16)
        for k in far_first:
            for g in range(2):
                back_copy(g, k).start()
        back_copy(0, 0).start()
        cr[z] = pb[1, z]

    project_z(xr)

    @pl.when(c == 1)
    def _():
        await_bytes(xb.at[pl.ds(0, 112)], bk_r)

    @pl.when(c == 0)
    def _():
        await_bytes(cr, bk_r)

    def out_step(q, carry):
        at = pl.multiple_of(q * Q, Q)
        state = (sl[q] + pdr[q][0:1, :] * cr[...].reshape(NS, DL).astype(F32)).astype(BF16)
        cross = dot(cmat[pl.ds(at, Q), :], state)
        g = (yv[pl.ds(at, Q), :] + ef[q] * cross) * zs[pl.ds(at, Q), :]
        sqc[pl.ds(at, Q), :] = jnp.broadcast_to(jnp.sum(g * g, axis=1, keepdims=True), (Q, Q))
        gb[pl.ds(at, Q), :] = (g * norm_gain[...]).astype(BF16)
        return carry

    def pair_copy(d, lo, width, sem):
        return remote(
            part.at[2 * d + 1 - c, :, :, pl.ds(lo, width)], pr.at[d, :, :, pl.ds(lo, width)],
            pp_s, pp_r.at[sem], (s, partner),
        )

    def out_part(d, lo, width, sem):
        n = gb[pl.ds(pl.multiple_of(d * CH, CH), CH), :]
        for at in range(lo, lo + width, 256):
            end = min(at + 256, lo + width)
            part[pl.ds(2 * d, 2), :, :, at:end] = (
                dot(n, wout[:, at:end]).astype(BF16).reshape(2, 2, HALF, end - at)
            )
        pair_copy(d, lo, width, sem).start()

    def out_chip(d):
        out_part(d, 0, D, d)

    def pair_sum(d, half):
        return part[2 * d + c, half].astype(F32) + pr[d, half].astype(F32)

    def pair_wait(d):
        remote(part.at[0], pr.at[d], pp_s, pp_r.at[d], (s, partner)).wait_recv()

    d1 = xo + 1 - 2 * (xo % 2)
    d2 = x + 1 - 2 * (x % 2)
    out_step(late, 0)
    out_step(late + 1, 0)
    cuts = ((0, 512), (512, 896), (1408, 1152))
    pieces = len(cuts)

    def relay_copy(half, i):
        here = pl.ds(*cuts[i])
        return remote(
            ps.at[0, half, :, here], rl.at[half, :, here], rl_s, rl_r.at[half, i],
            (s, hl if half else hr),
        )

    def relay(i):
        here = pl.ds(*cuts[i])
        pair_copy(xo, *cuts[i], 4 + i).wait_recv()
        for half in range(2):
            ps[0, half, :, here] = (
                part[2 * xo + c, half, :, here].astype(F32) + pr[xo, half, :, here].astype(F32)
            ).astype(BF16)
            relay_copy(half, i).start()

    @pl.when(c == 0)
    def _():
        for i in range(pieces):
            out_part(xo, *cuts[i], 4 + i)
            if i > 0:
                relay(i - 1)
        relay(pieces - 1)
        out_step(other, 0)
        out_chip(d1)

    @pl.when(c == 1)
    def _():
        for i in range(pieces):
            out_part(xo, *cuts[i], 4 + i)
        relay(0)
        out_step(other, 0)
        relay(1)
        out_chip(d1)
        relay(2)

    lax.fori_loop(near * 3, near * 3 + 3, out_step, 0)
    out_chip(d2)

    def side_of(d):
        return jnp.where(d == xr, 0, 1)

    finals = []

    def final_send(slot, d, half):
        side = side_of(d)
        cp = remote(
            ps.at[slot, half], rf.at[side, half], rf_s, rf_r.at[side, half], (s, 2 * d + c)
        )
        cp.start()
        finals.append(cp)

    def send_direct(slot, d):
        half = 1 - side_of(d)
        pair_wait(d)
        ps[slot, half] = pair_sum(d, half).astype(BF16)
        final_send(slot, d, half)

    def send_relayed(slot, d):
        half = side_of(d)
        for i in range(pieces):
            here = pl.ds(*cuts[i])
            remote(
                ps.at[0, 0, :, here], rl.at[half, :, here], rl_s, rl_r.at[half, i], (s, hr)
            ).wait_recv()
        ps[slot, half] = (pair_sum(d, half) + rl[half].astype(F32)).astype(BF16)
        final_send(slot, d, half)

    send_direct(1, d1)
    sq_sends = []
    for k in range(8):
        col = sqc[pl.ds(pl.multiple_of(((h + k) % 8) * R, 32), Q), :]
        sqs[(h + k) % 8] = jnp.transpose(col)[0:8, :]
        if k == 0:
            sqr[h] = sqs[h]
        else:
            cp = remote(sqs.at[(h + k) % 8], sqr.at[h], sq_s, sq_r, (s, (h + k) % 8))
            cp.start()
            sq_sends.append(cp)
    send_direct(2, d2)
    send_relayed(1, d1)
    send_relayed(2, d2)
    out_chip(x)

    pair_wait(x)

    def final_wait(side, half):
        remote(
            ps.at[1, half], rf.at[side, half], rf_s, rf_r.at[side, half], (s, hl)
        ).wait_recv()

    for half in range(2):
        final_wait(1 - half, half)
        tot[half] = pair_sum(x, half) + rf[1 - half, half].astype(F32)
    await_bytes(dtr.at[pl.ds(0, 56)], sq_r)
    squares = jnp.sum(sqr[...], axis=0)[0:1, :]
    inv_row = lax.rsqrt(squares / (DL * 8) + NORM_FLOOR)
    inv_col = jnp.transpose(jnp.broadcast_to(inv_row, (Q, Q)))
    for half in range(2):
        final_wait(half, half)
        out[half * HALF : (half + 1) * HALF, :] = (
            (tot[half] + rf[half, half].astype(F32)) * inv_col[half * HALF : (half + 1) * HALF, 0:1]
        ).astype(BF16)

    await_bytes(rows.at[pl.ds(0, 7)], ag_s)
    await_bytes(part.at[pl.ds(0, 4)], pp_s)
    await_bytes(part.at[0], rl_s)
    await_bytes(part.at[pl.ds(0, 2)], rf_s)
    await_bytes(dtr.at[pl.ds(0, 56)], sq_s)

    @pl.when(s < 31)
    def _():
        halo.wait_send()

    @pl.when(c == 0)
    def _():
        await_bytes(rd.at[0], zd_s)
        await_bytes(rz.at[0], zs_s)

    @pl.when(c == 1)
    def _():
        await_bytes(dtr.at[pl.ds(0, 56)], zd_s)
        await_bytes(xb.at[pl.ds(0, 112)], zs_s)
        await_bytes(xb.at[pl.ds(0, 240)], bk_s)
        for k in range(1, NY):
            @pl.when(y + k < NY)
            def _(k=k):
                sum_copy(k).wait_send()
                sum_rate_copy(k).wait_send()


def on_device(
    tokens, pre_gain, inner_proj, outer_proj, kernel_x, kernel_bc, offset_x, offset_bc, dt_bias, a_log,
    skip_gain, norm_gain, out_proj,
):
    vm = pl.BlockSpec(memory_space=pltpu.VMEM)
    hbm = pl.BlockSpec(memory_space=pltpu.HBM)
    dma = pltpu.SemaphoreType.DMA
    V = pltpu.VMEM
    scratch = [
        V((R, D), BF16), V((D // Q, Q), F32), V((4, DL), F32), V((4, 2 * NS), F32), V((DL // Q, Q), F32),
        V((1, 2 * NS), F32), V((1, HEADS), F32), V((1, HEADS), F32), V((1, HEADS), F32), V((DL // Q, Q), F32),
        V((D, 2, DL), BF16), V((D, DL), BF16), V((D, 1024), BF16), V((384, D), BF16), V((DL, D), BF16), V((8, 2, HALF, D), BF16),
        V((T + 8, DL + 2 * NS), F32), V((T, Q), F32), V((T, DL), F32), V((T, DL), BF16),
        V((T, NS), BF16), V((T, NS), BF16), V((NQ, Q, Q), F32), V((NQ, Q, Q), F32),
        V((2 * Q, DL), BF16), V((NQ, Q, DL), F32), V((NQ, NS, DL), F32), V((NS, DL), F32),
        V((NQ, 8, DL), F32),
        V((T, DL), F32), V((NS, DL), BF16), V((8, Q), F32), V((2, NZ, 16, DL), BF16), V((2, NZ, 8, Q), F32), V((2, NZ, DL), F32),
        V((2, NZ, 16, DL), F32), V((2, NZ, 8, DL), F32), V((2, 16, DL), BF16), V((2, 8, DL), F32),
        V((NY, 2, 16, DL), BF16), V((NY, 2, 8, DL), F32), V((2, 16, DL), F32), V((2, NZ, 16, DL), BF16),
        V((NZ, 16, DL), BF16), V((T, DL), BF16), V((T + 32, Q), F32), V((8, 2, HALF, D), BF16),
        V((NX, 2, HALF, D), BF16), V((3, 2, HALF, D), BF16), V((2, HALF, D), BF16), V((2, 2, HALF, D), BF16),
        V((8, 8, Q), F32), V((8, 8, Q), F32), V((8, Q), F32), V((1, D), F32), V((1, DL), F32),
        V((1, DL), F32), V((2, HALF, D), F32),
        dma, dma((13,)), dma, dma, dma, dma((2,)), dma, dma((2,)),
        dma((NY - 1,)), dma((NY - 1,)), dma((NY - 1,)), dma((NY - 1,)), dma, dma,
        dma, dma((7,)), dma, dma((2, 3)), dma, dma((2, 2)), dma, dma,
        dma((6,)), dma((10,)),
    ]
    args = (
        tokens, pre_gain.reshape(D // Q, Q), inner_proj, outer_proj.T, kernel_x, kernel_bc,
        offset_x.reshape(DL // Q, Q), offset_bc[None], dt_bias[None], a_log[None], skip_gain[None],
        norm_gain.reshape(DL // Q, Q), out_proj,
    )
    args = [pltpu.with_memory_space_constraint(v, pltpu.HBM) for v in args]
    return pl.pallas_call(
        kernel,
        out_shape=jax.ShapeDtypeStruct((R, D), BF16),
        in_specs=[hbm] * 13,
        out_specs=vm,
        scratch_shapes=scratch,
        compiler_params=pltpu.CompilerParams(
            collective_id=0, has_side_effects=True, vmem_limit_bytes=55_000_000
        ),
    )(*args)


def solution(mesh):
    in_specs = (
        P(("seq", "head"), None), P(), P(None, None, "head"), P(), P(None, "head"), P(), P("head"), P(),
        P("head"), P("head"), P("head"), P("head"), P("head", None),
    )
    return jax.shard_map(
        on_device, mesh=mesh, in_specs=in_specs, out_specs=P(("seq", "head"), None), check_vma=False
    )
```

```python
import jax
import jax.numpy as jnp
from jax import lax
from jax.experimental import pallas as pl
from jax.experimental.pallas import tpu as pltpu
from jax.sharding import PartitionSpec as P

MESH = pl.DeviceIdType.MESH
BF16 = jnp.bfloat16
F32 = jnp.float32

NORM_FLOOR = 0.1
D = 2560
DL = 640
NS = 128
R = 96
HALF = 48
T = 768
Q = 128
NQ = 6
CH = 192
HEADS = 10
NY, NZ, NX = 4, 8, 4


def dot(a, b):
    return jnp.dot(a, b, preferred_element_type=F32)


def dot_t(a, b):
    return lax.dot_general(a, b, (((1,), (1,)), ((), ())), preferred_element_type=F32)


def t_dot(a, b):
    return lax.dot_general(a, b, (((0,), (0,)), ((), ())), preferred_element_type=F32)


def split2(v):
    hi = v.astype(BF16)
    lo = (v - hi.astype(F32)).astype(BF16)
    return hi, lo


def split3(v):
    hi, mid = split2(v)
    lo = (v - hi.astype(F32) - mid.astype(F32)).astype(BF16)
    return hi, mid, lo


def silu(v):
    half = 0.5 * v
    return half + half * jnp.tanh(half)


def remote(src, dst, send, recv, device):
    return pltpu.make_async_remote_copy(
        src_ref=src, dst_ref=dst, send_sem=send, recv_sem=recv, device_id=device, device_id_type=MESH
    )


def kernel(
    tokens_in, pre_gain_in, w_hbm, wo_hbm, kernel_x_in, kernel_bc_in, offset_x_in, offset_bc_in, dt_bias_in,
    a_log_in, skip_gain_in, norm_gain_in, wout_hbm,
    out,
    tokens, pre_gain_v, kernel_x, kernel_bc, offset_x_v, offset_bc, dt_bias, a_log, skip_gain, norm_gain_v,
    wraw, wz, wx, wo, wout, rows, xin, dtr, zs, xb, bmat, cmat, dts, cum, expand, ef, sl, sacc, pdr,
    yv, sb, drow, rz, rd, dxs, pz, pdz, tb, tdb, ty, tdy, cacc, pb, cr, gb, sqc, part, pr, ps, rl, rf,
    sqs, sqr, small, pre_gain, offset_x, norm_gain, tot,
    ag_s, ag_r, halo_s, halo_r, zs_s, zs_r, zd_s, zd_r, y_s, y_r, yd_s, yd_r, bk_s, bk_r,
    pp_s, pp_r, rl_s, rl_r, rf_s, rf_r, sq_s, sq_r, w_s, in_s,
):
    s = lax.axis_index("seq")
    h = lax.axis_index("head")
    y = s // NZ
    z = s % NZ
    x = h // 2
    c = h % 2
    partner = x * 2 + (1 - c)
    xr = (x + 1) % NX
    xl = (x + NX - 1) % NX
    xo = (x + 2) % NX
    hr, hl, ho = xr * 2 + c, xl * 2 + c, xo * 2 + c

    def await_bytes(like, sem):
        pltpu.make_async_copy(like, like, sem).wait()

    barrier = pltpu.get_barrier_semaphore()
    for k in range(1, 8):
        pl.semaphore_signal(barrier, inc=1, device_id=(s, (h + k) % 8), device_id_type=MESH)
    for k in range(1, NZ):
        pl.semaphore_signal(barrier, inc=1, device_id=(y * NZ + (z + k) % NZ, h), device_id_type=MESH)
    for k in range(1, NZ):
        pl.semaphore_signal(barrier, inc=1, device_id=(y * NZ + (z + k) % NZ, partner), device_id_type=MESH)
    for k in range(1, NY):
        pl.semaphore_signal(barrier, inc=1, device_id=(((y + k) % NY) * NZ + z, h), device_id_type=MESH)
    for k in (1, 31):
        pl.semaphore_signal(barrier, inc=1, device_id=((s + k) % 32, h), device_id_type=MESH)

    pairs = (
        (tokens_in, tokens), (pre_gain_in, pre_gain_v), (kernel_x_in, kernel_x), (kernel_bc_in, kernel_bc),
        (offset_x_in, offset_x_v), (offset_bc_in, offset_bc), (dt_bias_in, dt_bias), (a_log_in, a_log),
        (skip_gain_in, skip_gain), (norm_gain_in, norm_gain_v),
    )
    in_copies = [pltpu.make_async_copy(src, dst, in_s.at[i]) for i, (src, dst) in enumerate(pairs)]
    quarter = D // 4
    w_copies = [
        pltpu.make_async_copy(
            w_hbm.at[pl.ds(i * quarter, quarter)], wraw.at[pl.ds(i * quarter, quarter)], w_s.at[i]
        )
        for i in range(4)
    ]
    late_copies = [
        pltpu.make_async_copy(wo_hbm, wo.at[pl.ds(0, 336)], w_s.at[4]),
        pltpu.make_async_copy(wout_hbm, wout, w_s.at[5]),
    ]
    for cp in in_copies[0:2]:
        cp.start()
    for cp in in_copies[2:]:
        cp.start()
    for cp in in_copies[0:2]:
        cp.wait()
    for cp in w_copies:
        cp.start()

    def as_row(src, dst):
        for i in range(src.shape[0]):
            dst[0:1, i * Q : (i + 1) * Q] = src[i : i + 1, :]

    as_row(pre_gain_v, pre_gain)

    for half in range(2):
        tk = tokens[half * HALF : (half + 1) * HALF, :].astype(F32)
        inv = lax.rsqrt(jnp.mean(tk * tk, axis=1, keepdims=True) + NORM_FLOOR)
        rows[h, half] = (tk * inv * pre_gain[...]).astype(BF16)

    pl.semaphore_wait(barrier, 26)

    def ag(origin, half, role, device):
        return remote(
            rows.at[origin, half], rows.at[origin, half], ag_s, ag_r.at[role], (s, device)
        )

    own_pair = remote(rows.at[h], rows.at[h], ag_s, ag_r.at[6], (s, partner))
    sends = [ag(h, 0, 0, hr), ag(h, 1, 3, hl), ag(h, 1, 1, hr), ag(h, 0, 2, hl)]
    own_pair.start()
    for cp in sends:
        cp.start()

    for cp in late_copies:
        cp.start()
    for cp in in_copies[2:]:
        cp.wait()
    as_row(offset_x_v, offset_x)
    as_row(norm_gain_v, norm_gain)

    li = lax.broadcasted_iota(jnp.int32, (2 * Q, DL), 0)
    lc = lax.broadcasted_iota(jnp.int32, (2 * Q, DL), 1)
    head_of = lax.shift_right_logical(lc, 6)
    expand[...] = jnp.where(jnp.bitwise_and(li, Q - 1) == head_of, 1.0, 0.0).astype(BF16)
    small[...] = jnp.zeros_like(small)
    small[0:1, 0:HEADS] = dt_bias[...]
    small[1:2, 0:HEADS] = a_log[...]
    small[2:3, 0:HEADS] = skip_gain[...]
    pick_r = lax.broadcasted_iota(jnp.int32, (2 * Q, 2 * Q), 0)
    pick_c = lax.broadcasted_iota(jnp.int32, (2 * Q, 2 * Q), 1)
    pick_t = jnp.where(pick_r < Q, 2 * pick_r, 2 * (pick_r - Q) + 1)
    pick = jnp.where(pick_c == pick_t, 1.0, 0.0).astype(BF16)
    wflat = wraw.reshape(2 * D, DL)

    def split_step(i, carry):
        v = wflat[pl.ds(pl.multiple_of(i * 2 * Q, 2 * Q), 2 * Q), :]
        r = dot(pick, v).astype(BF16)
        wz[pl.ds(pl.multiple_of(i * Q, Q), Q), :] = r[0:Q, :]
        wx[pl.ds(pl.multiple_of(i * Q, Q), Q), 0:DL] = r[Q : 2 * Q, :]
        return carry

    for i in range(4):
        w_copies[i].wait()
        lax.fori_loop(i * quarter // Q, (i + 1) * quarter // Q, split_step, 0)
    for cp in late_copies:
        cp.wait()

    wo[336:384, :] = jnp.zeros((48, D), BF16)
    same = jnp.where(pick_r == pick_c, 1.0, 0.0).astype(BF16)
    for i in range(D // (2 * Q)):
        at = slice(i * 2 * Q, (i + 1) * 2 * Q)
        wx[at, DL:] = dot_t(same, wo[:, at]).astype(BF16)

    def put_rows(n, places):
        r = dot(n, wx[...])
        for at, lo, hi in places:
            xin[pl.ds(pl.multiple_of(at + 8, 8), hi - lo), :] = r[lo:hi, 0 : DL + 2 * NS].astype(BF16).astype(F32)
            dtr[pl.ds(pl.multiple_of(at, 8), hi - lo), :] = r[lo:hi, DL + 2 * NS :]

    def project_x(chip):
        n = rows[pl.ds(2 * chip, 2)].reshape(CH, D)
        put_rows(n, [(chip * CH, 0, CH)])

    def project_halves(chip_a, half_a, chip_b, half_b):
        n = jnp.concatenate(
            [rows[pl.ds(2 * chip_a, 2), half_a].reshape(R, D), rows[pl.ds(2 * chip_b, 2), half_b].reshape(R, D)],
            axis=0,
        )
        places = []
        for i, (chip, half) in enumerate(((chip_a, half_a), (chip_b, half_b))):
            for core in range(2):
                lo = i * R + core * HALF
                places.append((chip * CH + core * R + half * HALF, lo, lo + HALF))
        put_rows(n, places)

    def project_z(chip):
        n = rows[pl.ds(2 * chip, 2)].reshape(CH, D)
        zs[pl.ds(pl.multiple_of(chip * CH, CH), CH), :] = silu(dot(n, wz[...]).astype(BF16).astype(F32))

    def to_partner(origin, half, role):
        cp = ag(origin, half, 7 + role, partner)
        cp.start()
        sends.append(cp)

    def partner_done(chip, half, role):
        ag(chip * 2 + 1 - c, half, 7 + role, partner).wait_recv()

    def onward(origin, half, role, device):
        cp = ag(origin, half, role, device)
        cp.start()
        sends.append(cp)

    lane = lax.broadcasted_iota(jnp.int32, (1, Q), 1)
    ri = lax.broadcasted_iota(jnp.int32, (Q, Q), 0)
    ci = lax.broadcasted_iota(jnp.int32, (Q, Q), 1)
    tri = jnp.where(ri >= ci, 1.0, 0.0).astype(BF16)
    shift = (Q - h * HEADS) % Q

    def step_sizes(q):
        raw = pltpu.roll(dtr[pl.ds(pl.multiple_of(q * Q, Q), Q), :], shift, 1) + small[0:1, :]
        step = jnp.maximum(raw, 0.0) + jnp.log1p(jnp.exp(-jnp.abs(raw)))
        step = jnp.where(lane < HEADS, step, 0.0)
        la = step * -jnp.exp(small[1:2, :])
        dts[q] = step
        p3 = dot(tri, jnp.concatenate(split3(la), axis=1))
        cum[q] = p3[:, 0:Q] + p3[:, Q : 2 * Q] + p3[:, 2 * Q : 3 * Q]

    def conv_block(i):
        at = pl.multiple_of(i * 64, 64)
        for j in range((DL + 2 * NS) // Q):
            kern, off, lo = (kernel_x, offset_x, j * Q) if j < 5 else (kernel_bc, offset_bc, (j - 5) * Q)
            v = xin[pl.ds(at, 72), j * Q : (j + 1) * Q]
            u = kern[0:1, lo : lo + Q] * v
            for k in range(1, 4):
                u = pltpu.roll(u, 1, 0) + kern[k : k + 1, lo : lo + Q] * v
            v = silu(u[8:72, :] + off[:, lo : lo + Q]).astype(BF16)
            if j < 5:
                xb[pl.ds(at, 64), lo : lo + Q] = v
            else:
                (bmat, cmat)[j - 5][pl.ds(at, 64), :] = v

    def chunk_state(q):
        at = pl.multiple_of(q * Q, Q)
        cq = cum[q]
        fac = jnp.exp(cq[Q - 1 : Q, :] - cq) * dts[q]
        fx = dot(jnp.concatenate(split2(fac), axis=1), expand[...])
        xw = (xb[pl.ds(at, Q), :].astype(F32) * fx).astype(BF16)
        sl[q] = t_dot(bmat[pl.ds(at, Q), :], xw)

    far = xo // 2
    near = 1 - far
    odd = xo % 2
    late = 3 * far + odd
    other = 3 * far + 2 - 2 * odd

    def conv_early(i, carry):
        chip = (x + 3 + i // 3) % NX
        block = 3 * chip + i % 3
        block = jnp.where(jnp.logical_or(block == 0, i == 0), block + 1, block)
        conv_block(block)
        return carry

    remote(rows.at[partner], rows.at[partner], ag_s, ag_r.at[6], (s, partner)).wait_recv()
    ag(hl, 0, 0, hr).wait_recv()
    onward(hl, 0, 4, hr)
    ag(hr, 1, 3, hl).wait_recv()
    onward(hr, 1, 5, hl)
    to_partner(hl, 0, 0)
    to_partner(hr, 1, 3)
    project_x(x)
    partner_done(xl, 0, 0)
    partner_done(xr, 1, 3)
    project_halves(xl, 0, xr, 1)
    ag(hl, 1, 1, hr).wait_recv()
    to_partner(hl, 1, 1)
    ag(hr, 0, 2, hl).wait_recv()
    to_partner(hr, 0, 2)

    @pl.when(c == 0)
    def _():
        partner_done(xl, 1, 1)
        partner_done(xr, 0, 2)

    def put_seconds(core):
        n = jnp.concatenate([rows[2 * xl + core, 1], rows[2 * xr + core, 0]], axis=0)
        put_rows(
            n,
            [(xl * CH + core * R + HALF, 0, HALF), (xr * CH + core * R, HALF, R)],
        )

    put_seconds(1)
    lax.fori_loop(4, 6, conv_early, 0)

    @pl.when(c == 1)
    def _():
        partner_done(xl, 1, 1)
        partner_done(xr, 0, 2)

    put_seconds(0)

    def opposite_in():
        ag(ho, 0, 4, hr).wait_recv()
        ag(ho, 0, 11, partner).start()
        ag(ho, 1, 5, hl).wait_recv()
        ag(ho, 1, 12, partner).start()

    @pl.when(c == 1)
    def _():
        opposite_in()

    for q in (3 * near, 3 * near + 1, 3 * near + 2, other):
        step_sizes(q)
    lax.fori_loop(1, 4, conv_early, 0)
    lax.fori_loop(6, 8, conv_early, 0)

    @pl.when(c == 0)
    def _():
        opposite_in()

    lax.fori_loop(8, 9, conv_early, 0)
    chunk_state(3 * near + 1)
    chunk_state(3 * near + 2)
    partner_done(xo, 0, 4)
    partner_done(xo, 1, 5)
    project_x(xo)

    halo = remote(xin.at[pl.ds(T, 8)], xin.at[pl.ds(0, 8)], halo_s, halo_r, ((s + 1) % 32, h))

    @pl.when(s < 31)
    def _():
        halo.start()

    step_sizes(late)
    step_sizes(late + 1)
    total = cum[0][Q - 1 : Q, :]
    for q in range(1, NQ):
        total = total + cum[q][Q - 1 : Q, :]
    drow[...] = jnp.broadcast_to(jnp.exp(total), (8, Q))

    owner = 2 * x + 1
    far_first = (4, 3, 5, 2, 6, 1, 7)

    def z_peer(k):
        return (z + k) % NZ

    def rate_copy(k):
        return remote(
            drow, rd.at[c, z], zd_s, zd_r.at[c], (y * NZ + z_peer(k), owner)
        )

    def state_copy(k):
        at = pl.multiple_of(z_peer(k) * 16, 16)
        return remote(
            sb.at[pl.ds(at, 16)], rz.at[c, z], zs_s, zs_r.at[c], (y * NZ + z_peer(k), owner)
        )

    def sum_copy(k):
        return remote(tb, ty.at[y], y_s.at[k - 1], y_r.at[y], ((y + k) % NY * NZ + z, h))

    def sum_rate_copy(k):
        return remote(tdb, tdy.at[y], yd_s.at[k - 1], yd_r.at[y], ((y + k) % NY * NZ + z, h))

    def back_copy(g, k):
        zp = z_peer(k)
        return remote(pb.at[g, zp], cr.at[z], bk_s, bk_r, (y * NZ + zp, 2 * x + g))

    for k in range(1, NZ):
        rate_copy(k).start()

    @pl.when(c == 0)
    def _():
        rate_copy(0).start()

    @pl.when(c == 1)
    def _():
        rd[1, z] = drow[...]

    conv_block(3 * xo + 1)
    conv_block(3 * xo + 2)
    conv_block(jnp.where(xo == 0, 3 * xl, 3 * xo))
    conv_block(jnp.where(xl == 0, 3 * xo, 3 * xl))

    rest = jnp.where(near == 0, 3, 1)
    for k in range(3):
        chunk_state(rest + k)

    ends = jnp.concatenate([cum[q][Q - 1 : Q, :] for q in range(NQ)] + [jnp.zeros((2, Q), F32)], axis=0)
    decs = dot(jnp.concatenate(split2(jnp.exp(ends)), axis=1), expand[...])
    for lo in range(0, DL, Q):
        acc = sl[1, :, lo : lo + Q]
        for q in range(2, NQ):
            acc = acc * decs[q : q + 1, lo : lo + Q] + sl[q, :, lo : lo + Q]
        sacc[:, lo : lo + Q] = acc

    @pl.when(s == 0)
    def _():
        xin[0:8, :] = jnp.zeros((8, DL + 2 * NS), F32)

    @pl.when(s > 0)
    def _():
        halo.wait_recv()

    conv_block(0)
    chunk_state(0)
    later = decs[1:2, :]
    for q in range(2, NQ):
        later = later * decs[q : q + 1, :]
    sb[...] = (sacc[...] + later * sl[0]).astype(BF16)

    for k in far_first:
        state_copy(k).start()

    @pl.when(c == 0)
    def _():
        state_copy(0).start()

    @pl.when(c == 1)
    def _():
        rz[1, z] = sb[pl.ds(pl.multiple_of(z * 16, 16), 16), :]

    for lo in range(0, DL, Q):
        acc = jnp.zeros((NS, Q), F32)
        pd = jnp.ones((1, Q), F32)
        for q in range(NQ):
            st = sl[q, :, lo : lo + Q]
            dec = decs[q : q + 1, lo : lo + Q]
            sl[q, :, lo : lo + Q] = acc
            pdr[q, 0:1, lo : lo + Q] = pd
            acc = acc * dec + st
            pd = pd * dec

    project_z(xo)
    s3 = jnp.concatenate(split2(jnp.broadcast_to(small[2:3, :], (8, Q))), axis=1)
    skip_row = dot(s3, expand[...])[0:1, :]
    low = lax.broadcasted_iota(jnp.int32, (Q, Q), 1) < 64

    def intra_step(q, carry):
        at = pl.multiple_of(q * Q, Q)
        cq = cum[q]
        ef[q] = dot(jnp.concatenate(split2(jnp.exp(cq)), axis=1), expand[...])
        cqt = jnp.transpose(cq)
        dtt = jnp.transpose(dts[q])
        cb = dot_t(cmat[pl.ds(at, Q), :], bmat[pl.ds(at, Q), :])
        cbm = jnp.where(ri >= ci, cb, 0.0)
        for j in range(HEADS // 2):
            mixes = []
            for hh in (2 * j, 2 * j + 1):
                gap = jnp.minimum(cq[:, hh : hh + 1] - cqt[hh : hh + 1, :], 0.0)
                mixes.append((cbm * jnp.exp(gap) * dtt[hh : hh + 1, :]).astype(BF16))
            xp = xb[pl.ds(at, Q), j * Q : (j + 1) * Q].astype(F32)
            xd = jnp.concatenate(
                [jnp.where(low, xp, 0.0).astype(BF16), jnp.where(low, 0.0, xp).astype(BF16)], axis=0
            )
            yq = dot(jnp.concatenate(mixes, axis=1), xd)
            yv[pl.ds(at, Q), j * Q : (j + 1) * Q] = yq + skip_row[:, j * Q : (j + 1) * Q] * xp
        return carry

    lax.fori_loop(0, NQ, intra_step, 0)

    @pl.when(c == 1)
    def _():
        for g in (1, 0):
            if g == 1:
                await_bytes(dtr.at[pl.ds(0, 56)], zd_r.at[1])
            else:
                await_bytes(rd.at[0], zd_r.at[0])
            dz = jnp.concatenate([rd[g, k][0:1, :] for k in range(NZ)], axis=0)
            dx = dot(jnp.concatenate(split2(dz), axis=1), expand[...])
            dxs[g] = dx
            pd = jnp.ones((1, DL), F32)
            for k in range(NZ):
                pdz[g, k] = jnp.broadcast_to(pd, (8, DL))
                pd = pd * dx[k : k + 1, :]
            tdb[g] = jnp.broadcast_to(pd, (8, DL))
        for k in range(1, NY):
            @pl.when(y + k < NY)
            def _(k=k):
                sum_rate_copy(k).start()

    project_z(xl)

    @pl.when(c == 1)
    def _():
        for g in (1, 0):
            if g == 1:
                await_bytes(xb.at[pl.ds(0, 112)], zs_r.at[1])
            else:
                await_bytes(rz.at[0], zs_r.at[0])
            dx = dxs[g]
            acc = jnp.zeros((16, DL), F32)
            for k in range(NZ):
                pz[g, k] = acc
                acc = acc * dx[k : k + 1, :] + rz[g, k].astype(F32)
            tb[g] = acc.astype(BF16)
        for k in (2, 1, 3):
            @pl.when(y + k < NY)
            def _(k=k):
                sum_copy(k).start()


    @pl.when(c == 1)
    def _():
        cacc[...] = jnp.zeros_like(cacc)
        for k in range(NY - 1):
            @pl.when(k < y)
            def _(k=k):
                dev = (k * NZ + z, h)
                remote(tb, ty.at[k], y_s.at[0], y_r.at[k], dev).wait_recv()
                remote(tdb, tdy.at[k], yd_s.at[0], yd_r.at[k], dev).wait_recv()
                for g in range(2):
                    cacc[g] = cacc[g] * tdy[k, g][0:1, :] + ty[k, g].astype(F32)
        for g in range(2):
            for k in range(NZ):
                pb[g, k] = (pz[g, k] + pdz[g, k][0:1, :] * cacc[g]).astype(BF16)
        for k in far_first:
            for g in range(2):
                back_copy(g, k).start()
        back_copy(0, 0).start()
        cr[z] = pb[1, z]

    project_z(x)
    project_z(xr)

    @pl.when(c == 1)
    def _():
        await_bytes(xb.at[pl.ds(0, 112)], bk_r)

    @pl.when(c == 0)
    def _():
        await_bytes(cr, bk_r)

    def out_step(q, carry):
        at = pl.multiple_of(q * Q, Q)
        state = (sl[q] + pdr[q][0:1, :] * cr[...].reshape(NS, DL).astype(F32)).astype(BF16)
        cross = dot(cmat[pl.ds(at, Q), :], state)
        g = (yv[pl.ds(at, Q), :] + ef[q] * cross) * zs[pl.ds(at, Q), :]
        sqc[pl.ds(at, Q), :] = jnp.broadcast_to(jnp.sum(g * g, axis=1, keepdims=True), (Q, Q))
        gb[pl.ds(at, Q), :] = (g * norm_gain[...]).astype(BF16)
        return carry

    def pair_copy(d, lo, width, sem):
        return remote(
            part.at[2 * d + 1 - c, :, :, pl.ds(lo, width)], pr.at[d, :, :, pl.ds(lo, width)],
            pp_s, pp_r.at[sem], (s, partner),
        )

    def out_part(d, lo, width, sem):
        n = gb[pl.ds(pl.multiple_of(d * CH, CH), CH), :]
        for at in range(lo, lo + width, 256):
            end = min(at + 256, lo + width)
            part[pl.ds(2 * d, 2), :, :, at:end] = (
                dot(n, wout[:, at:end]).astype(BF16).reshape(2, 2, HALF, end - at)
            )
        pair_copy(d, lo, width, sem).start()

    def out_chip(d):
        out_part(d, 0, D, d)

    def pair_sum(d, half):
        return part[2 * d + c, half].astype(F32) + pr[d, half].astype(F32)

    def pair_wait(d):
        remote(part.at[0], pr.at[d], pp_s, pp_r.at[d], (s, partner)).wait_recv()

    d1 = xo + 1 - 2 * (xo % 2)
    d2 = x + 1 - 2 * (x % 2)
    out_step(late, 0)
    out_step(late + 1, 0)
    cuts = ((0, 512), (512, 896), (1408, 1152))
    pieces = len(cuts)

    def relay_copy(half, i):
        here = pl.ds(*cuts[i])
        return remote(
            ps.at[0, half, :, here], rl.at[half, :, here], rl_s, rl_r.at[half, i],
            (s, hl if half else hr),
        )

    def relay(i):
        here = pl.ds(*cuts[i])
        pair_copy(xo, *cuts[i], 4 + i).wait_recv()
        for half in range(2):
            ps[0, half, :, here] = (
                part[2 * xo + c, half, :, here].astype(F32) + pr[xo, half, :, here].astype(F32)
            ).astype(BF16)
            relay_copy(half, i).start()

    @pl.when(c == 0)
    def _():
        for i in range(pieces):
            out_part(xo, *cuts[i], 4 + i)
            if i > 0:
                relay(i - 1)
        relay(pieces - 1)
        out_step(other, 0)
        out_chip(d1)

    @pl.when(c == 1)
    def _():
        for i in range(pieces):
            out_part(xo, *cuts[i], 4 + i)
        relay(0)
        out_step(other, 0)
        relay(1)
        out_chip(d1)
        relay(2)

    lax.fori_loop(near * 3, near * 3 + 3, out_step, 0)
    out_chip(d2)

    def side_of(d):
        return jnp.where(d == xr, 0, 1)

    finals = []

    def final_send(slot, d, half):
        side = side_of(d)
        cp = remote(
            ps.at[slot, half], rf.at[side, half], rf_s, rf_r.at[side, half], (s, 2 * d + c)
        )
        cp.start()
        finals.append(cp)

    def send_direct(slot, d):
        half = 1 - side_of(d)
        pair_wait(d)
        ps[slot, half] = pair_sum(d, half).astype(BF16)
        final_send(slot, d, half)

    def send_relayed(slot, d):
        half = side_of(d)
        for i in range(pieces):
            here = pl.ds(*cuts[i])
            remote(
                ps.at[0, 0, :, here], rl.at[half, :, here], rl_s, rl_r.at[half, i], (s, hr)
            ).wait_recv()
        ps[slot, half] = (pair_sum(d, half) + rl[half].astype(F32)).astype(BF16)
        final_send(slot, d, half)

    send_direct(1, d1)
    sq_sends = []
    for k in range(8):
        col = sqc[pl.ds(pl.multiple_of(((h + k) % 8) * R, 32), Q), :]
        sqs[(h + k) % 8] = jnp.transpose(col)[0:8, :]
        if k == 0:
            sqr[h] = sqs[h]
        else:
            cp = remote(sqs.at[(h + k) % 8], sqr.at[h], sq_s, sq_r, (s, (h + k) % 8))
            cp.start()
            sq_sends.append(cp)
    send_direct(2, d2)
    send_relayed(1, d1)
    send_relayed(2, d2)
    out_chip(x)

    pair_wait(x)

    def final_wait(side, half):
        remote(
            ps.at[1, half], rf.at[side, half], rf_s, rf_r.at[side, half], (s, hl)
        ).wait_recv()

    for half in range(2):
        final_wait(1 - half, half)
        tot[half] = pair_sum(x, half) + rf[1 - half, half].astype(F32)
    await_bytes(dtr.at[pl.ds(0, 56)], sq_r)
    squares = jnp.sum(sqr[...], axis=0)[0:1, :]
    inv_row = lax.rsqrt(squares / (DL * 8) + NORM_FLOOR)
    inv_col = jnp.transpose(jnp.broadcast_to(inv_row, (Q, Q)))
    for half in range(2):
        final_wait(half, half)
        out[half * HALF : (half + 1) * HALF, :] = (
            (tot[half] + rf[half, half].astype(F32)) * inv_col[half * HALF : (half + 1) * HALF, 0:1]
        ).astype(BF16)

    await_bytes(rows.at[pl.ds(0, 7)], ag_s)
    await_bytes(part.at[pl.ds(0, 4)], pp_s)
    await_bytes(part.at[0], rl_s)
    await_bytes(part.at[pl.ds(0, 2)], rf_s)
    await_bytes(dtr.at[pl.ds(0, 56)], sq_s)

    @pl.when(s < 31)
    def _():
        halo.wait_send()

    @pl.when(c == 0)
    def _():
        await_bytes(rd.at[0], zd_s)
        await_bytes(rz.at[0], zs_s)

    @pl.when(c == 1)
    def _():
        await_bytes(dtr.at[pl.ds(0, 56)], zd_s)
        await_bytes(xb.at[pl.ds(0, 112)], zs_s)
        await_bytes(xb.at[pl.ds(0, 240)], bk_s)
        for k in range(1, NY):
            @pl.when(y + k < NY)
            def _(k=k):
                sum_copy(k).wait_send()
                sum_rate_copy(k).wait_send()


def on_device(
    tokens, pre_gain, inner_proj, outer_proj, kernel_x, kernel_bc, offset_x, offset_bc, dt_bias, a_log,
    skip_gain, norm_gain, out_proj,
):
    vm = pl.BlockSpec(memory_space=pltpu.VMEM)
    hbm = pl.BlockSpec(memory_space=pltpu.HBM)
    dma = pltpu.SemaphoreType.DMA
    V = pltpu.VMEM
    scratch = [
        V((R, D), BF16), V((D // Q, Q), F32), V((4, DL), F32), V((4, 2 * NS), F32), V((DL // Q, Q), F32),
        V((1, 2 * NS), F32), V((1, HEADS), F32), V((1, HEADS), F32), V((1, HEADS), F32), V((DL // Q, Q), F32),
        V((D, 2, DL), BF16), V((D, DL), BF16), V((D, 1024), BF16), V((384, D), BF16), V((DL, D), BF16), V((8, 2, HALF, D), BF16),
        V((T + 8, DL + 2 * NS), F32), V((T, Q), F32), V((T, DL), F32), V((T, DL), BF16),
        V((T, NS), BF16), V((T, NS), BF16), V((NQ, Q, Q), F32), V((NQ, Q, Q), F32),
        V((2 * Q, DL), BF16), V((NQ, Q, DL), F32), V((NQ, NS, DL), F32), V((NS, DL), F32),
        V((NQ, 8, DL), F32),
        V((T, DL), F32), V((NS, DL), BF16), V((8, Q), F32), V((2, NZ, 16, DL), BF16), V((2, NZ, 8, Q), F32), V((2, NZ, DL), F32),
        V((2, NZ, 16, DL), F32), V((2, NZ, 8, DL), F32), V((2, 16, DL), BF16), V((2, 8, DL), F32),
        V((NY, 2, 16, DL), BF16), V((NY, 2, 8, DL), F32), V((2, 16, DL), F32), V((2, NZ, 16, DL), BF16),
        V((NZ, 16, DL), BF16), V((T, DL), BF16), V((T + 32, Q), F32), V((8, 2, HALF, D), BF16),
        V((NX, 2, HALF, D), BF16), V((3, 2, HALF, D), BF16), V((2, HALF, D), BF16), V((2, 2, HALF, D), BF16),
        V((8, 8, Q), F32), V((8, 8, Q), F32), V((8, Q), F32), V((1, D), F32), V((1, DL), F32),
        V((1, DL), F32), V((2, HALF, D), F32),
        dma, dma((13,)), dma, dma, dma, dma((2,)), dma, dma((2,)),
        dma((NY - 1,)), dma((NY - 1,)), dma((NY - 1,)), dma((NY - 1,)), dma, dma,
        dma, dma((7,)), dma, dma((2, 3)), dma, dma((2, 2)), dma, dma,
        dma((6,)), dma((10,)),
    ]
    args = (
        tokens, pre_gain.reshape(D // Q, Q), inner_proj, outer_proj.T, kernel_x, kernel_bc,
        offset_x.reshape(DL // Q, Q), offset_bc[None], dt_bias[None], a_log[None], skip_gain[None],
        norm_gain.reshape(DL // Q, Q), out_proj,
    )
    args = [pltpu.with_memory_space_constraint(v, pltpu.HBM) for v in args]
    return pl.pallas_call(
        kernel,
        out_shape=jax.ShapeDtypeStruct((R, D), BF16),
        in_specs=[hbm] * 13,
        out_specs=vm,
        scratch_shapes=scratch,
        compiler_params=pltpu.CompilerParams(
            collective_id=0, has_side_effects=True, vmem_limit_bytes=55_000_000
        ),
    )(*args)


def solution(mesh):
    in_specs = (
        P(("seq", "head"), None), P(), P(None, None, "head"), P(), P(None, "head"), P(), P("head"), P(),
        P("head"), P("head"), P("head"), P("head"), P("head", None),
    )
    return jax.shard_map(
        on_device, mesh=mesh, in_specs=in_specs, out_specs=P(("seq", "head"), None), check_vma=False
    )
```

```python
import jax
import jax.numpy as jnp
from jax import lax
from jax.experimental import pallas as pl
from jax.experimental.pallas import tpu as pltpu
from jax.sharding import PartitionSpec as P

MESH = pl.DeviceIdType.MESH
BF16 = jnp.bfloat16
F32 = jnp.float32

NORM_FLOOR = 0.1
D = 2560
DL = 640
NS = 128
R = 96
HALF = 48
T = 768
Q = 128
NQ = 6
CH = 192
HEADS = 10
NY, NZ, NX = 4, 8, 4


def dot(a, b):
    return jnp.dot(a, b, preferred_element_type=F32)


def dot_t(a, b):
    return lax.dot_general(a, b, (((1,), (1,)), ((), ())), preferred_element_type=F32)


def t_dot(a, b):
    return lax.dot_general(a, b, (((0,), (0,)), ((), ())), preferred_element_type=F32)


def split2(v):
    hi = v.astype(BF16)
    lo = (v - hi.astype(F32)).astype(BF16)
    return hi, lo


def split3(v):
    hi, mid = split2(v)
    lo = (v - hi.astype(F32) - mid.astype(F32)).astype(BF16)
    return hi, mid, lo


def silu(v):
    half = 0.5 * v
    return half + half * jnp.tanh(half)


def remote(src, dst, send, recv, device):
    return pltpu.make_async_remote_copy(
        src_ref=src, dst_ref=dst, send_sem=send, recv_sem=recv, device_id=device, device_id_type=MESH
    )


def kernel(
    tokens_in, pre_gain_in, w_hbm, wo_hbm, kernel_x_in, kernel_bc_in, offset_x_in, offset_bc_in, dt_bias_in,
    a_log_in, skip_gain_in, norm_gain_in, wout_hbm,
    out,
    tokens, pre_gain_v, kernel_x, kernel_bc, offset_x_v, offset_bc, dt_bias, a_log, skip_gain, norm_gain_v,
    wraw, wz, wx, wo, wout, rows, xin, dtr, zs, xb, bmat, cmat, dts, cum, expand, ef, sl, sacc, pdr,
    yv, sb, drow, rz, rd, dxs, pz, pdz, tb, tdb, ty, tdy, cacc, pb, cr, gb, sqc, part, pr, ps, rl, rf,
    sqs, sqr, small, pre_gain, offset_x, norm_gain, tot,
    ag_s, ag_r, halo_s, halo_r, zs_s, zs_r, zd_s, zd_r, y_s, y_r, yd_s, yd_r, bk_s, bk_r,
    pp_s, pp_r, rl_s, rl_r, rf_s, rf_r, sq_s, sq_r, w_s, in_s,
):
    s = lax.axis_index("seq")
    h = lax.axis_index("head")
    y = s // NZ
    z = s % NZ
    x = h // 2
    c = h % 2
    partner = x * 2 + (1 - c)
    xr = (x + 1) % NX
    xl = (x + NX - 1) % NX
    xo = (x + 2) % NX
    hr, hl, ho = xr * 2 + c, xl * 2 + c, xo * 2 + c

    def await_bytes(like, sem):
        pltpu.make_async_copy(like, like, sem).wait()

    barrier = pltpu.get_barrier_semaphore()
    for k in range(1, 8):
        pl.semaphore_signal(barrier, inc=1, device_id=(s, (h + k) % 8), device_id_type=MESH)
    for k in range(1, NZ):
        pl.semaphore_signal(barrier, inc=1, device_id=(y * NZ + (z + k) % NZ, h), device_id_type=MESH)
    for k in range(1, NZ):
        pl.semaphore_signal(barrier, inc=1, device_id=(y * NZ + (z + k) % NZ, partner), device_id_type=MESH)
    for k in range(1, NY):
        pl.semaphore_signal(barrier, inc=1, device_id=(((y + k) % NY) * NZ + z, h), device_id_type=MESH)
    for k in (1, 31):
        pl.semaphore_signal(barrier, inc=1, device_id=((s + k) % 32, h), device_id_type=MESH)

    pairs = (
        (tokens_in, tokens), (pre_gain_in, pre_gain_v), (kernel_x_in, kernel_x), (kernel_bc_in, kernel_bc),
        (offset_x_in, offset_x_v), (offset_bc_in, offset_bc), (dt_bias_in, dt_bias), (a_log_in, a_log),
        (skip_gain_in, skip_gain), (norm_gain_in, norm_gain_v),
    )
    in_copies = [pltpu.make_async_copy(src, dst, in_s.at[i]) for i, (src, dst) in enumerate(pairs)]
    quarter = D // 4
    w_copies = [
        pltpu.make_async_copy(
            w_hbm.at[pl.ds(i * quarter, quarter)], wraw.at[pl.ds(i * quarter, quarter)], w_s.at[i]
        )
        for i in range(4)
    ]
    late_copies = [
        pltpu.make_async_copy(wo_hbm, wo.at[pl.ds(0, 336)], w_s.at[4]),
        pltpu.make_async_copy(wout_hbm, wout, w_s.at[5]),
    ]
    for cp in in_copies[0:2]:
        cp.start()
    for cp in in_copies[2:]:
        cp.start()
    for cp in in_copies[0:2]:
        cp.wait()
    for cp in w_copies:
        cp.start()

    def as_row(src, dst):
        for i in range(src.shape[0]):
            dst[0:1, i * Q : (i + 1) * Q] = src[i : i + 1, :]

    as_row(pre_gain_v, pre_gain)

    for half in range(2):
        tk = tokens[half * HALF : (half + 1) * HALF, :].astype(F32)
        inv = lax.rsqrt(jnp.mean(tk * tk, axis=1, keepdims=True) + NORM_FLOOR)
        rows[h, half] = (tk * inv * pre_gain[...]).astype(BF16)

    pl.semaphore_wait(barrier, 26)

    def ag(origin, half, role, device):
        return remote(
            rows.at[origin, half], rows.at[origin, half], ag_s, ag_r.at[role], (s, device)
        )

    own_pair = remote(rows.at[h], rows.at[h], ag_s, ag_r.at[6], (s, partner))
    sends = [ag(h, 0, 0, hr), ag(h, 1, 3, hl), ag(h, 1, 1, hr), ag(h, 0, 2, hl)]
    own_pair.start()
    for cp in sends:
        cp.start()

    for cp in late_copies:
        cp.start()
    for cp in in_copies[2:]:
        cp.wait()
    as_row(offset_x_v, offset_x)
    as_row(norm_gain_v, norm_gain)

    li = lax.broadcasted_iota(jnp.int32, (2 * Q, DL), 0)
    lc = lax.broadcasted_iota(jnp.int32, (2 * Q, DL), 1)
    head_of = lax.shift_right_logical(lc, 6)
    expand[...] = jnp.where(jnp.bitwise_and(li, Q - 1) == head_of, 1.0, 0.0).astype(BF16)
    small[...] = jnp.zeros_like(small)
    small[0:1, 0:HEADS] = dt_bias[...]
    small[1:2, 0:HEADS] = a_log[...]
    small[2:3, 0:HEADS] = skip_gain[...]
    pick_r = lax.broadcasted_iota(jnp.int32, (2 * Q, 2 * Q), 0)
    pick_c = lax.broadcasted_iota(jnp.int32, (2 * Q, 2 * Q), 1)
    pick_t = jnp.where(pick_r < Q, 2 * pick_r, 2 * (pick_r - Q) + 1)
    pick = jnp.where(pick_c == pick_t, 1.0, 0.0).astype(BF16)
    wflat = wraw.reshape(2 * D, DL)

    def split_step(i, carry):
        v = wflat[pl.ds(pl.multiple_of(i * 2 * Q, 2 * Q), 2 * Q), :]
        r = dot(pick, v).astype(BF16)
        wz[pl.ds(pl.multiple_of(i * Q, Q), Q), :] = r[0:Q, :]
        wx[pl.ds(pl.multiple_of(i * Q, Q), Q), 0:DL] = r[Q : 2 * Q, :]
        return carry

    for i in range(4):
        w_copies[i].wait()
        lax.fori_loop(i * quarter // Q, (i + 1) * quarter // Q, split_step, 0)
    for cp in late_copies:
        cp.wait()

    wo[336:384, :] = jnp.zeros((48, D), BF16)
    same = jnp.where(pick_r == pick_c, 1.0, 0.0).astype(BF16)
    for i in range(D // (2 * Q)):
        at = slice(i * 2 * Q, (i + 1) * 2 * Q)
        wx[at, DL:] = dot_t(same, wo[:, at]).astype(BF16)

    def put_rows(n, places):
        r = dot(n, wx[...])
        for at, lo, hi in places:
            xin[pl.ds(pl.multiple_of(at + 8, 8), hi - lo), :] = r[lo:hi, 0 : DL + 2 * NS].astype(BF16).astype(F32)
            dtr[pl.ds(pl.multiple_of(at, 8), hi - lo), :] = r[lo:hi, DL + 2 * NS :]

    def project_x(chip):
        n = rows[pl.ds(2 * chip, 2)].reshape(CH, D)
        put_rows(n, [(chip * CH, 0, CH)])

    def project_halves(chip_a, half_a, chip_b, half_b):
        n = jnp.concatenate(
            [rows[pl.ds(2 * chip_a, 2), half_a].reshape(R, D), rows[pl.ds(2 * chip_b, 2), half_b].reshape(R, D)],
            axis=0,
        )
        places = []
        for i, (chip, half) in enumerate(((chip_a, half_a), (chip_b, half_b))):
            for core in range(2):
                lo = i * R + core * HALF
                places.append((chip * CH + core * R + half * HALF, lo, lo + HALF))
        put_rows(n, places)

    def project_z(chip):
        n = rows[pl.ds(2 * chip, 2)].reshape(CH, D)
        zs[pl.ds(pl.multiple_of(chip * CH, CH), CH), :] = silu(dot(n, wz[...]).astype(BF16).astype(F32))

    def to_partner(origin, half, role):
        cp = ag(origin, half, 7 + role, partner)
        cp.start()
        sends.append(cp)

    def partner_done(chip, half, role):
        ag(chip * 2 + 1 - c, half, 7 + role, partner).wait_recv()

    def onward(origin, half, role, device):
        cp = ag(origin, half, role, device)
        cp.start()
        sends.append(cp)

    lane = lax.broadcasted_iota(jnp.int32, (1, Q), 1)
    ri = lax.broadcasted_iota(jnp.int32, (Q, Q), 0)
    ci = lax.broadcasted_iota(jnp.int32, (Q, Q), 1)
    tri = jnp.where(ri >= ci, 1.0, 0.0).astype(BF16)
    shift = (Q - h * HEADS) % Q

    def step_sizes(q):
        raw = pltpu.roll(dtr[pl.ds(pl.multiple_of(q * Q, Q), Q), :], shift, 1) + small[0:1, :]
        step = jnp.maximum(raw, 0.0) + jnp.log1p(jnp.exp(-jnp.abs(raw)))
        step = jnp.where(lane < HEADS, step, 0.0)
        la = step * -jnp.exp(small[1:2, :])
        dts[q] = step
        p3 = dot(tri, jnp.concatenate(split3(la), axis=1))
        cum[q] = p3[:, 0:Q] + p3[:, Q : 2 * Q] + p3[:, 2 * Q : 3 * Q]

    def conv_block(i):
        at = pl.multiple_of(i * 64, 64)
        for j in range((DL + 2 * NS) // Q):
            kern, off, lo = (kernel_x, offset_x, j * Q) if j < 5 else (kernel_bc, offset_bc, (j - 5) * Q)
            v = xin[pl.ds(at, 72), j * Q : (j + 1) * Q]
            u = kern[0:1, lo : lo + Q] * v
            for k in range(1, 4):
                u = pltpu.roll(u, 1, 0) + kern[k : k + 1, lo : lo + Q] * v
            v = silu(u[8:72, :] + off[:, lo : lo + Q]).astype(BF16)
            if j < 5:
                xb[pl.ds(at, 64), lo : lo + Q] = v
            else:
                (bmat, cmat)[j - 5][pl.ds(at, 64), :] = v

    def chunk_state(q):
        at = pl.multiple_of(q * Q, Q)
        cq = cum[q]
        fac = jnp.exp(cq[Q - 1 : Q, :] - cq) * dts[q]
        fx = dot(jnp.concatenate(split2(fac), axis=1), expand[...])
        xw = (xb[pl.ds(at, Q), :].astype(F32) * fx).astype(BF16)
        sl[q] = t_dot(bmat[pl.ds(at, Q), :], xw)

    far = xo // 2
    near = 1 - far
    odd = xo % 2
    late = 3 * far + odd
    other = 3 * far + 2 - 2 * odd

    def conv_early(i, carry):
        chip = (x + 3 + i // 3) % NX
        block = 3 * chip + i % 3
        block = jnp.where(jnp.logical_or(block == 0, i == 0), block + 1, block)
        conv_block(block)
        return carry

    remote(rows.at[partner], rows.at[partner], ag_s, ag_r.at[6], (s, partner)).wait_recv()
    ag(hl, 0, 0, hr).wait_recv()
    onward(hl, 0, 4, hr)
    ag(hr, 1, 3, hl).wait_recv()
    onward(hr, 1, 5, hl)
    to_partner(hl, 0, 0)
    to_partner(hr, 1, 3)
    project_x(x)
    partner_done(xl, 0, 0)
    partner_done(xr, 1, 3)
    project_halves(xl, 0, xr, 1)
    ag(hl, 1, 1, hr).wait_recv()
    to_partner(hl, 1, 1)
    ag(hr, 0, 2, hl).wait_recv()
    to_partner(hr, 0, 2)

    @pl.when(c == 0)
    def _():
        partner_done(xl, 1, 1)
        partner_done(xr, 0, 2)

    def put_seconds(core):
        n = jnp.concatenate([rows[2 * xl + core, 1], rows[2 * xr + core, 0]], axis=0)
        put_rows(
            n,
            [(xl * CH + core * R + HALF, 0, HALF), (xr * CH + core * R, HALF, R)],
        )

    put_seconds(1)
    lax.fori_loop(4, 6, conv_early, 0)

    @pl.when(c == 1)
    def _():
        partner_done(xl, 1, 1)
        partner_done(xr, 0, 2)

    put_seconds(0)

    halo = remote(xin.at[pl.ds(T, 8)], xin.at[pl.ds(0, 8)], halo_s, halo_r, ((s + 1) % 32, h))

    @pl.when(jnp.logical_and(s < 31, xo != 3))
    def _():
        halo.start()


    def opposite_in():
        ag(ho, 0, 4, hr).wait_recv()
        ag(ho, 0, 11, partner).start()
        ag(ho, 1, 5, hl).wait_recv()
        ag(ho, 1, 12, partner).start()

    @pl.when(c == 1)
    def _():
        opposite_in()

    for q in (3 * near, 3 * near + 1, 3 * near + 2, other):
        step_sizes(q)
    lax.fori_loop(1, 4, conv_early, 0)
    lax.fori_loop(6, 8, conv_early, 0)

    @pl.when(c == 0)
    def _():
        opposite_in()

    lax.fori_loop(8, 9, conv_early, 0)
    chunk_state(3 * near + 1)
    chunk_state(3 * near + 2)
    partner_done(xo, 0, 4)
    partner_done(xo, 1, 5)
    project_x(xo)

    @pl.when(jnp.logical_and(s < 31, xo == 3))
    def _():
        halo.start()

    step_sizes(late)
    step_sizes(late + 1)
    total = cum[0][Q - 1 : Q, :]
    for q in range(1, NQ):
        total = total + cum[q][Q - 1 : Q, :]
    drow[...] = jnp.broadcast_to(jnp.exp(total), (8, Q))

    owner = 2 * x + 1
    far_first = (4, 3, 5, 2, 6, 1, 7)

    def z_peer(k):
        return (z + k) % NZ

    def rate_copy(k):
        return remote(
            drow, rd.at[c, z], zd_s, zd_r.at[c], (y * NZ + z_peer(k), owner)
        )

    def state_copy(k):
        at = pl.multiple_of(z_peer(k) * 16, 16)
        return remote(
            sb.at[pl.ds(at, 16)], rz.at[c, z], zs_s, zs_r.at[c], (y * NZ + z_peer(k), owner)
        )

    def sum_copy(k):
        return remote(tb, ty.at[y], y_s.at[k - 1], y_r.at[y], ((y + k) % NY * NZ + z, h))

    def sum_rate_copy(k):
        return remote(tdb, tdy.at[y], yd_s.at[k - 1], yd_r.at[y], ((y + k) % NY * NZ + z, h))

    def back_copy(g, k):
        zp = z_peer(k)
        return remote(pb.at[g, zp], cr.at[z], bk_s, bk_r, (y * NZ + zp, 2 * x + g))

    for k in range(1, NZ):
        rate_copy(k).start()

    @pl.when(c == 0)
    def _():
        rate_copy(0).start()

    @pl.when(c == 1)
    def _():
        rd[1, z] = drow[...]

    conv_block(3 * xo + 1)
    conv_block(3 * xo + 2)
    conv_block(jnp.where(xo == 0, 3 * xl, 3 * xo))
    conv_block(jnp.where(xl == 0, 3 * xo, 3 * xl))

    rest = jnp.where(near == 0, 3, 1)
    for k in range(3):
        chunk_state(rest + k)

    ends = jnp.concatenate([cum[q][Q - 1 : Q, :] for q in range(NQ)] + [jnp.zeros((2, Q), F32)], axis=0)
    decs = dot(jnp.concatenate(split2(jnp.exp(ends)), axis=1), expand[...])
    for lo in range(0, DL, Q):
        acc = sl[1, :, lo : lo + Q]
        for q in range(2, NQ):
            acc = acc * decs[q : q + 1, lo : lo + Q] + sl[q, :, lo : lo + Q]
        sacc[:, lo : lo + Q] = acc

    @pl.when(s == 0)
    def _():
        xin[0:8, :] = jnp.zeros((8, DL + 2 * NS), F32)

    @pl.when(s > 0)
    def _():
        halo.wait_recv()

    conv_block(0)
    chunk_state(0)
    later = decs[1:2, :]
    for q in range(2, NQ):
        later = later * decs[q : q + 1, :]
    sb[...] = (sacc[...] + later * sl[0]).astype(BF16)

    for k in far_first:
        state_copy(k).start()

    @pl.when(c == 0)
    def _():
        state_copy(0).start()

    @pl.when(c == 1)
    def _():
        rz[1, z] = sb[pl.ds(pl.multiple_of(z * 16, 16), 16), :]

    for lo in range(0, DL, Q):
        acc = jnp.zeros((NS, Q), F32)
        pd = jnp.ones((1, Q), F32)
        for q in range(NQ):
            st = sl[q, :, lo : lo + Q]
            dec = decs[q : q + 1, lo : lo + Q]
            sl[q, :, lo : lo + Q] = acc
            pdr[q, 0:1, lo : lo + Q] = pd
            acc = acc * dec + st
            pd = pd * dec

    project_z(xo)
    s3 = jnp.concatenate(split2(jnp.broadcast_to(small[2:3, :], (8, Q))), axis=1)
    skip_row = dot(s3, expand[...])[0:1, :]
    low = lax.broadcasted_iota(jnp.int32, (Q, Q), 1) < 64

    def intra_step(q, carry):
        at = pl.multiple_of(q * Q, Q)
        cq = cum[q]
        ef[q] = dot(jnp.concatenate(split2(jnp.exp(cq)), axis=1), expand[...])
        cqt = jnp.transpose(cq)
        dtt = jnp.transpose(dts[q])
        cb = dot_t(cmat[pl.ds(at, Q), :], bmat[pl.ds(at, Q), :])
        cbm = jnp.where(ri >= ci, cb, 0.0)
        for j in range(HEADS // 2):
            mixes = []
            for hh in (2 * j, 2 * j + 1):
                gap = jnp.minimum(cq[:, hh : hh + 1] - cqt[hh : hh + 1, :], 0.0)
                mixes.append((cbm * jnp.exp(gap) * dtt[hh : hh + 1, :]).astype(BF16))
            xp = xb[pl.ds(at, Q), j * Q : (j + 1) * Q].astype(F32)
            xd = jnp.concatenate(
                [jnp.where(low, xp, 0.0).astype(BF16), jnp.where(low, 0.0, xp).astype(BF16)], axis=0
            )
            yq = dot(jnp.concatenate(mixes, axis=1), xd)
            yv[pl.ds(at, Q), j * Q : (j + 1) * Q] = yq + skip_row[:, j * Q : (j + 1) * Q] * xp
        return carry

    lax.fori_loop(0, NQ, intra_step, 0)

    @pl.when(c == 1)
    def _():
        for g in (1, 0):
            if g == 1:
                await_bytes(dtr.at[pl.ds(0, 56)], zd_r.at[1])
            else:
                await_bytes(rd.at[0], zd_r.at[0])
            dz = jnp.concatenate([rd[g, k][0:1, :] for k in range(NZ)], axis=0)
            dx = dot(jnp.concatenate(split2(dz), axis=1), expand[...])
            dxs[g] = dx
            pd = jnp.ones((1, DL), F32)
            for k in range(NZ):
                pdz[g, k] = jnp.broadcast_to(pd, (8, DL))
                pd = pd * dx[k : k + 1, :]
            tdb[g] = jnp.broadcast_to(pd, (8, DL))
        for k in range(1, NY):
            @pl.when(y + k < NY)
            def _(k=k):
                sum_rate_copy(k).start()

    project_z(xl)

    @pl.when(c == 1)
    def _():
        for g in (1, 0):
            if g == 1:
                await_bytes(xb.at[pl.ds(0, 112)], zs_r.at[1])
            else:
                await_bytes(rz.at[0], zs_r.at[0])
            dx = dxs[g]
            acc = jnp.zeros((16, DL), F32)
            for k in range(NZ):
                pz[g, k] = acc
                acc = acc * dx[k : k + 1, :] + rz[g, k].astype(F32)
            tb[g] = acc.astype(BF16)
        for k in (2, 1, 3):
            @pl.when(y + k < NY)
            def _(k=k):
                sum_copy(k).start()


    @pl.when(c == 1)
    def _():
        cacc[...] = jnp.zeros_like(cacc)
        for k in range(NY - 1):
            @pl.when(k < y)
            def _(k=k):
                dev = (k * NZ + z, h)
                remote(tb, ty.at[k], y_s.at[0], y_r.at[k], dev).wait_recv()
                remote(tdb, tdy.at[k], yd_s.at[0], yd_r.at[k], dev).wait_recv()
                for g in range(2):
                    cacc[g] = cacc[g] * tdy[k, g][0:1, :] + ty[k, g].astype(F32)
        for g in range(2):
            for k in range(NZ):
                pb[g, k] = (pz[g, k] + pdz[g, k][0:1, :] * cacc[g]).astype(BF16)
        for k in far_first:
            for g in range(2):
                back_copy(g, k).start()
        back_copy(0, 0).start()
        cr[z] = pb[1, z]

    project_z(x)
    project_z(xr)

    @pl.when(c == 1)
    def _():
        await_bytes(xb.at[pl.ds(0, 112)], bk_r)

    @pl.when(c == 0)
    def _():
        await_bytes(cr, bk_r)

    def out_step(q, carry):
        at = pl.multiple_of(q * Q, Q)
        state = (sl[q] + pdr[q][0:1, :] * cr[...].reshape(NS, DL).astype(F32)).astype(BF16)
        cross = dot(cmat[pl.ds(at, Q), :], state)
        g = (yv[pl.ds(at, Q), :] + ef[q] * cross) * zs[pl.ds(at, Q), :]
        sqc[pl.ds(at, Q), :] = jnp.broadcast_to(jnp.sum(g * g, axis=1, keepdims=True), (Q, Q))
        gb[pl.ds(at, Q), :] = (g * norm_gain[...]).astype(BF16)
        return carry

    def pair_copy(d, lo, width, sem):
        return remote(
            part.at[2 * d + 1 - c, :, :, pl.ds(lo, width)], pr.at[d, :, :, pl.ds(lo, width)],
            pp_s, pp_r.at[sem], (s, partner),
        )

    def out_part(d, lo, width, sem):
        n = gb[pl.ds(pl.multiple_of(d * CH, CH), CH), :]
        for at in range(lo, lo + width, 256):
            end = min(at + 256, lo + width)
            part[pl.ds(2 * d, 2), :, :, at:end] = (
                dot(n, wout[:, at:end]).astype(BF16).reshape(2, 2, HALF, end - at)
            )
        pair_copy(d, lo, width, sem).start()

    def out_chip(d):
        out_part(d, 0, D, d)

    def pair_sum(d, half):
        return part[2 * d + c, half].astype(F32) + pr[d, half].astype(F32)

    def pair_wait(d):
        remote(part.at[0], pr.at[d], pp_s, pp_r.at[d], (s, partner)).wait_recv()

    d1 = xo + 1 - 2 * (xo % 2)
    d2 = x + 1 - 2 * (x % 2)
    out_step(late, 0)
    out_step(late + 1, 0)
    cuts = ((0, 512), (512, 896), (1408, 1152))
    pieces = len(cuts)

    def relay_copy(half, i):
        here = pl.ds(*cuts[i])
        return remote(
            ps.at[0, half, :, here], rl.at[half, :, here], rl_s, rl_r.at[half, i],
            (s, hl if half else hr),
        )

    def relay(i):
        here = pl.ds(*cuts[i])
        pair_copy(xo, *cuts[i], 4 + i).wait_recv()
        for half in range(2):
            ps[0, half, :, here] = (
                part[2 * xo + c, half, :, here].astype(F32) + pr[xo, half, :, here].astype(F32)
            ).astype(BF16)
            relay_copy(half, i).start()

    @pl.when(c == 0)
    def _():
        for i in range(pieces):
            out_part(xo, *cuts[i], 4 + i)
            if i > 0:
                relay(i - 1)
        relay(pieces - 1)
        out_step(other, 0)
        out_chip(d1)

    @pl.when(c == 1)
    def _():
        for i in range(pieces):
            out_part(xo, *cuts[i], 4 + i)
        relay(0)
        out_step(other, 0)
        relay(1)
        out_chip(d1)
        relay(2)

    lax.fori_loop(near * 3, near * 3 + 3, out_step, 0)
    out_chip(d2)

    def side_of(d):
        return jnp.where(d == xr, 0, 1)

    finals = []

    def final_send(slot, d, half):
        side = side_of(d)
        cp = remote(
            ps.at[slot, half], rf.at[side, half], rf_s, rf_r.at[side, half], (s, 2 * d + c)
        )
        cp.start()
        finals.append(cp)

    def send_direct(slot, d):
        half = 1 - side_of(d)
        pair_wait(d)
        ps[slot, half] = pair_sum(d, half).astype(BF16)
        final_send(slot, d, half)

    def send_relayed(slot, d):
        half = side_of(d)
        for i in range(pieces):
            here = pl.ds(*cuts[i])
            remote(
                ps.at[0, 0, :, here], rl.at[half, :, here], rl_s, rl_r.at[half, i], (s, hr)
            ).wait_recv()
        ps[slot, half] = (pair_sum(d, half) + rl[half].astype(F32)).astype(BF16)
        final_send(slot, d, half)

    send_direct(1, d1)
    sq_sends = []
    for k in range(8):
        col = sqc[pl.ds(pl.multiple_of(((h + k) % 8) * R, 32), Q), :]
        sqs[(h + k) % 8] = jnp.transpose(col)[0:8, :]
        if k == 0:
            sqr[h] = sqs[h]
        else:
            cp = remote(sqs.at[(h + k) % 8], sqr.at[h], sq_s, sq_r, (s, (h + k) % 8))
            cp.start()
            sq_sends.append(cp)
    send_direct(2, d2)
    send_relayed(1, d1)
    send_relayed(2, d2)
    out_chip(x)

    pair_wait(x)

    def final_wait(side, half):
        remote(
            ps.at[1, half], rf.at[side, half], rf_s, rf_r.at[side, half], (s, hl)
        ).wait_recv()

    for half in range(2):
        final_wait(1 - half, half)
        tot[half] = pair_sum(x, half) + rf[1 - half, half].astype(F32)
    await_bytes(dtr.at[pl.ds(0, 56)], sq_r)
    squares = jnp.sum(sqr[...], axis=0)[0:1, :]
    inv_row = lax.rsqrt(squares / (DL * 8) + NORM_FLOOR)
    inv_col = jnp.transpose(jnp.broadcast_to(inv_row, (Q, Q)))
    for half in range(2):
        final_wait(half, half)
        out[half * HALF : (half + 1) * HALF, :] = (
            (tot[half] + rf[half, half].astype(F32)) * inv_col[half * HALF : (half + 1) * HALF, 0:1]
        ).astype(BF16)

    await_bytes(rows.at[pl.ds(0, 7)], ag_s)
    await_bytes(part.at[pl.ds(0, 4)], pp_s)
    await_bytes(part.at[0], rl_s)
    await_bytes(part.at[pl.ds(0, 2)], rf_s)
    await_bytes(dtr.at[pl.ds(0, 56)], sq_s)

    @pl.when(s < 31)
    def _():
        halo.wait_send()

    @pl.when(c == 0)
    def _():
        await_bytes(rd.at[0], zd_s)
        await_bytes(rz.at[0], zs_s)

    @pl.when(c == 1)
    def _():
        await_bytes(dtr.at[pl.ds(0, 56)], zd_s)
        await_bytes(xb.at[pl.ds(0, 112)], zs_s)
        await_bytes(xb.at[pl.ds(0, 240)], bk_s)
        for k in range(1, NY):
            @pl.when(y + k < NY)
            def _(k=k):
                sum_copy(k).wait_send()
                sum_rate_copy(k).wait_send()


def on_device(
    tokens, pre_gain, inner_proj, outer_proj, kernel_x, kernel_bc, offset_x, offset_bc, dt_bias, a_log,
    skip_gain, norm_gain, out_proj,
):
    vm = pl.BlockSpec(memory_space=pltpu.VMEM)
    hbm = pl.BlockSpec(memory_space=pltpu.HBM)
    dma = pltpu.SemaphoreType.DMA
    V = pltpu.VMEM
    scratch = [
        V((R, D), BF16), V((D // Q, Q), F32), V((4, DL), F32), V((4, 2 * NS), F32), V((DL // Q, Q), F32),
        V((1, 2 * NS), F32), V((1, HEADS), F32), V((1, HEADS), F32), V((1, HEADS), F32), V((DL // Q, Q), F32),
        V((D, 2, DL), BF16), V((D, DL), BF16), V((D, 1024), BF16), V((384, D), BF16), V((DL, D), BF16), V((8, 2, HALF, D), BF16),
        V((T + 8, DL + 2 * NS), F32), V((T, Q), F32), V((T, DL), F32), V((T, DL), BF16),
        V((T, NS), BF16), V((T, NS), BF16), V((NQ, Q, Q), F32), V((NQ, Q, Q), F32),
        V((2 * Q, DL), BF16), V((NQ, Q, DL), F32), V((NQ, NS, DL), F32), V((NS, DL), F32),
        V((NQ, 8, DL), F32),
        V((T, DL), F32), V((NS, DL), BF16), V((8, Q), F32), V((2, NZ, 16, DL), BF16), V((2, NZ, 8, Q), F32), V((2, NZ, DL), F32),
        V((2, NZ, 16, DL), F32), V((2, NZ, 8, DL), F32), V((2, 16, DL), BF16), V((2, 8, DL), F32),
        V((NY, 2, 16, DL), BF16), V((NY, 2, 8, DL), F32), V((2, 16, DL), F32), V((2, NZ, 16, DL), BF16),
        V((NZ, 16, DL), BF16), V((T, DL), BF16), V((T + 32, Q), F32), V((8, 2, HALF, D), BF16),
        V((NX, 2, HALF, D), BF16), V((3, 2, HALF, D), BF16), V((2, HALF, D), BF16), V((2, 2, HALF, D), BF16),
        V((8, 8, Q), F32), V((8, 8, Q), F32), V((8, Q), F32), V((1, D), F32), V((1, DL), F32),
        V((1, DL), F32), V((2, HALF, D), F32),
        dma, dma((13,)), dma, dma, dma, dma((2,)), dma, dma((2,)),
        dma((NY - 1,)), dma((NY - 1,)), dma((NY - 1,)), dma((NY - 1,)), dma, dma,
        dma, dma((7,)), dma, dma((2, 3)), dma, dma((2, 2)), dma, dma,
        dma((6,)), dma((10,)),
    ]
    args = (
        tokens, pre_gain.reshape(D // Q, Q), inner_proj, outer_proj.T, kernel_x, kernel_bc,
        offset_x.reshape(DL // Q, Q), offset_bc[None], dt_bias[None], a_log[None], skip_gain[None],
        norm_gain.reshape(DL // Q, Q), out_proj,
    )
    args = [pltpu.with_memory_space_constraint(v, pltpu.HBM) for v in args]
    return pl.pallas_call(
        kernel,
        out_shape=jax.ShapeDtypeStruct((R, D), BF16),
        in_specs=[hbm] * 13,
        out_specs=vm,
        scratch_shapes=scratch,
        compiler_params=pltpu.CompilerParams(
            collective_id=0, has_side_effects=True, vmem_limit_bytes=55_000_000
        ),
    )(*args)


def solution(mesh):
    in_specs = (
        P(("seq", "head"), None), P(), P(None, None, "head"), P(), P(None, "head"), P(), P("head"), P(),
        P("head"), P("head"), P("head"), P("head"), P("head", None),
    )
    return jax.shard_map(
        on_device, mesh=mesh, in_specs=in_specs, out_specs=P(("seq", "head"), None), check_vma=False
    )
```
